256 devices in a mesh: context: 16 (over z, core), tensor: 4 (over x), fsdp: 4 (over y).
Axes of the slice: x: 4, y: 4, z: 8, core: 2. Of those that a mesh axis runs over, the one named last changes fastest.
Arguments:
- input_raw: bfloat16 [4, 8192, 5120], P('fsdp', ('context', 'tensor')), may hold values from -6 to 6
- state_proj_raw: bfloat16 [4, 8192, 256], P('fsdp', ('context', 'tensor')), may hold values from -6 to 6
- gate_branch: bfloat16 [4, 8192, 5120], P('fsdp', ('context', 'tensor')), may hold values from -6 to 6
- step_raw: bfloat16 [4, 8192, 80], P('fsdp', ('context', 'tensor')), may hold values from -6 to 6
- convolution_taps: float32 [4, 5376], replicated, may hold values from -3 to 3
- convolution_bias: float32 [5376], replicated, may hold values from -3 to 3
- step_bias: float32 [80], P('tensor'), may hold values from -1.5 to 0.5
- decay_log_rate: float32 [80], P('tensor'), may hold values from -13 to -2, as said below
- skip_weight: float32 [80], P('tensor'), may hold values from 0.5 to 2
- gated_norm_gain: float32 [5120], P('tensor'), may hold values from 0.1 to 1.9
- output_weight: bfloat16 [5120, 2560], P('tensor', 'fsdp'), may hold values from -0.078125 to 0.078125
- adapter_down: bfloat16 [5120, 16], P('tensor'), may hold values from -0.078125 to 0.078125
- adapter_up: bfloat16 [16, 2560], replicated, may hold values from -0.29882812 to 0.29882812
- cotangent: bfloat16 [4, 8192, 2560], P('fsdp', ('context', 'tensor')), may hold values from -6 to 6
Outputs:
- mixed: bfloat16 [4, 8192, 2560], P('fsdp', ('context', 'tensor'))
- grad_a: float32 [5120, 16], P('tensor')
- grad_b: float32 [16, 2560], replicated
The draws below stay inside these ranges and needn't reach their ends.
Inputs may be any that keep to these rules, and one draw needn't show every extreme that they name: `decay_log_rate`: logarithms of positive decay rates.
All inputs are finite; a program needn't handle non-finite values.
Results may differ from the reference program's by a relative error of at most 0.017.
Values may be sent and summed in bfloat16 or wider, within the bound.
A program may use at most 128 MiB of HBM per device.

```python
import math
import jax
import jax.numpy as jnp
from jax import lax

MODEL_WIDTH = 2560
H = 80
N = 128
ADAPTER_RANK = 16
CONV = 4
MIXER_WIDTH = 5120
SEQS = 4
LEN = 8192


def draw_decay_log_rate(key, part):
    pick_key, slow_key, fast_key = jax.random.split(jax.random.fold_in(key, 11), 3)
    keep_share = 5
    slow_mask = jax.random.randint(pick_key, (H,), 0, 10) < keep_share
    low_log = jnp.log(0.5 / LEN)
    high_log = jnp.log(2.5 / LEN)
    slow_rate = jax.random.uniform(slow_key, (H,), jnp.float32, low_log, high_log)
    fast_rate = jnp.log(jax.random.uniform(fast_key, (H,), jnp.float32, 1.0 / 60.0, 1.0 / 20.0))
    return jnp.where(slow_mask, slow_rate, fast_rate)


def block_levels(rng, dims, cuts, low, largest):
    gain, own = 1.0, jax.random.fold_in(rng, 6)
    for position, parts in cuts:
        heights = jnp.exp(jax.random.uniform(jax.random.fold_in(own, position), (parts,), jnp.float32, low / len(cuts), largest / len(cuts)))
        gain = gain * jnp.repeat(heights, dims[position] // parts).reshape([-1 if axis == position else 1 for axis in range(len(dims))])
    return gain


def centred(stream_key, dims, width, reach, cuts=(), held_as=jnp.bfloat16):
    level = block_levels(stream_key, dims, cuts, -0.22, 0.18) if cuts else 1.0
    result = jax.random.normal(stream_key, dims, jnp.float32) * width * level
    return jnp.minimum(jnp.maximum(result, -reach), reach).astype(held_as)


def setup_inputs(seed: int = 0) -> dict:
    arg_keys = jax.random.split(jax.random.key(seed), 15)
    input_raw = centred(arg_keys[0], (SEQS, LEN, MIXER_WIDTH), 1.0, 6.0, ((0, 4), (1, 64)))
    state_proj_raw = centred(arg_keys[1], (SEQS, LEN, 2 * N), 1.0, 6.0, ((0, 4), (1, 64)))
    gate_branch = centred(arg_keys[2], (SEQS, LEN, MIXER_WIDTH), 1.0, 6.0, ((0, 4), (1, 64)))
    step_raw = centred(arg_keys[3], (SEQS, LEN, H), 1.0, 6.0, ((0, 4), (1, 64)))
    convolution_taps = centred(arg_keys[4], (CONV, MIXER_WIDTH + 2 * N), CONV ** -0.5, 3.0, (), jnp.float32)
    convolution_bias = centred(arg_keys[5], (MIXER_WIDTH + 2 * N,), 0.5, 3.0, (), jnp.float32)
    step_bias = jnp.clip(-1.5 + 2.0 * jax.random.uniform(arg_keys[6], (H,), jnp.float32) ** block_levels(arg_keys[6], (H,), ((0, 4),), -0.2, 0.2), -1.5, 0.5)
    decay_log_rate = draw_decay_log_rate(jax.random.fold_in(arg_keys[14], 71), 0)
    skip_weight = jnp.clip(0.5 + 1.5 * jax.random.uniform(arg_keys[8], (H,), jnp.float32) ** block_levels(arg_keys[8], (H,), ((0, 4),), -0.2, 0.2), 0.5, 2.0)
    gated_norm_gain = jnp.clip(1.0 + 0.18 * jax.random.normal(arg_keys[9], (MIXER_WIDTH,), jnp.float32), 0.1, 1.9)
    output_weight = centred(arg_keys[10], (MIXER_WIDTH, MODEL_WIDTH), MIXER_WIDTH ** -0.5, 0.078125, ((0, 4), (1, 4)))
    adapter_down = centred(arg_keys[11], (MIXER_WIDTH, ADAPTER_RANK), MIXER_WIDTH ** -0.5, 0.078125, ((0, 4),))
    adapter_up = centred(arg_keys[12], (ADAPTER_RANK, MODEL_WIDTH), 0.05, 0.29882812)
    cotangent = centred(arg_keys[13], (SEQS, LEN, MODEL_WIDTH), 1.0, 6.0, ((0, 4), (1, 64)))
    return dict(input_raw=input_raw, state_proj_raw=state_proj_raw, gate_branch=gate_branch, step_raw=step_raw, convolution_taps=convolution_taps, convolution_bias=convolution_bias, step_bias=step_bias, decay_log_rate=decay_log_rate, skip_weight=skip_weight, gated_norm_gain=gated_norm_gain, output_weight=output_weight, adapter_down=adapter_down, adapter_up=adapter_up, cotangent=cotangent)


def ssd_blocks(x_heads, b_rows, c_rows, step_size, log_decay, block_len):
    highest = lax.Precision.HIGHEST
    length = x_heads.shape[0]
    head_count = x_heads.shape[1]
    head_size = x_heads.shape[2]
    state_size = b_rows.shape[1]
    blocks = length // block_len
    causal = jnp.arange(block_len)[:, None] >= jnp.arange(block_len)[None, :]

    def advance(state_now, pieces):
        x_block, b_block, c_block, step_block, decay_block = pieces
        cum_decay = jnp.cumsum(decay_block, axis=0)
        cum_heads = cum_decay.T
        gap_decay = cum_heads[:, :, None] - cum_heads[:, None, :]
        decay_mat = jnp.where(causal[None], jnp.exp(jnp.where(causal[None], gap_decay, 0.0)), 0.0)
        gram_mat = jnp.dot(c_block, b_block.T, precision=highest)
        x_scaled = x_block * step_block[:, :, None]
        y_inner = jnp.einsum('hij,jhp->ihp', decay_mat * gram_mat[None], x_scaled, precision=highest)
        y_state = jnp.exp(cum_decay)[:, :, None] * jnp.einsum('in,hpn->ihp', c_block, state_now, precision=highest)
        tail_decay = jnp.exp(cum_decay[-1][None, :] - cum_decay)
        state_next = jnp.exp(cum_decay[-1])[:, None, None] * state_now + jnp.einsum('jhp,jn->hpn', x_scaled * tail_decay[:, :, None], b_block, precision=highest)
        return (state_next, y_inner + y_state)
    start_state = jnp.zeros((head_count, head_size, state_size), jnp.float32)
    state_end, y_blocks = lax.scan(advance, start_state, (x_heads.reshape(blocks, block_len, head_count, head_size), b_rows.reshape(blocks, block_len, state_size), c_rows.reshape(blocks, block_len, state_size), step_size.reshape(blocks, block_len, head_count), log_decay.reshape(blocks, block_len, head_count)))
    return (y_blocks.reshape(length, head_count, head_size), state_end)

def reference(input_raw, state_proj_raw, gate_branch, step_raw, convolution_taps, convolution_bias, step_bias, decay_log_rate, skip_weight, gated_norm_gain, output_weight, adapter_down, adapter_up, cotangent):
    highest = lax.Precision.HIGHEST
    inner_width = input_raw.shape[2]
    state_size = state_proj_raw.shape[2] // 2
    head_count = decay_log_rate.shape[0]
    head_size = inner_width // head_count
    length = input_raw.shape[1]
    taps = convolution_taps.shape[0]
    block_len = math.gcd(length, 256)
    lowrank_factor = 2.0 / math.sqrt(input_raw.shape[0] * length)
    decay_rate = jnp.exp(decay_log_rate)

    def one_sequence(pieces):
        x_seq, bc_seq, z_seq, dt_seq, cotangent_sequence = pieces
        joined = jnp.concatenate([x_seq, bc_seq], axis=1)
        padded = jnp.concatenate([jnp.zeros((taps - 1, joined.shape[1]), joined.dtype), joined], axis=0)
        pre_act = convolution_bias[None, :] + convolution_taps[0][None, :] * padded[0:length].astype(jnp.float32)
        for tap_index in range(1, taps):
            pre_act = pre_act + convolution_taps[tap_index][None, :] * padded[tap_index:tap_index + length].astype(jnp.float32)
        xbc = jax.nn.silu(pre_act).astype(jnp.bfloat16)
        x_heads = xbc[:, :inner_width].astype(jnp.float32).reshape(length, head_count, head_size)
        b_rows = xbc[:, inner_width:inner_width + state_size].astype(jnp.float32)
        c_rows = xbc[:, inner_width + state_size:].astype(jnp.float32)
        step_size = jax.nn.softplus(dt_seq.astype(jnp.float32) + step_bias[None, :])
        log_decay = -step_size * decay_rate[None, :]
        y_heads, state_end = ssd_blocks(x_heads, b_rows, c_rows, step_size, log_decay, block_len)
        y_heads = y_heads + skip_weight[None, :, None] * x_heads
        gated = y_heads.reshape(length, inner_width) * jax.nn.silu(z_seq.astype(jnp.float32))
        row_norm_scale = lax.rsqrt(lax.optimization_barrier(jnp.mean(gated * gated, axis=1)) + 1e-05)
        gated_output = (gated * gated_norm_gain[None, :]).astype(jnp.bfloat16)
        adapter_branch = jnp.dot(gated_output, adapter_down, preferred_element_type=jnp.float32).astype(jnp.bfloat16)
        frozen_piece = jnp.dot(gated_output, output_weight, preferred_element_type=jnp.float32)
        frozen_piece = frozen_piece + 2.0 * jnp.dot(adapter_branch, adapter_up, preferred_element_type=jnp.float32)
        mixed = (row_norm_scale[:, None] * frozen_piece).astype(jnp.bfloat16)
        weighted = lowrank_factor * row_norm_scale[:, None] * adapter_branch.astype(jnp.float32)
        grad_b_part = jnp.dot(weighted.T, cotangent_sequence.astype(jnp.float32), precision=highest)
        adapter_gradient = lowrank_factor * row_norm_scale[:, None] * jnp.dot(cotangent_sequence, adapter_up.T, preferred_element_type=jnp.float32)
        grad_a_part = jnp.dot(gated_output.astype(jnp.float32).T, adapter_gradient, precision=highest)
        return (mixed, grad_a_part, grad_b_part)
    mixed, grad_a_parts, grad_b_parts = lax.map(one_sequence, (input_raw, state_proj_raw, gate_branch, step_raw, cotangent))
    return (mixed, lax.optimization_barrier(jnp.sum(grad_a_parts, axis=0)), lax.optimization_barrier(jnp.sum(grad_b_parts, axis=0)))
```

```python
import functools

import jax
import jax.numpy as jnp
from jax import lax
from jax.experimental import pallas as pl
from jax.experimental.pallas import tpu as pltpu
from jax.sharding import Mesh
from jax.sharding import PartitionSpec as P

MESH = pl.DeviceIdType.MESH
CONTEXT_TENSOR = ("context_0", "context_1", "tensor")
F32 = jnp.float32
BF16 = jnp.bfloat16

ROWS = 128
WIDTH = 1280
STATE = 128
OUT = 2560
HALF = 1280
RANK = 16
HEADS = 20
COLS = 640
TOKENS = 32768
EPS = 1e-05

NT = (((1,), (1,)), ((), ()))
TN = (((0,), (0,)), ((), ()))


def silu(v):
    half = 0.5 * v
    return half + half * jnp.tanh(half)


def dot(a, b, dims=(((1,), (0,)), ((), ())), precision=None):
    return lax.dot_general(a, b, dims, precision=precision, preferred_element_type=F32)


def kernel(
    x_in, bc_in, z_in, dt_in, w_in, cot_in, par, down_t, up,
    mixed, grad_a, grad_b,
    x_ext, xr, xc, bc_ext, bcc, dt_all, gate, zr, wt, cot,
    spread, step, cum, log_dec, y_in, blocks, state, st_send, st_recv, dec_all, dec_wide, back_send, back_recv,
    gated, gt, sq, ap_send, ap_recv,
    rs_send, rs_recv, own,
    v_send, v_recv, xy_recv, v_all,
    sx, rx, sl, sc, rc_, sd, rd, sb, rb, sv, rv, sxy, rxy, sg, rg,
):
    z, k = lax.axis_index("context_0"), lax.axis_index("context_1")
    t, s = lax.axis_index("tensor"), lax.axis_index("fsdp")
    c = 2 * z + k
    right, left, far = lax.rem(t + 1, 4), lax.rem(t + 3, 4), lax.rem(t + 2, 4)
    up_y, down_y = lax.rem(s + 1, 4), lax.rem(s + 3, 4)
    started = []

    def remote(src, dst, index, where):
        return pltpu.make_async_remote_copy(
            src_ref=src, dst_ref=dst, send_sem=sx.at[index], recv_sem=rx.at[index],
            device_id=where, device_id_type=MESH,
        )

    def send(src, dst, index, where):
        copy = remote(src, dst, index, where)
        copy.start()
        started.append(copy)

    def arrived(dst, index):
        remote(dst, dst, index, {"tensor": right}).wait_recv()

    def context_peer(j):
        target = lax.rem(c + j, 16)
        return {"context_0": lax.div(target, 2), "context_1": lax.rem(target, 2)}

    def plane_peer(j):
        return {"tensor": lax.rem(t + lax.div(j, 4), 4), "fsdp": lax.rem(s + lax.rem(j, 4), 4)}

    def exchange(make, how_many=16):
        def go(j, carry):
            make(j).start()
            return carry

        lax.fori_loop(1, how_many, go, 0)

    def settle(make, how_many=16, received=True):
        def go(j, carry):
            if received:
                make(j).wait_recv()
            else:
                make(j).wait_send()
            return carry

        lax.fori_loop(1, how_many, go, 0)

    barrier = pltpu.get_barrier_semaphore()

    def greet(j, carry):
        pl.semaphore_signal(barrier, inc=1, device_id=context_peer(j), device_id_type=MESH)
        pl.semaphore_signal(barrier, inc=1, device_id=plane_peer(j), device_id_type=MESH)
        return carry

    lax.fori_loop(1, 16, greet, 0)
    before = lax.rem(c + 15, 16)
    after = lax.rem(c + 1, 16)

    @pl.when(c > 0)
    def _():
        pl.semaphore_signal(
            barrier, inc=1,
            device_id={"context_0": lax.div(before, 2), "context_1": lax.rem(before, 2), "tensor": 3},
            device_id_type=MESH,
        )

    gives_rim = jnp.logical_and(t == 3, c < 15)

    @pl.when(gives_rim)
    def _():
        pl.semaphore_wait(barrier, 34)

    @pl.when(jnp.logical_not(gives_rim))
    def _():
        pl.semaphore_wait(barrier, 30)

    def rim_copies():
        copies = []
        for p in range(4):
            where = {"context_0": lax.div(after, 2), "context_1": lax.rem(after, 2), "tensor": p}
            copies.append(pltpu.make_async_remote_copy(
                src_ref=x_in.at[pl.ds(112, 16), pl.ds(p * WIDTH, WIDTH)], dst_ref=x_ext.at[pl.ds(0, 16)],
                send_sem=sl.at[16 + p], recv_sem=rx.at[30], device_id=where, device_id_type=MESH))
            copies.append(pltpu.make_async_remote_copy(
                src_ref=bc_in.at[pl.ds(112, 16)], dst_ref=bc_ext.at[pl.ds(0, 16)],
                send_sem=sl.at[20 + p], recv_sem=rx.at[31], device_id=where, device_id_type=MESH))
        return copies

    @pl.when(gives_rim)
    def _():
        for copy in rim_copies():
            copy.start()

    def columns(p):
        return pl.ds(pl.multiple_of(p * WIDTH, WIDTH), WIDTH)

    def x_rows(p, first, count):
        return x_ext.at[pl.ds(pl.multiple_of(16 + p * ROWS + first, 16), count)]

    def z_rows(p, first, count):
        return gate.at[p, pl.ds(first, count)]

    def spread_start(src, rows, relay, base):
        send(src.at[pl.ds(0, 64), columns(far)], relay.at[0], base, {"tensor": right})
        send(src.at[pl.ds(64, 64), columns(far)], relay.at[1], base + 1, {"tensor": left})
        send(src.at[:, columns(right)], rows(t, 0, ROWS), base + 2, {"tensor": right})
        send(src.at[:, columns(left)], rows(t, 0, ROWS), base + 3, {"tensor": left})

    def spread_forward(rows, relay, base):
        arrived(relay.at[0], base)
        send(relay.at[0], rows(left, 0, 64), base + 4, {"tensor": right})
        arrived(relay.at[1], base + 1)
        send(relay.at[1], rows(right, 64, 64), base + 5, {"tensor": left})

    def spread_wait(rows, base):
        arrived(rows(left, 0, ROWS), base + 2)
        arrived(rows(right, 0, ROWS), base + 3)
        arrived(rows(far, 0, 64), base + 4)
        arrived(rows(far, 64, 64), base + 5)

    for j in range(1, 4):
        peer = {"tensor": lax.rem(t + j, 4)}
        send(bc_in, bc_ext.at[pl.ds(pl.multiple_of(16 + t * ROWS, 16), ROWS)], 12 + j, peer)
        send(dt_in, dt_all.at[t], 15 + j, peer)
    spread_start(x_in, x_rows, xr, 0)

    def w_part(rows_from, count, y):
        return wt.at[
            pl.ds(pl.multiple_of(rows_from, 64), count), pl.ds(pl.multiple_of(y * COLS, COLS), COLS)
        ]

    mine, other = k * 640, (1 - k) * 640

    def w_src(first):
        return w_in.at[pl.ds(pl.multiple_of(mine + first, 64), 320)]

    send(w_src(0), w_part(mine, 320, s), 32, {"fsdp": up_y})
    send(w_src(320), w_part(mine + 320, 320, s), 33, {"fsdp": down_y})
    send(w_src(320), w_part(mine + 320, 320, s), 34, {"fsdp": up_y})
    send(w_src(0), w_part(mine, 320, s), 35, {"fsdp": down_y})

    local = [
        pltpu.make_async_copy(cot_in, cot, sl.at[0]),
        pltpu.make_async_copy(bc_in, bc_ext.at[pl.ds(pl.multiple_of(16 + t * ROWS, 16), ROWS)], sl.at[1]),
        pltpu.make_async_copy(dt_in, dt_all.at[t], sl.at[2]),
        pltpu.make_async_copy(x_in.at[:, columns(t)], x_rows(t, 0, ROWS), sl.at[3]),
        pltpu.make_async_copy(z_in.at[:, columns(t)], gate.at[t], sl.at[4]),
        pltpu.make_async_copy(w_in, w_part(0, 1280, s), sl.at[5]),
    ]
    for copy in local:
        copy.start()

    def head_mask(i, carry):
        lanes = pl.ds(pl.multiple_of(i * 128, 128), 128)
        head = lax.broadcasted_iota(jnp.int32, (256, 128), 0)
        head = jnp.where(head >= 128, head - 128, head)
        lane = lax.broadcasted_iota(jnp.int32, (256, 128), 1)
        own_head = 2 * i + jnp.where(lane >= 64, 1, 0)
        spread[:, lanes] = jnp.where(head == own_head, 1.0, 0.0).astype(BF16)
        return carry

    lax.fori_loop(0, 10, head_mask, 0)

    def widen(v):
        high = v.astype(BF16)
        low = (v - high.astype(F32)).astype(BF16)
        return dot(jnp.concatenate([high, low], axis=1), spread[...])

    scale = 2.0 / (TOKENS ** 0.5)

    local[0].wait()
    gt[t] = dot(up[...], cot[...], NT) * scale
    for j in range(1, 4):
        send(gt.at[t], gt.at[t], 18 + j, {"tensor": lax.rem(t + j, 4)})

    local[1].wait()
    local[2].wait()
    for j in range(1, 4):
        source = lax.rem(t + 4 - j, 4)
        arrived(bc_ext.at[pl.ds(pl.multiple_of(16 + source * ROWS, 16), ROWS)], 12 + j)
        arrived(dt_all.at[source], 15 + j)

    row = lax.broadcasted_iota(jnp.int32, (128, 128), 0)
    col = lax.broadcasted_iota(jnp.int32, (128, 128), 1)
    causal = row >= col

    def steps(p, carry):
        pick_row = lax.broadcasted_iota(jnp.int32, (80, 128), 0)
        pick_col = lax.broadcasted_iota(jnp.int32, (80, 128), 1)
        hit = jnp.logical_and(pick_row == pick_col + t * HEADS, pick_col < HEADS)
        raw = dot(dt_all[p], jnp.where(hit, 1.0, 0.0).astype(BF16))
        raw = raw + par[7:8, 0:128]
        step_now = jnp.maximum(raw, 0.0) + jnp.log1p(jnp.exp(-jnp.abs(raw)))
        decay = -step_now * jnp.exp(par[8:9, 0:128])
        tri = jnp.where(row >= col, 1.0, 0.0)
        step[p] = step_now
        cum[p] = dot(tri, decay, precision=lax.Precision.HIGHEST)
        return carry

    lax.fori_loop(0, 4, steps, 0)

    @pl.when(c == 0)
    def _():
        x_ext[0:16, :] = jnp.zeros((16, WIDTH), BF16)
        bc_ext[0:16, :] = jnp.zeros((16, 256), BF16)

    @pl.when(c > 0)
    def _():
        arrived(x_ext.at[pl.ds(0, 16)], 30)
        arrived(bc_ext.at[pl.ds(0, 16)], 31)

    def convolved(ext, p, lanes, taps):
        v = ext[pl.ds(pl.multiple_of(p * ROWS, 16), ROWS + 16), lanes].astype(F32)
        acc = par[4:5, taps] + par[0:1, taps] * pltpu.roll(v, 3, 0)
        acc = acc + par[1:2, taps] * pltpu.roll(v, 2, 0)
        acc = acc + par[2:3, taps] * pltpu.roll(v, 1, 0)
        acc = acc + par[3:4, taps] * v
        return silu(acc[16:]).astype(BF16)

    def conv_shared(p, carry):
        for i in range(2):
            bcc[p, :, pl.ds(i * 128, 128)] = convolved(
                bc_ext, p, pl.ds(i * 128, 128), pl.ds(WIDTH + i * 128, 128))
        return carry

    lax.fori_loop(0, 4, conv_shared, 0)

    spread_forward(x_rows, xr, 0)
    spread_start(z_in, z_rows, zr, 6)
    local[3].wait()
    spread_wait(x_rows, 0)

    def conv_own(p, carry):
        def tile(i, inner):
            lanes = pl.ds(pl.multiple_of(i * 128, 128), 128)
            xc[p, :, lanes] = convolved(x_ext, p, lanes, lanes)
            return inner

        return lax.fori_loop(0, 10, tile, carry)

    lax.fori_loop(0, 4, conv_own, 0)

    state[...] = jnp.zeros((STATE, WIDTH), F32)
    log_dec[...] = jnp.zeros((4, 8, 128), F32)

    def advance(p, total):
        cum_now = cum[p]
        last = cum_now[127:128, :]
        weight = widen(step[p] * jnp.exp(last - cum_now))
        scaled = (xc[p].astype(F32) * weight).astype(BF16)
        fresh = dot(bcc[p, :, 0:128], scaled, TN)
        kept = widen(jnp.broadcast_to(jnp.exp(last), (8, 128)))[0:1, :]
        blocks[p] = state[...]
        state[...] = kept * state[...] + fresh
        log_dec[p] = jnp.broadcast_to(total, (8, 128))
        return total + last

    total = lax.fori_loop(0, 4, advance, jnp.zeros((1, 128), F32))
    dec_all[c] = jnp.broadcast_to(jnp.exp(total), (8, 128))

    def pack_state(i, carry):
        st_send[i] = state[pl.ds(pl.multiple_of(i * 8, 8), 8), :].astype(BF16)
        return carry

    lax.fori_loop(0, 16, pack_state, 0)
    st_recv[c] = st_send[c]

    def state_copy(j):
        return pltpu.make_async_remote_copy(
            src_ref=st_send.at[lax.rem(c + j, 16)], dst_ref=st_recv.at[c],
            send_sem=sc.at[j], recv_sem=rc_.at[j], device_id=context_peer(j), device_id_type=MESH)

    def decay_copy(j):
        return pltpu.make_async_remote_copy(
            src_ref=dec_all.at[c], dst_ref=dec_all.at[c],
            send_sem=sd.at[j], recv_sem=rd.at[j], device_id=context_peer(j), device_id_type=MESH)

    exchange(decay_copy)
    exchange(state_copy)

    arrived(w_part(mine, 320, down_y), 32)
    send(w_part(mine, 320, down_y), w_part(mine, 320, down_y), 36, {"fsdp": up_y})
    arrived(w_part(mine + 320, 320, up_y), 33)
    send(w_part(mine + 320, 320, up_y), w_part(mine + 320, 320, up_y), 37, {"fsdp": down_y})
    spread_forward(z_rows, zr, 6)

    def inside(p, carry):
        b_now, c_now = bcc[p, :, 0:128], bcc[p, :, 128:256]
        gram = dot(c_now, b_now, NT)
        cum_now = cum[p]
        shifted = (cum_now - jnp.log(step[p])).T
        lane = lax.broadcasted_iota(jnp.int32, (1, 128), 1)
        low = jnp.where(lane < 64, 1.0, 0.0)
        for q in range(HEADS // 2):
            mats = []
            for h in (2 * q, 2 * q + 1):
                gap = cum_now[:, h : h + 1] - shifted[h : h + 1, :]
                mats.append(jnp.exp(jnp.where(causal, gap, -1e30)) * gram)
            both = jnp.concatenate(mats, axis=1).astype(BF16)
            x_pair = xc[p, :, pl.ds(q * 128, 128)].astype(F32)
            x_two = jnp.concatenate([x_pair * low, x_pair * (1.0 - low)], axis=0).astype(BF16)
            y_in[p, :, pl.ds(q * 128, 128)] = dot(both, x_two) + x_pair * par[6:7, pl.ds(q * 128, 128)]
        return carry

    lax.fori_loop(0, 4, inside, 0)

    settle(decay_copy)
    dec_wide[...] = widen(dec_all[...].reshape(128, 128))
    settle(state_copy)

    def chain(i, held):
        back_send[i] = held.astype(BF16)
        return dec_wide[pl.ds(pl.multiple_of(i * 8, 8), 8), :] * held + st_recv[i].astype(F32)

    lax.fori_loop(0, 16, chain, jnp.zeros((8, WIDTH), F32))
    back_recv[c] = back_send[c]

    def back_copy(j):
        return pltpu.make_async_remote_copy(
            src_ref=back_send.at[lax.rem(c + j, 16)], dst_ref=back_recv.at[c],
            send_sem=sb.at[j], recv_sem=rb.at[j], device_id=context_peer(j), device_id_type=MESH)

    exchange(back_copy)

    core = {"context_1": 1 - k}
    arrived(w_part(mine + 320, 320, down_y), 34)
    send(w_part(mine, 640, down_y), w_part(mine, 640, down_y), 38, core)
    arrived(w_part(mine, 320, up_y), 35)
    send(w_part(mine, 640, up_y), w_part(mine, 640, up_y), 39, core)
    far_y = lax.rem(s + 2, 4)
    arrived(w_part(mine, 320, far_y), 36)
    arrived(w_part(mine + 320, 320, far_y), 37)
    send(w_part(mine, 640, far_y), w_part(mine, 640, far_y), 40, core)

    local[4].wait()
    spread_wait(z_rows, 6)

    settle(back_copy)

    def unpack_state(i, carry):
        state[pl.ds(pl.multiple_of(i * 8, 8), 8), :] = back_recv[i].astype(F32)
        return carry

    lax.fori_loop(0, 16, unpack_state, 0)

    def finish(p, carry):
        start = blocks[p] + widen(jnp.exp(log_dec[p]))[0:1, :] * state[...]
        reach = widen(jnp.exp(cum[p]))
        y_now = y_in[p] + reach * dot(bcc[p, :, 128:256], start.astype(BF16))
        now = y_now * silu(gate[p].astype(F32))
        squares = (now * now).astype(BF16)
        sq[t, p] = dot(jnp.ones((8, WIDTH), BF16), squares, NT)
        out = (now * par[5:6, 0:WIDTH]).astype(BF16)
        gated[p] = out
        ap_send[p] = dot(down_t[...], out, NT)
        return carry

    lax.fori_loop(0, 4, finish, 0)
    ap_recv[t] = ap_send[t]
    for j in range(1, 4):
        peer = lax.rem(t + j, 4)
        send(sq.at[t], sq.at[t], 21 + j, {"tensor": peer})
        send(ap_send.at[peer], ap_recv.at[t], 24 + j, {"tensor": peer})

    local[5].wait()
    arrived(w_part(other, 640, down_y), 38)
    arrived(w_part(other, 640, up_y), 39)
    arrived(w_part(other, 640, far_y), 40)

    def project(p, half, store):
        def piece(i, carry):
            lanes = pl.ds(pl.multiple_of(i * 256, 256), 256)
            lanes_w = pl.ds(pl.multiple_of(half * HALF + i * 256, 256), 256)
            store(lanes, dot(gated[p], wt[:, lanes_w]))
            return carry

        lax.fori_loop(0, 5, piece, 0)

    def to_slot(slot, extra=None):
        def store(lanes, v):
            if extra is not None:
                v = v + rs_recv[extra, :, lanes].astype(F32)
            rs_send[slot, :, lanes] = v.astype(BF16)

        return store

    project(far, 0, to_slot(0))
    send(rs_send.at[0], rs_recv.at[0], 41, {"tensor": right})
    project(far, 1, to_slot(1))
    send(rs_send.at[1], rs_recv.at[1], 42, {"tensor": left})
    project(right, 1, to_slot(2))
    send(rs_send.at[2], rs_recv.at[2], 43, {"tensor": right})
    project(left, 0, to_slot(3))
    send(rs_send.at[3], rs_recv.at[3], 44, {"tensor": left})

    for j in range(1, 4):
        source = lax.rem(t + 4 - j, 4)
        arrived(gt.at[source], 18 + j)
        arrived(sq.at[source], 21 + j)
        arrived(ap_recv.at[source], 24 + j)

    def row_scale(p):
        squares = (sq[0, p] + sq[1, p]) + (sq[2, p] + sq[3, p])
        return lax.rsqrt(squares * (1.0 / 5120.0) + EPS)

    adapter = ((ap_recv[0] + ap_recv[1]) + (ap_recv[2] + ap_recv[3])).astype(BF16)
    own_scale = row_scale(t)
    weighted = (scale * own_scale[0:1, :] * adapter.astype(F32)).astype(BF16)
    grad_a_now = jnp.zeros((RANK, WIDTH), F32)
    for p in range(4):
        rows_grad = (row_scale(p)[0:1, :] * gt[p]).astype(BF16)
        grad_a_now = grad_a_now + dot(rows_grad, gated[p])
    grad_b_now = dot(weighted, cot[...])
    for i in range(30):
        v_send[i // 2, i % 2] = (
            grad_a_now[:, i * 128 : i * 128 + 128] if i < 10
            else grad_b_now[:, (i - 10) * 128 : (i - 10) * 128 + 128])
    v_send[15] = jnp.zeros((2, RANK, 128), F32)
    v_recv[c] = v_send[c]

    def v_copy(j):
        return pltpu.make_async_remote_copy(
            src_ref=v_send.at[lax.rem(c + j, 16)], dst_ref=v_recv.at[c],
            send_sem=sv.at[j], recv_sem=rv.at[j], device_id=context_peer(j), device_id_type=MESH)

    exchange(v_copy)

    arrived(rs_recv.at[0], 41)
    project(right, 0, to_slot(4, 0))
    send(rs_send.at[4], rs_recv.at[4], 45, {"tensor": right})
    arrived(rs_recv.at[1], 42)
    project(left, 1, to_slot(5, 1))
    send(rs_send.at[5], rs_recv.at[5], 46, {"tensor": left})

    settle(v_copy)

    def add_v(i, held):
        return held + v_recv[i]

    me = 4 * t + s
    xy_recv[me] = lax.fori_loop(1, 16, add_v, v_recv[0])

    def xy_copy(j):
        return pltpu.make_async_remote_copy(
            src_ref=xy_recv.at[me], dst_ref=xy_recv.at[me],
            send_sem=sxy.at[j], recv_sem=rxy.at[j], device_id=plane_peer(j), device_id_type=MESH)

    exchange(xy_copy)

    def own_part(half):
        def store(lanes, v):
            lanes_up = pl.ds(pl.multiple_of(half * HALF + lanes.start, 256), 256)
            own[half, :, lanes] = v + 2.0 * dot(adapter, up[:, lanes_up], TN)

        return store

    project(t, 0, own_part(0))
    project(t, 1, own_part(1))

    settle(xy_copy)

    def add_xy(i, held):
        keep = jnp.where(jnp.logical_or(c >= 5, lax.div(i, 4) == t), 1.0, 0.0)
        return held + keep * xy_recv[i]

    v_all[c] = lax.fori_loop(0, 16, add_xy, jnp.zeros((2, RANK, 128), F32))

    def all_copy(j):
        return pltpu.make_async_remote_copy(
            src_ref=v_all.at[c], dst_ref=v_all.at[c],
            send_sem=sg.at[j], recv_sem=rg.at[j], device_id=context_peer(j), device_id_type=MESH)

    exchange(all_copy)

    arrived(rs_recv.at[2], 43)
    arrived(rs_recv.at[3], 44)
    arrived(rs_recv.at[4], 45)
    arrived(rs_recv.at[5], 46)
    scale_col = jnp.broadcast_to(own_scale[0:1, :], (128, 128)).T

    def close(i, carry):
        lanes = pl.ds(pl.multiple_of(i * 128, 128), 128)
        first = own[0, :, lanes] + rs_recv[4, :, lanes].astype(F32) + rs_recv[3, :, lanes].astype(F32)
        second = own[1, :, lanes] + rs_recv[2, :, lanes].astype(F32) + rs_recv[5, :, lanes].astype(F32)
        mixed[:, lanes] = (scale_col * first).astype(BF16)
        mixed[:, pl.ds(pl.multiple_of(HALF + i * 128, 128), 128)] = (scale_col * second).astype(BF16)
        return carry

    lax.fori_loop(0, 10, close, 0)

    settle(all_copy)
    for i in range(10):
        grad_a[:, i * 128 : i * 128 + 128] = v_all[i // 2, i % 2]
    for i in range(20):
        grad_b[:, i * 128 : i * 128 + 128] = v_all[5 + i // 2, i % 2]

    for make in (decay_copy, state_copy, back_copy, v_copy, xy_copy, all_copy):
        settle(make, received=False)
    for copy in started:
        copy.wait_send()

    @pl.when(gives_rim)
    def _():
        for copy in rim_copies():
            copy.wait_send()


def shards(
    input_raw, state_proj_raw, gate_branch, step_raw, convolution_taps, convolution_bias, step_bias,
    decay_log_rate, skip_weight, gated_norm_gain, output_weight, adapter_down, adapter_up, cotangent,
):
    first = lax.axis_index("tensor") * WIDTH
    conv = jnp.concatenate([convolution_taps, convolution_bias[None, :]], axis=0)
    conv = jnp.concatenate(
        [lax.dynamic_slice_in_dim(conv, first, WIDTH, 1), conv[:, 4 * WIDTH :]], axis=1)

    def line(v):
        return jnp.pad(v, (0, WIDTH + 256 - v.shape[0]))[None, :]

    par = jnp.concatenate(
        [conv, line(gated_norm_gain), line(jnp.repeat(skip_weight, 64)), line(step_bias),
         line(decay_log_rate), jnp.zeros((7, WIDTH + 256), F32)], axis=0)
    hbm = pl.BlockSpec(memory_space=pl.ANY)
    vmem = pl.BlockSpec(memory_space=pltpu.VMEM)
    dma = pltpu.SemaphoreType.DMA
    mixed, grad_a, grad_b = pl.pallas_call(
        kernel,
        out_shape=(
            jax.ShapeDtypeStruct((ROWS, OUT), BF16),
            jax.ShapeDtypeStruct((RANK, WIDTH), F32),
            jax.ShapeDtypeStruct((RANK, OUT), F32),
        ),
        in_specs=[hbm] * 6 + [vmem] * 3,
        out_specs=(vmem, vmem, vmem),
        scratch_shapes=[
            pltpu.VMEM((16 + 512, WIDTH), BF16),
            pltpu.VMEM((2, 64, WIDTH), BF16),
            pltpu.VMEM((4, ROWS, WIDTH), BF16),
            pltpu.VMEM((16 + 512, 256), BF16),
            pltpu.VMEM((4, ROWS, 256), BF16),
            pltpu.VMEM((4, ROWS, 80), BF16),
            pltpu.VMEM((4, ROWS, WIDTH), BF16),
            pltpu.VMEM((2, 64, WIDTH), BF16),
            pltpu.VMEM((WIDTH, OUT), BF16),
            pltpu.VMEM((ROWS, OUT), BF16),
            pltpu.VMEM((256, WIDTH), BF16),
            pltpu.VMEM((4, ROWS, 128), F32),
            pltpu.VMEM((4, ROWS, 128), F32),
            pltpu.VMEM((4, 8, 128), F32),
            pltpu.VMEM((4, ROWS, WIDTH), F32),
            pltpu.VMEM((4, STATE, WIDTH), F32),
            pltpu.VMEM((STATE, WIDTH), F32),
            pltpu.VMEM((16, 8, WIDTH), BF16),
            pltpu.VMEM((16, 8, WIDTH), BF16),
            pltpu.VMEM((16, 8, 128), F32),
            pltpu.VMEM((128, WIDTH), F32),
            pltpu.VMEM((16, 8, WIDTH), BF16),
            pltpu.VMEM((16, 8, WIDTH), BF16),
            pltpu.VMEM((4, ROWS, WIDTH), BF16),
            pltpu.VMEM((4, RANK, 128), F32),
            pltpu.VMEM((4, 4, 8, 128), F32),
            pltpu.VMEM((4, RANK, 128), F32),
            pltpu.VMEM((4, RANK, 128), F32),
            pltpu.VMEM((6, ROWS, HALF), BF16),
            pltpu.VMEM((6, ROWS, HALF), BF16),
            pltpu.VMEM((2, ROWS, HALF), F32),
            pltpu.VMEM((16, 2, RANK, 128), F32),
            pltpu.VMEM((16, 2, RANK, 128), F32),
            pltpu.VMEM((16, 2, RANK, 128), F32),
            pltpu.VMEM((16, 2, RANK, 128), F32),
            dma((48,)), dma((48,)), dma((24,)),
            dma((16,)), dma((16,)), dma((16,)), dma((16,)), dma((16,)), dma((16,)),
            dma((16,)), dma((16,)), dma((16,)), dma((16,)), dma((16,)), dma((16,)),
        ],
        compiler_params=pltpu.CompilerParams(
            collective_id=0, has_side_effects=True, vmem_limit_bytes=64 * 1000 * 1000),
    )(
        input_raw[0], state_proj_raw[0], gate_branch[0], step_raw[0], output_weight, cotangent[0],
        par, adapter_down.T, adapter_up,
    )
    return (mixed[None], grad_a.T, grad_b)


def solution(mesh):
    torus = Mesh(
        mesh.devices.reshape(8, 2, mesh.shape["tensor"], mesh.shape["fsdp"]),
        ("context_0", "context_1", "tensor", "fsdp"),
    )
    tokens = P("fsdp", CONTEXT_TENSOR, None)
    return jax.shard_map(
        shards,
        mesh=torus,
        in_specs=(
            tokens, tokens, tokens, tokens, P(), P(), P("tensor"), P("tensor"), P("tensor"), P("tensor"),
            P("tensor", "fsdp"), P("tensor", None), P(), tokens,
        ),
        out_specs=(tokens, P("tensor", None), P()),
        check_vma=False,
    )
```

```python
import functools

import jax
import jax.numpy as jnp
from jax import lax
from jax.experimental import pallas as pl
from jax.experimental.pallas import tpu as pltpu
from jax.sharding import Mesh
from jax.sharding import PartitionSpec as P

MESH = pl.DeviceIdType.MESH
CONTEXT_TENSOR = ("context_0", "context_1", "tensor")
F32 = jnp.float32
BF16 = jnp.bfloat16

ROWS = 128
WIDTH = 1280
STATE = 128
OUT = 2560
HALF = 1280
RANK = 16
HEADS = 20
COLS = 640
TOKENS = 32768
EPS = 1e-05

NT = (((1,), (1,)), ((), ()))
TN = (((0,), (0,)), ((), ()))


def silu(v):
    half = 0.5 * v
    return half + half * jnp.tanh(half)


def dot(a, b, dims=(((1,), (0,)), ((), ())), precision=None):
    return lax.dot_general(a, b, dims, precision=precision, preferred_element_type=F32)


def kernel(
    x_in, bc_in, z_in, dt_in, w_in, cot_in, taps_in, bias_in, step_bias_in, rate_in, skip_in, gain_in, down_in, up_in,
    mixed, grad_a, grad_b,
    x_ext, xr, xc, bc_ext, bcc, dt_all, gate, zr, wt, cot,
    taps_x, taps_bc, bias_x, bias_bc, head_par, gain, down_t, up, skip,
    spread, step, cum, log_start, log_tail, y_in, blocks, kept, state, peer_state,
    st_send, st_recv, dec_all, dec_wide, back_send, back_recv, in_send, in_recv, s_in,
    gated, gt, sq, ap_send, ap_recv,
    rs_send, rs_recv, own,
    v_send, v_recv, y_recv, t_recv, v_all,
    sx, rx, sl, sc, rc_, sd, rd, sb, rb, sv, rv, sg, rg,
):
    z, k = lax.axis_index("context_0"), lax.axis_index("context_1")
    t, s = lax.axis_index("tensor"), lax.axis_index("fsdp")
    c = 2 * z + k
    right, left, far = lax.rem(t + 1, 4), lax.rem(t + 3, 4), lax.rem(t + 2, 4)
    up_y, down_y, far_y = lax.rem(s + 1, 4), lax.rem(s + 3, 4), lax.rem(s + 2, 4)
    started = []
    slots = {}

    def slot(name):
        return slots.setdefault(name, len(slots))

    def remote(src, dst, name, where):
        return pltpu.make_async_remote_copy(
            src_ref=src, dst_ref=dst, send_sem=sx.at[slot(name)], recv_sem=rx.at[slot(name)],
            device_id=where, device_id_type=MESH,
        )

    def send(src, dst, name, where):
        copy = remote(src, dst, name, where)
        copy.start()
        started.append(copy)

    def arrived(dst, name):
        remote(dst, dst, name, {"tensor": right}).wait_recv()

    def context_peer(j):
        target = lax.rem(c + j, 16)
        return {"context_0": lax.div(target, 2), "context_1": lax.rem(target, 2)}

    def chip_peer(j):
        return {"context_0": lax.rem(z + j, 8)}

    def exchange(make, how_many=16):
        def go(j, carry):
            make(j).start()
            return carry

        lax.fori_loop(1, how_many, go, 0)

    def settle(make, how_many=16, received=True):
        def go(j, carry):
            if received:
                make(j).wait_recv()
            else:
                make(j).wait_send()
            return carry

        lax.fori_loop(1, how_many, go, 0)

    def tile(i):
        return pl.ds(pl.multiple_of(i * 128, 128), 128)

    barrier = pltpu.get_barrier_semaphore()

    def greet(j, carry):
        pl.semaphore_signal(barrier, inc=1, device_id=context_peer(j), device_id_type=MESH)
        return carry

    for j in range(1, 4):
        pl.semaphore_signal(barrier, inc=1, device_id={"tensor": lax.rem(t + j, 4)}, device_id_type=MESH)
        pl.semaphore_signal(barrier, inc=1, device_id={"fsdp": lax.rem(s + j, 4)}, device_id_type=MESH)
    lax.fori_loop(1, 16, greet, 0)
    before = lax.rem(c + 15, 16)
    after = lax.rem(c + 1, 16)

    @pl.when(c > 0)
    def _():
        pl.semaphore_signal(
            barrier, inc=1,
            device_id={"context_0": lax.div(before, 2), "context_1": lax.rem(before, 2), "tensor": 3},
            device_id_type=MESH,
        )

    def columns(p):
        return pl.ds(pl.multiple_of(p * WIDTH, WIDTH), WIDTH)

    def x_rows(p, first, count):
        return x_ext.at[pl.ds(pl.multiple_of(16 + p * ROWS + first, 16), count)]

    def z_rows(p, first, count):
        return gate.at[p, pl.ds(first, count)]

    def bc_rows(p, first, count):
        return bc_ext.at[pl.ds(pl.multiple_of(16 + p * ROWS + first, 16), count)]

    def w_part(rows_from, count, y):
        return wt.at[
            pl.ds(pl.multiple_of(rows_from, 64), count), pl.ds(pl.multiple_of(y * COLS, COLS), COLS)
        ]

    def dt_window(p):
        return dt_in.at[pl.ds(pl.multiple_of(8 * lax.div(5 * p, 2), 8), 24)]

    local = {}

    def copy_here(name, src, dst):
        local[name] = pltpu.make_async_copy(src, dst, sl.at[len(local)])
        local[name].start()

    copy_here("cot", cot_in, cot)
    copy_here("up", up_in, up)
    copy_here("step_bias", step_bias_in, head_par.at[0])
    copy_here("rate", rate_in, head_par.at[1])
    copy_here("skip", skip_in, head_par.at[2])
    copy_here("bc", bc_in, bc_rows(t, 0, ROWS))
    copy_here("dt", dt_window(t), dt_all.at[t])
    copy_here("taps_x", taps_in.at[:, columns(t)], taps_x)
    copy_here("taps_bc", taps_in.at[:, pl.ds(4 * WIDTH, 256)], taps_bc)
    copy_here("bias_x", bias_in.at[:, columns(t)], bias_x)
    copy_here("bias_bc", bias_in.at[:, pl.ds(4 * WIDTH, 256)], bias_bc)
    copy_here("x", x_in.at[:, columns(t)], x_rows(t, 0, ROWS))
    copy_here("gain", gain_in, gain)
    copy_here("down", down_in, down_t)
    copy_here("gate", z_in.at[:, columns(t)], gate.at[t])
    copy_here("w", w_in, w_part(0, 1280, s))

    def head_mask(i, carry):
        head = lax.broadcasted_iota(jnp.int32, (256, 128), 0)
        head = jnp.where(head >= 128, head - 128, head)
        lane = lax.broadcasted_iota(jnp.int32, (256, 128), 1)
        own_head = 2 * i + jnp.where(lane >= 64, 1, 0)
        spread[:, tile(i)] = jnp.where(head == own_head, 1.0, 0.0).astype(BF16)
        return carry

    lax.fori_loop(0, 10, head_mask, 0)

    def widen(v):
        high = v.astype(BF16)
        low = (v - high.astype(F32)).astype(BF16)
        return dot(jnp.concatenate([high, low], axis=1), spread[...])

    scale = 2.0 / (TOKENS ** 0.5)

    local["cot"].wait()
    local["up"].wait()
    gt[t] = dot(up[...], cot[...], NT) * scale

    gives_rim = jnp.logical_and(t == 3, c < 15)

    @pl.when(gives_rim)
    def _():
        pl.semaphore_wait(barrier, 25)

    @pl.when(jnp.logical_not(gives_rim))
    def _():
        pl.semaphore_wait(barrier, 21)

    def far_start(src, relay, name):
        send(src.at[pl.ds(0, 64), columns(far)], relay.at[0], name + "0", {"tensor": right})
        send(src.at[pl.ds(64, 64), columns(far)], relay.at[1], name + "1", {"tensor": left})

    def near_start(src, rows, name):
        send(src.at[:, columns(right)], rows(t, 0, ROWS), name + "2", {"tensor": right})
        send(src.at[:, columns(left)], rows(t, 0, ROWS), name + "3", {"tensor": left})

    def far_forward(rows, relay, name):
        arrived(relay.at[0], name + "0")
        send(relay.at[0], rows(left, 0, 64), name + "4", {"tensor": right})
        arrived(relay.at[1], name + "1")
        send(relay.at[1], rows(right, 64, 64), name + "5", {"tensor": left})

    def near_wait(rows, name):
        arrived(rows(left, 0, ROWS), name + "2")
        arrived(rows(right, 0, ROWS), name + "3")

    def far_wait(rows, name):
        arrived(rows(far, 0, 64), name + "4")
        arrived(rows(far, 64, 64), name + "5")

    far_start(x_in, xr, "x")
    send(bc_in.at[pl.ds(0, 64)], bc_rows(t, 0, 64), "b0", {"tensor": right})
    send(bc_in.at[pl.ds(64, 64)], bc_rows(t, 64, 64), "b1", {"tensor": left})
    send(bc_in.at[pl.ds(64, 64)], bc_rows(t, 64, 64), "b2", {"tensor": right})
    send(bc_in.at[pl.ds(0, 64)], bc_rows(t, 0, 64), "b3", {"tensor": left})
    for j in (1, 3, 2):
        peer = lax.rem(t + j, 4)
        send(dt_window(peer), dt_all.at[t], "dt%d" % j, {"tensor": peer})
    near_start(x_in, x_rows, "x")

    def rim_copies():
        copies = []
        for p in range(4):
            where = {"context_0": lax.div(after, 2), "context_1": lax.rem(after, 2), "tensor": p}
            copies.append(pltpu.make_async_remote_copy(
                src_ref=x_in.at[pl.ds(112, 16), pl.ds(p * WIDTH, WIDTH)], dst_ref=x_ext.at[pl.ds(0, 16)],
                send_sem=sl.at[16 + p], recv_sem=rx.at[slot("rim_x")], device_id=where, device_id_type=MESH))
            copies.append(pltpu.make_async_remote_copy(
                src_ref=bc_in.at[pl.ds(112, 16)], dst_ref=bc_ext.at[pl.ds(0, 16)],
                send_sem=sl.at[20 + p], recv_sem=rx.at[slot("rim_b")], device_id=where, device_id_type=MESH))
        return copies

    @pl.when(gives_rim)
    def _():
        for copy in rim_copies():
            copy.start()

    @pl.when(c == 0)
    def _():
        x_ext[0:16, :] = jnp.zeros((16, WIDTH), BF16)
        bc_ext[0:16, :] = jnp.zeros((16, 256), BF16)

    mine, other = k * 640, (1 - k) * 640

    def w_src(first):
        return w_in.at[pl.ds(pl.multiple_of(mine + first, 64), 320)]

    send(w_src(0), w_part(mine, 320, s), "w0", {"fsdp": up_y})
    send(w_src(320), w_part(mine + 320, 320, s), "w1", {"fsdp": down_y})
    send(w_src(320), w_part(mine + 320, 320, s), "w2", {"fsdp": up_y})
    send(w_src(0), w_part(mine, 320, s), "w3", {"fsdp": down_y})

    for name in ("step_bias", "rate", "skip", "bc", "dt", "taps_x", "taps_bc", "bias_x", "bias_bc", "x", "gain", "down"):
        local[name].wait()
    pick20 = jnp.where(
        lax.broadcasted_iota(jnp.int32, (HEADS, 128), 0) == lax.broadcasted_iota(jnp.int32, (HEADS, 128), 1), 1.0, 0.0)

    def head_row(i):
        return dot(jnp.broadcast_to(head_par[i], (8, HEADS)), pick20, precision=lax.Precision.HIGHEST)

    step_bias = head_row(0)[0:1, :]
    rate = jnp.exp(head_row(1))[0:1, :]
    skip[...] = widen(head_row(2))

    for j in range(1, 4):
        arrived(dt_all.at[lax.rem(t + 4 - j, 4)], "dt%d" % j)

    row = lax.broadcasted_iota(jnp.int32, (128, 128), 0)
    col = lax.broadcasted_iota(jnp.int32, (128, 128), 1)
    causal = row >= col
    tri = jnp.where(causal, 1.0, 0.0)
    pick_row = lax.broadcasted_iota(jnp.int32, (24, 128), 0)
    pick_col = lax.broadcasted_iota(jnp.int32, (24, 128), 1)
    hit = jnp.logical_and(pick_row == pick_col + 4 * lax.rem(t, 2), pick_col < HEADS)
    pick = jnp.where(hit, 1.0, 0.0).astype(BF16)

    total = jnp.zeros((1, 128), F32)
    for p in range(4):
        raw = dot(dt_all[p], pick, TN) + step_bias
        step_now = jnp.maximum(raw, 0.0) + jnp.log1p(jnp.exp(-jnp.abs(raw)))
        cum_now = dot(tri, -step_now * rate, precision=lax.Precision.HIGHEST)
        step[p] = step_now
        cum[p] = cum_now
        log_start[p] = jnp.broadcast_to(total, (8, 128))
        total = total + cum_now[127:128, :]
    for p in range(4):
        log_tail[p] = total - log_start[p] - cum[p, 127:128, :]
        kept[p] = widen(jnp.broadcast_to(jnp.exp(cum[p, 127:128, :]), (8, 128)))
    dec_all[c] = jnp.broadcast_to(jnp.exp(total), (8, 128))

    arrived(bc_rows(left, 0, 64), "b0")
    send(bc_rows(left, 0, 64), bc_rows(left, 0, 64), "b4", {"tensor": right})
    arrived(bc_rows(right, 64, 64), "b1")
    send(bc_rows(right, 64, 64), bc_rows(right, 64, 64), "b5", {"tensor": left})
    far_forward(x_rows, xr, "x")
    far_start(z_in, zr, "z")
    near_start(z_in, z_rows, "z")

    def decay_copy(j):
        return pltpu.make_async_remote_copy(
            src_ref=dec_all.at[c], dst_ref=dec_all.at[c],
            send_sem=sd.at[j], recv_sem=rd.at[j], device_id=context_peer(j), device_id_type=MESH)

    exchange(decay_copy)
    for j in range(1, 4):
        send(gt.at[t], gt.at[t], "g%d" % j, {"tensor": lax.rem(t + j, 4)})

    def convolved(ext, p, lanes, taps, bias):
        v = ext[pl.ds(pl.multiple_of(p * ROWS, 16), ROWS + 16), lanes].astype(F32)
        acc = bias[:, lanes] + taps[0:1, lanes] * pltpu.roll(v, 3, 0)
        acc = acc + taps[1:2, lanes] * pltpu.roll(v, 2, 0)
        acc = acc + taps[2:3, lanes] * pltpu.roll(v, 1, 0)
        acc = acc + taps[3:4, lanes] * v
        return silu(acc[16:]).astype(BF16)

    @pl.when(c > 0)
    def _():
        arrived(x_ext.at[pl.ds(0, 16)], "rim_x")
        arrived(bc_ext.at[pl.ds(0, 16)], "rim_b")

    state[...] = jnp.zeros((STATE, WIDTH), F32)

    def block(i, carry):
        p = lax.rem(t + i, 4)
        for half in range(2):
            bcc[p, :, pl.ds(half * 128, 128)] = convolved(bc_ext, p, pl.ds(half * 128, 128), taps_bc, bias_bc)

        def lanes_of(j, inner):
            xc[p, :, tile(j)] = convolved(x_ext, p, tile(j), taps_x, bias_x)
            return inner

        lax.fori_loop(0, 10, lanes_of, 0)
        cum_now = cum[p]
        weight = widen(step[p] * jnp.exp(cum_now[127:128, :] - cum_now))
        scaled = (xc[p].astype(F32) * weight).astype(BF16)
        fresh = dot(bcc[p, :, 0:128], scaled, TN)
        blocks[p] = fresh
        state[...] = state[...] + widen(jnp.exp(log_tail[p]))[0:1, :] * fresh
        return carry

    arrived(bc_rows(left, 64, 64), "b2")
    arrived(bc_rows(right, 0, 64), "b3")
    near_wait(x_rows, "x")
    lax.fori_loop(0, 2, block, 0)
    arrived(bc_rows(far, 0, 64), "b4")
    arrived(bc_rows(far, 64, 64), "b5")
    far_wait(x_rows, "x")
    lax.fori_loop(2, 4, block, 0)

    core = {"context_1": 1 - k}

    def half_lanes(i):
        return pl.ds(pl.multiple_of(i * 640, 640), 640)

    send(state.at[:, half_lanes(1 - k)], peer_state, "pair", core)
    settle(decay_copy)
    dec_wide[...] = widen(dec_all[...].reshape(128, 128))
    arrived(peer_state, "pair")

    def chip_decay(of):
        return dec_wide[pl.ds(pl.multiple_of(16 * of, 16), 8), half_lanes(k)] * dec_wide[
            pl.ds(pl.multiple_of(16 * of + 8, 8), 8), half_lanes(k)]

    decay_second = dec_wide[pl.ds(pl.multiple_of(16 * z + 8, 8), 8), half_lanes(k)][0:1, :]
    weight_mine = jnp.where(k == 0, decay_second, jnp.ones_like(decay_second))
    weight_peer = jnp.where(k == 0, jnp.ones_like(decay_second), decay_second)

    def pack_state(i, carry):
        rows = pl.ds(pl.multiple_of(i * 16, 16), 16)
        both = weight_mine * state[rows, half_lanes(k)] + weight_peer * peer_state[rows, :]
        st_send[i] = both.astype(BF16)
        return carry

    lax.fori_loop(0, 8, pack_state, 0)

    def state_copy(j):
        return pltpu.make_async_remote_copy(
            src_ref=st_send.at[lax.rem(z + j, 8)], dst_ref=st_recv.at[z],
            send_sem=sc.at[j], recv_sem=rc_.at[j], device_id=chip_peer(j), device_id_type=MESH)

    exchange(state_copy, 8)
    st_recv[z] = st_send[z]

    arrived(w_part(mine, 320, down_y), "w0")
    send(w_part(mine, 320, down_y), w_part(mine, 320, down_y), "w4", {"fsdp": up_y})
    arrived(w_part(mine + 320, 320, up_y), "w1")
    send(w_part(mine + 320, 320, up_y), w_part(mine + 320, 320, up_y), "w5", {"fsdp": down_y})
    far_forward(z_rows, zr, "z")

    def inside(p, carry):
        b_now, c_now = bcc[p, :, 0:128], bcc[p, :, 128:256]
        gram = dot(c_now, b_now, NT)
        cum_now = cum[p]
        shifted = (cum_now - jnp.log(step[p])).T
        lane = lax.broadcasted_iota(jnp.int32, (1, 128), 1)
        low = jnp.where(lane < 64, 1.0, 0.0)
        for q in range(HEADS // 2):
            mats = []
            for h in (2 * q, 2 * q + 1):
                gap = cum_now[:, h : h + 1] - shifted[h : h + 1, :]
                mats.append(jnp.exp(jnp.where(causal, gap, -1e30)) * gram)
            both = jnp.concatenate(mats, axis=1).astype(BF16)
            x_pair = xc[p, :, pl.ds(q * 128, 128)].astype(F32)
            x_two = jnp.concatenate([x_pair * low, x_pair * (1.0 - low)], axis=0).astype(BF16)
            y_in[p, :, pl.ds(q * 128, 128)] = dot(both, x_two) + x_pair * skip[0:1, pl.ds(q * 128, 128)]
        return carry

    lax.fori_loop(0, 4, inside, 0)

    settle(state_copy, 8)

    def chain(i, held):
        back_send[i] = held.astype(BF16)
        return chip_decay(i)[0:1, :] * held + st_recv[i].astype(F32)

    lax.fori_loop(0, 8, chain, jnp.zeros((16, 640), F32))

    def back_copy(j):
        return pltpu.make_async_remote_copy(
            src_ref=back_send.at[lax.rem(z + j, 8)], dst_ref=back_recv.at[z],
            send_sem=sb.at[j], recv_sem=rb.at[j], device_id=chip_peer(j), device_id_type=MESH)

    exchange(back_copy, 8)
    back_recv[z] = back_send[z]

    def starts(j, carry):
        held = jnp.zeros((STATE, 128), F32)
        for p in range(4):
            fresh = blocks[p, :, tile(j)]
            blocks[p, :, tile(j)] = held
            held = kept[p, 0:1, tile(j)] * held + fresh
        return carry

    lax.fori_loop(0, 10, starts, 0)

    arrived(w_part(mine + 320, 320, down_y), "w2")
    send(w_part(mine, 640, down_y), w_part(mine, 640, down_y), "w6", core)
    arrived(w_part(mine, 320, up_y), "w3")
    send(w_part(mine, 640, up_y), w_part(mine, 640, up_y), "w7", core)
    arrived(w_part(mine, 320, far_y), "w4")
    arrived(w_part(mine + 320, 320, far_y), "w5")
    send(w_part(mine, 640, far_y), w_part(mine, 640, far_y), "w8", core)

    local["gate"].wait()
    near_wait(z_rows, "z")
    far_wait(z_rows, "z")
    settle(back_copy, 8)

    decay_first = dec_wide[pl.ds(pl.multiple_of(16 * z, 8), 8), half_lanes(k)][0:1, :]

    def unpack_state(i, carry):
        rows = pl.ds(pl.multiple_of(i * 16, 16), 16)
        first = back_recv[i].astype(F32)
        span = jnp.where(k == 0, state[rows, half_lanes(k)], peer_state[rows, :])
        second = decay_first * first + span
        s_in[rows, half_lanes(k)] = jnp.where(k == 0, first, second)
        in_send[rows, :] = jnp.where(k == 0, second, first).astype(BF16)
        return carry

    lax.fori_loop(0, 8, unpack_state, 0)
    send(in_send, in_recv, "in", core)

    local["w"].wait()
    arrived(w_part(other, 640, down_y), "w6")
    arrived(w_part(other, 640, up_y), "w7")
    arrived(w_part(other, 640, far_y), "w8")
    arrived(in_recv, "in")
    s_in[:, half_lanes(1 - k)] = in_recv[...].astype(F32)

    def finish(i, carry):
        p = lax.rem(t + i, 4)
        start = blocks[p] + widen(jnp.exp(log_start[p]))[0:1, :] * s_in[...]
        reach = widen(jnp.exp(cum[p]))
        y_now = y_in[p] + reach * dot(bcc[p, :, 128:256], start.astype(BF16))
        now = y_now * silu(gate[p].astype(F32))
        squares = (now * now).astype(BF16)
        sq[t, p] = dot(jnp.ones((8, WIDTH), BF16), squares, NT)
        out = (now * gain[...]).astype(BF16)
        gated[p] = out
        ap_send[p] = dot(down_t[...], out, NT)
        return carry

    def project(p, half, store, first=0, count=5):
        def piece(i, carry):
            lanes = pl.ds(pl.multiple_of(i * 256, 256), 256)
            lanes_w = pl.ds(pl.multiple_of(half * HALF + i * 256, 256), 256)
            store(lanes, dot(gated[p], wt[:, lanes_w]))
            return carry

        lax.fori_loop(first, first + count, piece, 0)

    def to_slot(which, extra=None):
        def store(lanes, v):
            if extra is not None:
                v = v + rs_recv[extra, :, lanes].astype(F32)
            rs_send[which, :, lanes] = v.astype(BF16)

        return store

    def ship(which, where, first=0, count=5):
        part = pl.ds(first * 256, count * 256)
        send(rs_send.at[which, :, part], rs_recv.at[which, :, part], "r%d_%d" % (which, first), {"tensor": where})

    def landed(which, first=0, count=5):
        arrived(rs_recv.at[which, :, pl.ds(first * 256, count * 256)], "r%d_%d" % (which, first))

    lax.fori_loop(2, 3, finish, 0)
    project(far, 0, to_slot(0))
    ship(0, right)
    project(far, 1, to_slot(1))
    ship(1, left)
    lax.fori_loop(3, 6, finish, 0)
    ap_recv[t] = ap_send[t]
    for j in range(1, 4):
        peer = lax.rem(t + j, 4)
        send(sq.at[t], sq.at[t], "q%d" % j, {"tensor": peer})
        send(ap_send.at[peer], ap_recv.at[t], "a%d" % j, {"tensor": peer})
    project(right, 1, to_slot(2))
    ship(2, right)
    project(left, 0, to_slot(3))
    ship(3, left)

    for j in range(1, 4):
        source = lax.rem(t + 4 - j, 4)
        arrived(gt.at[source], "g%d" % j)
        arrived(sq.at[source], "q%d" % j)
        arrived(ap_recv.at[source], "a%d" % j)

    def row_scale(p):
        squares = (sq[0, p] + sq[1, p]) + (sq[2, p] + sq[3, p])
        return lax.rsqrt(squares * (1.0 / 5120.0) + EPS)

    adapter = ((ap_recv[0] + ap_recv[1]) + (ap_recv[2] + ap_recv[3])).astype(BF16)
    own_scale = row_scale(t)
    weighted = (scale * own_scale[0:1, :] * adapter.astype(F32)).astype(BF16)
    grad_a_now = jnp.zeros((RANK, WIDTH), F32)
    for p in range(4):
        rows_grad = (row_scale(p)[0:1, :] * gt[p]).astype(BF16)
        grad_a_now = grad_a_now + dot(rows_grad, gated[p])
    grad_b_now = dot(weighted, cot[...])
    for i in range(30):
        v_send[i // 2, i % 2] = (
            grad_a_now[:, i * 128 : i * 128 + 128] if i < 10
            else grad_b_now[:, (i - 10) * 128 : (i - 10) * 128 + 128]).astype(BF16)
    v_send[15] = jnp.zeros((2, RANK, 128), BF16)
    v_recv[c] = v_send[c]

    def v_copy(j):
        return pltpu.make_async_remote_copy(
            src_ref=v_send.at[lax.rem(c + j, 16)], dst_ref=v_recv.at[c],
            send_sem=sv.at[j], recv_sem=rv.at[j], device_id=context_peer(j), device_id_type=MESH)

    exchange(v_copy)

    landed(0)
    project(right, 0, to_slot(4, 0), 0, 3)
    ship(4, right, 0, 3)
    landed(1)
    project(left, 1, to_slot(5, 1), 0, 3)
    ship(5, left, 0, 3)

    settle(v_copy)

    def add_v(i, held):
        return held + v_recv[i].astype(F32)

    y_recv[s] = lax.fori_loop(0, 16, add_v, jnp.zeros((2, RANK, 128), F32))
    for j in range(1, 4):
        send(y_recv.at[s], y_recv.at[s], "y%d" % j, {"fsdp": lax.rem(s + j, 4)})
    project(right, 0, to_slot(4, 0), 3, 2)
    project(left, 1, to_slot(5, 1), 3, 2)
    for j in range(1, 4):
        arrived(y_recv.at[lax.rem(s + 4 - j, 4)], "y%d" % j)
    t_recv[t] = ((y_recv[0] + y_recv[1]) + (y_recv[2] + y_recv[3])).astype(BF16)
    for j in range(1, 4):
        send(t_recv.at[t], t_recv.at[t], "t%d" % j, {"tensor": lax.rem(t + j, 4)})
    ship(4, right, 3, 2)
    ship(5, left, 3, 2)

    def own_part(half):
        def store(lanes, v):
            lanes_up = pl.ds(pl.multiple_of(half * HALF + lanes.start, 256), 256)
            own[half, :, lanes] = v + 2.0 * dot(adapter, up[:, lanes_up], TN)

        return store

    project(t, 0, own_part(0))
    project(t, 1, own_part(1))

    for j in range(1, 4):
        arrived(t_recv.at[lax.rem(t + 4 - j, 4)], "t%d" % j)

    def add_t(i, held):
        keep = jnp.where(jnp.logical_or(c >= 5, i == t), 1.0, 0.0)
        return held + keep * t_recv[i].astype(F32)

    v_all[c] = lax.fori_loop(0, 4, add_t, jnp.zeros((2, RANK, 128), F32)).astype(BF16)

    def all_copy(j):
        return pltpu.make_async_remote_copy(
            src_ref=v_all.at[c], dst_ref=v_all.at[c],
            send_sem=sg.at[j], recv_sem=rg.at[j], device_id=context_peer(j), device_id_type=MESH)

    exchange(all_copy)

    landed(2)
    landed(3)
    landed(4, 0, 3)
    landed(5, 0, 3)
    landed(4, 3, 2)
    landed(5, 3, 2)
    scale_col = jnp.broadcast_to(own_scale[0:1, :], (128, 128)).T

    def close(i, carry):
        lanes = tile(i)
        first = own[0, :, lanes] + rs_recv[4, :, lanes].astype(F32) + rs_recv[3, :, lanes].astype(F32)
        second = own[1, :, lanes] + rs_recv[2, :, lanes].astype(F32) + rs_recv[5, :, lanes].astype(F32)
        mixed[:, lanes] = (scale_col * first).astype(BF16)
        mixed[:, pl.ds(pl.multiple_of(HALF + i * 128, 128), 128)] = (scale_col * second).astype(BF16)
        return carry

    lax.fori_loop(0, 10, close, 0)

    settle(all_copy)
    for i in range(10):
        grad_a[:, i * 128 : i * 128 + 128] = v_all[i // 2, i % 2].astype(F32)
    for i in range(20):
        grad_b[:, i * 128 : i * 128 + 128] = v_all[5 + i // 2, i % 2].astype(F32)

    for make, how_many in (
        (decay_copy, 16), (state_copy, 8), (back_copy, 8), (v_copy, 16), (all_copy, 16)
    ):
        settle(make, how_many, received=False)
    for copy in started:
        copy.wait_send()

    @pl.when(gives_rim)
    def _():
        for copy in rim_copies():
            copy.wait_send()


def shards(
    input_raw, state_proj_raw, gate_branch, step_raw, convolution_taps, convolution_bias, step_bias,
    decay_log_rate, skip_weight, gated_norm_gain, output_weight, adapter_down, adapter_up, cotangent,
):
    hbm = pl.BlockSpec(memory_space=pl.ANY)
    vmem = pl.BlockSpec(memory_space=pltpu.VMEM)
    dma = pltpu.SemaphoreType.DMA
    mixed, grad_a, grad_b = pl.pallas_call(
        kernel,
        out_shape=(
            jax.ShapeDtypeStruct((ROWS, OUT), BF16),
            jax.ShapeDtypeStruct((RANK, WIDTH), F32),
            jax.ShapeDtypeStruct((RANK, OUT), F32),
        ),
        in_specs=[hbm] * 14,
        out_specs=(vmem, vmem, vmem),
        scratch_shapes=[
            pltpu.VMEM((16 + 512, WIDTH), BF16),
            pltpu.VMEM((2, 64, WIDTH), BF16),
            pltpu.VMEM((4, ROWS, WIDTH), BF16),
            pltpu.VMEM((16 + 512, 256), BF16),
            pltpu.VMEM((4, ROWS, 256), BF16),
            pltpu.VMEM((4, 24, 128), BF16),
            pltpu.VMEM((4, ROWS, WIDTH), BF16),
            pltpu.VMEM((2, 64, WIDTH), BF16),
            pltpu.VMEM((WIDTH, OUT), BF16),
            pltpu.VMEM((ROWS, OUT), BF16),
            pltpu.VMEM((4, WIDTH), F32),
            pltpu.VMEM((4, 256), F32),
            pltpu.VMEM((1, WIDTH), F32),
            pltpu.VMEM((1, 256), F32),
            pltpu.VMEM((3, 1, HEADS), F32),
            pltpu.VMEM((1, WIDTH), F32),
            pltpu.VMEM((RANK, WIDTH), BF16),
            pltpu.VMEM((RANK, OUT), BF16),
            pltpu.VMEM((8, WIDTH), F32),
            pltpu.VMEM((256, WIDTH), BF16),
            pltpu.VMEM((4, ROWS, 128), F32),
            pltpu.VMEM((4, ROWS, 128), F32),
            pltpu.VMEM((4, 8, 128), F32),
            pltpu.VMEM((4, 8, 128), F32),
            pltpu.VMEM((4, ROWS, WIDTH), F32),
            pltpu.VMEM((4, STATE, WIDTH), F32),
            pltpu.VMEM((4, 8, WIDTH), F32),
            pltpu.VMEM((STATE, WIDTH), F32),
            pltpu.VMEM((STATE, 640), F32),
            pltpu.VMEM((8, 16, 640), BF16),
            pltpu.VMEM((8, 16, 640), BF16),
            pltpu.VMEM((16, 8, 128), F32),
            pltpu.VMEM((128, WIDTH), F32),
            pltpu.VMEM((8, 16, 640), BF16),
            pltpu.VMEM((8, 16, 640), BF16),
            pltpu.VMEM((STATE, 640), BF16),
            pltpu.VMEM((STATE, 640), BF16),
            pltpu.VMEM((STATE, WIDTH), F32),
            pltpu.VMEM((4, ROWS, WIDTH), BF16),
            pltpu.VMEM((4, RANK, 128), F32),
            pltpu.VMEM((4, 4, 8, 128), F32),
            pltpu.VMEM((4, RANK, 128), F32),
            pltpu.VMEM((4, RANK, 128), F32),
            pltpu.VMEM((6, ROWS, HALF), BF16),
            pltpu.VMEM((6, ROWS, HALF), BF16),
            pltpu.VMEM((2, ROWS, HALF), F32),
            pltpu.VMEM((16, 2, RANK, 128), BF16),
            pltpu.VMEM((16, 2, RANK, 128), BF16),
            pltpu.VMEM((4, 2, RANK, 128), F32),
            pltpu.VMEM((4, 2, RANK, 128), BF16),
            pltpu.VMEM((16, 2, RANK, 128), BF16),
            dma((72,)), dma((72,)), dma((24,)),
            dma((8,)), dma((8,)), dma((16,)), dma((16,)), dma((8,)), dma((8,)),
            dma((16,)), dma((16,)), dma((16,)), dma((16,)),
        ],
        compiler_params=pltpu.CompilerParams(
            collective_id=0, has_side_effects=True, vmem_limit_bytes=64 * 1000 * 1000),
    )(
        input_raw[0], state_proj_raw[0], gate_branch[0], step_raw[0].T, output_weight, cotangent[0],
        convolution_taps, convolution_bias[None, :], step_bias[None, :], decay_log_rate[None, :],
        skip_weight[None, :], gated_norm_gain[None, :], adapter_down.T, adapter_up,
    )
    return (mixed[None], grad_a.T, grad_b)


def solution(mesh):
    torus = Mesh(
        mesh.devices.reshape(8, 2, mesh.shape["tensor"], mesh.shape["fsdp"]),
        ("context_0", "context_1", "tensor", "fsdp"),
    )
    tokens = P("fsdp", CONTEXT_TENSOR, None)
    return jax.shard_map(
        shards,
        mesh=torus,
        in_specs=(
            tokens, tokens, tokens, tokens, P(), P(), P("tensor"), P("tensor"), P("tensor"), P("tensor"),
            P("tensor", "fsdp"), P("tensor", None), P(), tokens,
        ),
        out_specs=(tokens, P("tensor", None), P()),
        check_vma=False,
    )
```

```python
import functools

import jax
import jax.numpy as jnp
from jax import lax
from jax.experimental import pallas as pl
from jax.experimental.pallas import tpu as pltpu
from jax.sharding import Mesh
from jax.sharding import PartitionSpec as P

MESH = pl.DeviceIdType.MESH
CONTEXT_TENSOR = ("context_0", "context_1", "tensor")
F32 = jnp.float32
BF16 = jnp.bfloat16

ROWS = 128
WIDTH = 1280
STATE = 128
OUT = 2560
HALF = 1280
RANK = 16
HEADS = 20
COLS = 640
TOKENS = 32768
EPS = 1e-05

NT = (((1,), (1,)), ((), ()))
TN = (((0,), (0,)), ((), ()))


def silu(v):
    half = 0.5 * v
    return half + half * jnp.tanh(half)


def dot(a, b, dims=(((1,), (0,)), ((), ())), precision=None):
    return lax.dot_general(a, b, dims, precision=precision, preferred_element_type=F32)


def kernel(
    x_in, bc_in, z_in, dt_in, w_in, cot_in, taps_in, bias_in, step_bias_in, rate_in, skip_in, gain_in, down_in, up_in,
    mixed, grad_a, grad_b,
    x_ext, xr, xc, bc_ext, bcc, dt_all, gate, zr, wt, cot,
    taps_x, taps_bc, bias, head_par, gain_rows, gain, down_t, up, skip, weights, tails,
    spread, step, cum, log_start, log_tail, y_in, blocks, kept, state, peer_state,
    st_send, st_recv, dec_all, dec_wide, back_send, back_recv, in_send, in_recv, s_in,
    gated, gt, sq, ap_send, ap_recv,
    rs_send, rs_recv, own,
    v_send, v_recv, y_recv, t_recv, v_all, mixed_here, a_here, b_here,
    sx, rx, sl, sc, rc_, sd, rd, sb, rb, sv, rv, sg, rg,
):
    z, k = lax.axis_index("context_0"), lax.axis_index("context_1")
    t, s = lax.axis_index("tensor"), lax.axis_index("fsdp")
    c = 2 * z + k
    right, left, far = lax.rem(t + 1, 4), lax.rem(t + 3, 4), lax.rem(t + 2, 4)
    up_y, down_y, far_y = lax.rem(s + 1, 4), lax.rem(s + 3, 4), lax.rem(s + 2, 4)
    started = []
    slots = {}

    def slot(name):
        return slots.setdefault(name, len(slots))

    def remote(src, dst, name, where):
        return pltpu.make_async_remote_copy(
            src_ref=src, dst_ref=dst, send_sem=sx.at[slot(name)], recv_sem=rx.at[slot(name)],
            device_id=where, device_id_type=MESH,
        )

    def send(src, dst, name, where):
        copy = remote(src, dst, name, where)
        copy.start()
        started.append(copy)

    def arrived(dst, name):
        remote(dst, dst, name, {"tensor": right}).wait_recv()

    def chip_at(i):
        step_now = lax.div(i + 1, 2)
        return lax.rem(z + 4 + (1 - 2 * lax.rem(i, 2)) * step_now, 8)

    def core_at(j):
        return lax.rem(k + j, 2)

    def context_index(j):
        return 2 * chip_at(lax.div(j - 1, 2)) + core_at(j)

    def context_peer(j):
        return {"context_0": chip_at(lax.div(j - 1, 2)), "context_1": core_at(j)}

    def chip_peer(j):
        return {"context_0": chip_at(j - 1)}

    def exchange(make, how_many=16):
        def go(j, carry):
            make(j).start()
            return carry

        lax.fori_loop(1, how_many, go, 0)

    def settle(make, how_many=16, received=True):
        def go(j, carry):
            if received:
                make(j).wait_recv()
            else:
                make(j).wait_send()
            return carry

        lax.fori_loop(1, how_many, go, 0)

    def tile(i):
        return pl.ds(pl.multiple_of(i * 128, 128), 128)

    barrier = pltpu.get_barrier_semaphore()

    def greet(j, carry):
        pl.semaphore_signal(barrier, inc=1, device_id=context_peer(j), device_id_type=MESH)
        return carry

    for j in range(1, 4):
        pl.semaphore_signal(barrier, inc=1, device_id={"tensor": lax.rem(t + j, 4)}, device_id_type=MESH)
        pl.semaphore_signal(barrier, inc=1, device_id={"fsdp": lax.rem(s + j, 4)}, device_id_type=MESH)
    lax.fori_loop(1, 16, greet, 0)
    before = lax.rem(c + 15, 16)
    after = lax.rem(c + 1, 16)

    @pl.when(c > 0)
    def _():
        pl.semaphore_signal(
            barrier, inc=1,
            device_id={"context_0": lax.div(before, 2), "context_1": lax.rem(before, 2), "tensor": 3},
            device_id_type=MESH,
        )

    def columns(p):
        return pl.ds(pl.multiple_of(p * WIDTH, WIDTH), WIDTH)

    def x_rows(p, first, count):
        return x_ext.at[pl.ds(pl.multiple_of(16 + p * ROWS + first, 16), count)]

    def z_rows(p, first, count):
        return gate.at[p, pl.ds(first, count)]

    def bc_rows(p, first, count):
        return bc_ext.at[pl.ds(pl.multiple_of(16 + p * ROWS + first, 16), count)]

    def w_part(rows_from, count, y):
        return wt.at[
            pl.ds(pl.multiple_of(rows_from, 64), count), pl.ds(pl.multiple_of(y * COLS, COLS), COLS)
        ]

    def dt_window(p):
        return dt_in.at[pl.ds(pl.multiple_of(8 * lax.div(5 * p, 2), 8), 24)]

    local = {}

    def copy_here(name, src, dst):
        local[name] = pltpu.make_async_copy(src, dst, sl.at[8 + len(local)])
        local[name].start()

    copy_here("cot", cot_in, cot)
    copy_here("up", up_in, up)
    copy_here("step_bias", step_bias_in, head_par.at[0])
    copy_here("rate", rate_in, head_par.at[1])
    copy_here("skip", skip_in, head_par.at[2])
    copy_here("bc", bc_in, bc_rows(t, 0, ROWS))
    copy_here("dt", dt_window(t), dt_all.at[t])
    copy_here("taps_x", taps_in.at[:, columns(t)], taps_x)
    copy_here("taps_bc", taps_in.at[:, pl.ds(4 * WIDTH, 256)], taps_bc)
    copy_here("bias", bias_in, bias)
    copy_here("x", x_in.at[:, columns(t)], x_rows(t, 0, ROWS))
    copy_here("gain", gain_in, gain_rows)
    copy_here("down", down_in, down_t)
    copy_here("gate", z_in.at[:, columns(t)], gate.at[t])
    copy_here("w", w_in, w_part(0, 1280, s))

    def head_mask(i, carry):
        head = lax.broadcasted_iota(jnp.int32, (256, 128), 0)
        head = jnp.where(head >= 128, head - 128, head)
        lane = lax.broadcasted_iota(jnp.int32, (256, 128), 1)
        own_head = 2 * i + jnp.where(lane >= 64, 1, 0)
        spread[:, tile(i)] = jnp.where(head == own_head, 1.0, 0.0).astype(BF16)
        return carry

    lax.fori_loop(0, 10, head_mask, 0)

    def widen(v):
        high = v.astype(BF16)
        low = (v - high.astype(F32)).astype(BF16)
        return dot(jnp.concatenate([high, low], axis=1), spread[...])

    scale = 2.0 / (TOKENS ** 0.5)

    local["cot"].wait()
    local["up"].wait()
    gt[t] = dot(up[...], cot[...], NT) * scale

    gives_rim = jnp.logical_and(t == 3, c < 15)

    @pl.when(gives_rim)
    def _():
        pl.semaphore_wait(barrier, 25)

    @pl.when(jnp.logical_not(gives_rim))
    def _():
        pl.semaphore_wait(barrier, 21)

    def far_start(src, relay, name):
        send(src.at[pl.ds(0, 64), columns(far)], relay.at[0], name + "0", {"tensor": right})
        send(src.at[pl.ds(64, 64), columns(far)], relay.at[1], name + "1", {"tensor": left})

    def near_start(src, rows, name):
        send(src.at[:, columns(right)], rows(t, 0, ROWS), name + "2", {"tensor": right})
        send(src.at[:, columns(left)], rows(t, 0, ROWS), name + "3", {"tensor": left})

    def far_forward(rows, relay, name):
        arrived(relay.at[0], name + "0")
        send(relay.at[0], rows(left, 0, 64), name + "4", {"tensor": right})
        arrived(relay.at[1], name + "1")
        send(relay.at[1], rows(right, 64, 64), name + "5", {"tensor": left})

    def near_wait(rows, name):
        arrived(rows(left, 0, ROWS), name + "2")
        arrived(rows(right, 0, ROWS), name + "3")

    def far_wait(rows, name):
        arrived(rows(far, 0, 64), name + "4")
        arrived(rows(far, 64, 64), name + "5")

    far_start(x_in, xr, "x")
    send(bc_in.at[pl.ds(0, 64)], bc_rows(t, 0, 64), "b0", {"tensor": right})
    send(bc_in.at[pl.ds(64, 64)], bc_rows(t, 64, 64), "b1", {"tensor": left})
    send(bc_in.at[pl.ds(64, 64)], bc_rows(t, 64, 64), "b2", {"tensor": right})
    send(bc_in.at[pl.ds(0, 64)], bc_rows(t, 0, 64), "b3", {"tensor": left})
    for j in (1, 3, 2):
        peer = lax.rem(t + j, 4)
        send(dt_window(peer), dt_all.at[t], "dt%d" % j, {"tensor": peer})
    near_start(x_in, x_rows, "x")

    def rim_copies():
        copies = []
        for p in range(4):
            where = {"context_0": lax.div(after, 2), "context_1": lax.rem(after, 2), "tensor": p}
            copies.append(pltpu.make_async_remote_copy(
                src_ref=x_in.at[pl.ds(112, 16), pl.ds(p * WIDTH, WIDTH)], dst_ref=x_ext.at[pl.ds(0, 16)],
                send_sem=sl.at[p], recv_sem=rx.at[slot("rim_x")], device_id=where, device_id_type=MESH))
            copies.append(pltpu.make_async_remote_copy(
                src_ref=bc_in.at[pl.ds(112, 16)], dst_ref=bc_ext.at[pl.ds(0, 16)],
                send_sem=sl.at[4 + p], recv_sem=rx.at[slot("rim_b")], device_id=where, device_id_type=MESH))
        return copies

    @pl.when(gives_rim)
    def _():
        for copy in rim_copies():
            copy.start()

    @pl.when(c == 0)
    def _():
        x_ext[0:16, :] = jnp.zeros((16, WIDTH), BF16)
        bc_ext[0:16, :] = jnp.zeros((16, 256), BF16)

    mine, other = k * 640, (1 - k) * 640

    def w_src(first):
        return w_in.at[pl.ds(pl.multiple_of(mine + first, 64), 320)]

    send(w_src(0), w_part(mine, 320, s), "w0", {"fsdp": up_y})
    send(w_src(320), w_part(mine + 320, 320, s), "w1", {"fsdp": down_y})
    send(w_src(320), w_part(mine + 320, 320, s), "w2", {"fsdp": up_y})
    send(w_src(0), w_part(mine, 320, s), "w3", {"fsdp": down_y})

    for name in ("step_bias", "rate", "skip", "bc", "dt", "taps_x", "taps_bc", "bias", "x", "gain", "down"):
        local[name].wait()
    pick20 = jnp.where(
        lax.broadcasted_iota(jnp.int32, (HEADS, 128), 0) == lax.broadcasted_iota(jnp.int32, (HEADS, 128), 1), 1.0, 0.0)

    def head_row(i):
        return dot(jnp.broadcast_to(head_par[i], (8, HEADS)), pick20, precision=lax.Precision.HIGHEST)

    step_bias = head_row(0)[0:1, :]
    rate = jnp.exp(head_row(1))[0:1, :]
    skip[...] = widen(head_row(2))
    for i in range(10):
        gain[:, i * 128 : i * 128 + 128] = gain_rows[i : i + 1, :]

    for j in range(1, 4):
        arrived(dt_all.at[lax.rem(t + 4 - j, 4)], "dt%d" % j)

    row = lax.broadcasted_iota(jnp.int32, (128, 128), 0)
    col = lax.broadcasted_iota(jnp.int32, (128, 128), 1)
    causal = row >= col
    tri = jnp.where(causal, 1.0, 0.0)
    pick_row = lax.broadcasted_iota(jnp.int32, (24, 128), 0)
    pick_col = lax.broadcasted_iota(jnp.int32, (24, 128), 1)
    hit = jnp.logical_and(pick_row == pick_col + 4 * lax.rem(t, 2), pick_col < HEADS)
    pick = jnp.where(hit, 1.0, 0.0).astype(BF16)

    total = jnp.zeros((1, 128), F32)
    for p in range(4):
        raw = dot(dt_all[p], pick, TN) + step_bias
        step_now = jnp.maximum(raw, 0.0) + jnp.log1p(jnp.exp(-jnp.abs(raw)))
        cum_now = dot(tri, -step_now * rate, precision=lax.Precision.HIGHEST)
        step[p] = step_now
        cum[p] = cum_now
        log_start[p] = jnp.broadcast_to(total, (8, 128))
        total = total + cum_now[127:128, :]
    for p in range(4):
        log_tail[p] = total - log_start[p] - cum[p, 127:128, :]
        kept[p] = widen(jnp.broadcast_to(jnp.exp(cum[p, 127:128, :]), (8, 128)))
    dec_all[c] = jnp.broadcast_to(jnp.exp(total), (8, 128))

    arrived(bc_rows(left, 0, 64), "b0")
    send(bc_rows(left, 0, 64), bc_rows(left, 0, 64), "b4", {"tensor": right})
    arrived(bc_rows(right, 64, 64), "b1")
    send(bc_rows(right, 64, 64), bc_rows(right, 64, 64), "b5", {"tensor": left})
    far_forward(x_rows, xr, "x")
    far_start(z_in, zr, "z")
    near_start(z_in, z_rows, "z")

    def decay_copy(j):
        return pltpu.make_async_remote_copy(
            src_ref=dec_all.at[c], dst_ref=dec_all.at[c],
            send_sem=sd.at[j], recv_sem=rd.at[j], device_id=context_peer(j), device_id_type=MESH)

    exchange(decay_copy)
    for j in range(1, 4):
        send(gt.at[t], gt.at[t], "g%d" % j, {"tensor": lax.rem(t + j, 4)})

    def convolved(ext, p, lanes, taps, bias_row):
        v = ext[pl.ds(pl.multiple_of(p * ROWS, 16), ROWS + 16), lanes].astype(F32)
        acc = bias[pl.ds(bias_row, 1), :] + taps[0:1, lanes] * pltpu.roll(v, 3, 0)
        acc = acc + taps[1:2, lanes] * pltpu.roll(v, 2, 0)
        acc = acc + taps[2:3, lanes] * pltpu.roll(v, 1, 0)
        acc = acc + taps[3:4, lanes] * v
        return silu(acc[16:]).astype(BF16)

    @pl.when(c > 0)
    def _():
        arrived(x_ext.at[pl.ds(0, 16)], "rim_x")
        arrived(bc_ext.at[pl.ds(0, 16)], "rim_b")

    state[...] = jnp.zeros((STATE, WIDTH), F32)

    def block(i, carry):
        p = lax.rem(t + i, 4)
        for half in range(2):
            bcc[p, :, pl.ds(half * 128, 128)] = convolved(bc_ext, p, pl.ds(half * 128, 128), taps_bc, 40 + half)

        def lanes_of(j, inner):
            xc[p, :, tile(j)] = convolved(x_ext, p, tile(j), taps_x, 10 * t + j)
            return inner

        lax.fori_loop(0, 10, lanes_of, 0)
        scaled = (xc[p].astype(F32) * weights[p]).astype(BF16)
        fresh = dot(bcc[p, :, 0:128], scaled, TN)
        blocks[p] = fresh
        state[...] = state[...] + tails[p, 0:1, :] * fresh
        return carry

    def weigh(p, carry):
        cum_now = cum[p]
        weights[p] = widen(step[p] * jnp.exp(cum_now[127:128, :] - cum_now))
        tails[p] = widen(jnp.exp(log_tail[p]))
        return carry

    lax.fori_loop(0, 4, weigh, 0)
    arrived(bc_rows(left, 64, 64), "b2")
    arrived(bc_rows(right, 0, 64), "b3")
    near_wait(x_rows, "x")
    lax.fori_loop(0, 2, block, 0)
    arrived(bc_rows(far, 0, 64), "b4")
    arrived(bc_rows(far, 64, 64), "b5")
    far_wait(x_rows, "x")
    lax.fori_loop(2, 4, block, 0)

    core = {"context_1": 1 - k}

    def half_lanes(i):
        return pl.ds(pl.multiple_of(i * 640, 640), 640)

    send(state.at[:, half_lanes(1 - k)], peer_state, "pair", core)
    settle(decay_copy)
    dec_wide[...] = widen(dec_all[...].reshape(128, 128))
    arrived(peer_state, "pair")

    def chip_decay(of):
        return dec_wide[pl.ds(pl.multiple_of(16 * of, 16), 8), half_lanes(k)] * dec_wide[
            pl.ds(pl.multiple_of(16 * of + 8, 8), 8), half_lanes(k)]

    decay_second = dec_wide[pl.ds(pl.multiple_of(16 * z + 8, 8), 8), half_lanes(k)][0:1, :]
    weight_mine = jnp.where(k == 0, decay_second, jnp.ones_like(decay_second))
    weight_peer = jnp.where(k == 0, jnp.ones_like(decay_second), decay_second)

    def pack_state(i, carry):
        rows = pl.ds(pl.multiple_of(i * 16, 16), 16)
        both = weight_mine * state[rows, half_lanes(k)] + weight_peer * peer_state[rows, :]
        st_send[i] = both.astype(BF16)
        return carry

    lax.fori_loop(0, 8, pack_state, 0)

    def state_copy(j):
        return pltpu.make_async_remote_copy(
            src_ref=st_send.at[chip_at(j - 1)], dst_ref=st_recv.at[z],
            send_sem=sc.at[j], recv_sem=rc_.at[j], device_id=chip_peer(j), device_id_type=MESH)

    exchange(state_copy, 8)
    st_recv[z] = st_send[z]

    arrived(w_part(mine, 320, down_y), "w0")
    send(w_part(mine, 320, down_y), w_part(mine, 320, down_y), "w4", {"fsdp": up_y})
    arrived(w_part(mine + 320, 320, up_y), "w1")
    send(w_part(mine + 320, 320, up_y), w_part(mine + 320, 320, up_y), "w5", {"fsdp": down_y})
    far_forward(z_rows, zr, "z")

    def inside(p, carry):
        b_now, c_now = bcc[p, :, 0:128], bcc[p, :, 128:256]
        gram = dot(c_now, b_now, NT)
        cum_now = cum[p]
        shifted = (cum_now - jnp.log(step[p])).T
        lane = lax.broadcasted_iota(jnp.int32, (1, 128), 1)
        low = jnp.where(lane < 64, 1.0, 0.0)
        for q in range(HEADS // 2):
            mats = []
            for h in (2 * q, 2 * q + 1):
                gap = cum_now[:, h : h + 1] - shifted[h : h + 1, :]
                mats.append(jnp.exp(jnp.where(causal, gap, -1e30)) * gram)
            both = jnp.concatenate(mats, axis=1).astype(BF16)
            x_pair = xc[p, :, pl.ds(q * 128, 128)].astype(F32)
            x_two = jnp.concatenate([x_pair * low, x_pair * (1.0 - low)], axis=0).astype(BF16)
            y_in[p, :, pl.ds(q * 128, 128)] = dot(both, x_two) + x_pair * skip[0:1, pl.ds(q * 128, 128)]
        return carry

    lax.fori_loop(0, 4, inside, 0)

    settle(state_copy, 8)

    def chain(i, held):
        back_send[i] = held.astype(BF16)
        return chip_decay(i)[0:1, :] * held + st_recv[i].astype(F32)

    lax.fori_loop(0, 8, chain, jnp.zeros((16, 640), F32))

    def back_copy(j):
        return pltpu.make_async_remote_copy(
            src_ref=back_send.at[chip_at(j - 1)], dst_ref=back_recv.at[z],
            send_sem=sb.at[j], recv_sem=rb.at[j], device_id=chip_peer(j), device_id_type=MESH)

    exchange(back_copy, 8)
    back_recv[z] = back_send[z]

    def starts(j, carry):
        held = jnp.zeros((STATE, 128), F32)
        for p in range(4):
            fresh = blocks[p, :, tile(j)]
            blocks[p, :, tile(j)] = held
            held = kept[p, 0:1, tile(j)] * held + fresh
        return carry

    lax.fori_loop(0, 10, starts, 0)

    arrived(w_part(mine + 320, 320, down_y), "w2")
    send(w_part(mine, 640, down_y), w_part(mine, 640, down_y), "w6", core)
    arrived(w_part(mine, 320, up_y), "w3")
    send(w_part(mine, 640, up_y), w_part(mine, 640, up_y), "w7", core)
    arrived(w_part(mine, 320, far_y), "w4")
    arrived(w_part(mine + 320, 320, far_y), "w5")
    send(w_part(mine, 640, far_y), w_part(mine, 640, far_y), "w8", core)

    local["gate"].wait()
    near_wait(z_rows, "z")
    far_wait(z_rows, "z")
    settle(back_copy, 8)

    decay_first = dec_wide[pl.ds(pl.multiple_of(16 * z, 8), 8), half_lanes(k)][0:1, :]

    def unpack_state(i, carry):
        rows = pl.ds(pl.multiple_of(i * 16, 16), 16)
        first = back_recv[i].astype(F32)
        span = jnp.where(k == 0, state[rows, half_lanes(k)], peer_state[rows, :])
        second = decay_first * first + span
        s_in[rows, half_lanes(k)] = jnp.where(k == 0, first, second)
        in_send[rows, :] = jnp.where(k == 0, second, first).astype(BF16)
        return carry

    lax.fori_loop(0, 8, unpack_state, 0)
    send(in_send, in_recv, "in", core)

    local["w"].wait()
    arrived(w_part(other, 640, down_y), "w6")
    arrived(w_part(other, 640, up_y), "w7")
    arrived(w_part(other, 640, far_y), "w8")
    arrived(in_recv, "in")
    s_in[:, half_lanes(1 - k)] = in_recv[...].astype(F32)

    def finish(i, carry):
        p = lax.rem(t + i, 4)
        start = blocks[p] + widen(jnp.exp(log_start[p]))[0:1, :] * s_in[...]
        reach = widen(jnp.exp(cum[p]))
        y_now = y_in[p] + reach * dot(bcc[p, :, 128:256], start.astype(BF16))
        now = y_now * silu(gate[p].astype(F32))
        squares = (now * now).astype(BF16)
        sq[t, pl.ds(p, 1), :] = dot(jnp.ones((8, WIDTH), BF16), squares, NT)[0:1, :]
        out = (now * gain[...]).astype(BF16)
        gated[p] = out
        ap_send[p] = dot(down_t[...], out, NT)
        return carry

    def project(p, half, store, first=0, count=5):
        def piece(i, carry):
            lanes = pl.ds(pl.multiple_of(i * 256, 256), 256)
            lanes_w = pl.ds(pl.multiple_of(half * HALF + i * 256, 256), 256)
            store(lanes, dot(gated[p], wt[:, lanes_w]))
            return carry

        lax.fori_loop(first, first + count, piece, 0)

    def to_slot(which, extra=None):
        def store(lanes, v):
            if extra is not None:
                v = v + rs_recv[extra, :, lanes].astype(F32)
            rs_send[which, :, lanes] = v.astype(BF16)

        return store

    def piece_at(ref, which, i):
        return ref.at[which, :, pl.ds(i * 256, 256)]

    def ship(which, where, i):
        send(piece_at(rs_send, which, i), piece_at(rs_recv, which, i), "r%d_%d" % (which, i), {"tensor": where})

    def landed(which, i):
        arrived(piece_at(rs_recv, which, i), "r%d_%d" % (which, i))

    lax.fori_loop(2, 3, finish, 0)
    for i in range(5):
        project(far, 0, to_slot(0), i, 1)
        project(far, 1, to_slot(1), i, 1)
        if i < 3:
            ship(0, right, i)
            ship(1, left, i)
    lax.fori_loop(3, 6, finish, 0)
    ap_recv[t] = ap_send[t]
    for j in (2, 1, 3):
        peer = lax.rem(t + j, 4)
        send(sq.at[t], sq.at[t], "q%d" % j, {"tensor": peer})
        send(ap_send.at[peer], ap_recv.at[t], "a%d" % j, {"tensor": peer})
    for i in range(3, 5):
        ship(0, right, i)
        ship(1, left, i)
    for i in range(5):
        project(right, 1, to_slot(2), i, 1)
        ship(2, right, i)
        project(left, 0, to_slot(3), i, 1)
        ship(3, left, i)

    for j in range(1, 4):
        source = lax.rem(t + 4 - j, 4)
        arrived(gt.at[source], "g%d" % j)
        arrived(sq.at[source], "q%d" % j)
        arrived(ap_recv.at[source], "a%d" % j)

    def row_scale(p):
        rows = pl.ds(p, 1)
        squares = (sq[0, rows, :] + sq[1, rows, :]) + (sq[2, rows, :] + sq[3, rows, :])
        return lax.rsqrt(squares * (1.0 / 5120.0) + EPS)

    adapter = ((ap_recv[0] + ap_recv[1]) + (ap_recv[2] + ap_recv[3])).astype(BF16)
    own_scale = row_scale(t)
    weighted = (scale * own_scale[0:1, :] * adapter.astype(F32)).astype(BF16)
    grad_a_now = jnp.zeros((RANK, WIDTH), F32)
    for p in range(4):
        rows_grad = (row_scale(p)[0:1, :] * gt[p]).astype(BF16)
        grad_a_now = grad_a_now + dot(rows_grad, gated[p])
    grad_b_now = dot(weighted, cot[...])
    for i in range(30):
        v_send[i // 2, i % 2] = (
            grad_a_now[:, i * 128 : i * 128 + 128] if i < 10
            else grad_b_now[:, (i - 10) * 128 : (i - 10) * 128 + 128]).astype(BF16)
    v_send[15] = jnp.zeros((2, RANK, 128), BF16)
    v_recv[c] = v_send[c]

    def v_copy(j):
        return pltpu.make_async_remote_copy(
            src_ref=v_send.at[context_index(j)], dst_ref=v_recv.at[c],
            send_sem=sv.at[j], recv_sem=rv.at[j], device_id=context_peer(j), device_id_type=MESH)

    exchange(v_copy)

    for i in range(2):
        landed(0, i)
        project(right, 0, to_slot(4, 0), i, 1)
        ship(4, right, i)
        landed(1, i)
        project(left, 1, to_slot(5, 1), i, 1)
        ship(5, left, i)

    settle(v_copy)

    def add_v(i, held):
        return held + v_recv[i].astype(F32)

    y_recv[s] = lax.fori_loop(0, 16, add_v, jnp.zeros((2, RANK, 128), F32))
    for j in range(1, 4):
        send(y_recv.at[s], y_recv.at[s], "y%d" % j, {"fsdp": lax.rem(s + j, 4)})
    for i in range(2, 5):
        landed(0, i)
        project(right, 0, to_slot(4, 0), i, 1)
        landed(1, i)
        project(left, 1, to_slot(5, 1), i, 1)
    for j in range(1, 4):
        arrived(y_recv.at[lax.rem(s + 4 - j, 4)], "y%d" % j)
    t_recv[t] = ((y_recv[0] + y_recv[1]) + (y_recv[2] + y_recv[3])).astype(BF16)
    for j in range(1, 4):
        send(t_recv.at[t], t_recv.at[t], "t%d" % j, {"tensor": lax.rem(t + j, 4)})
    for i in range(2, 5):
        ship(4, right, i)
        ship(5, left, i)

    def own_part(half):
        def store(lanes, v):
            lanes_up = pl.ds(pl.multiple_of(half * HALF + lanes.start, 256), 256)
            own[half, :, lanes] = v + 2.0 * dot(adapter, up[:, lanes_up], TN)

        return store

    project(t, 0, own_part(0))
    project(t, 1, own_part(1))

    for j in range(1, 4):
        arrived(t_recv.at[lax.rem(t + 4 - j, 4)], "t%d" % j)

    def add_t(i, held):
        keep = jnp.where(jnp.logical_or(c >= 5, i == t), 1.0, 0.0)
        return held + keep * t_recv[i].astype(F32)

    v_all[c] = lax.fori_loop(0, 4, add_t, jnp.zeros((2, RANK, 128), F32)).astype(BF16)

    def all_copy(j):
        return pltpu.make_async_remote_copy(
            src_ref=v_all.at[c], dst_ref=v_all.at[c],
            send_sem=sg.at[j], recv_sem=rg.at[j], device_id=context_peer(j), device_id_type=MESH)

    exchange(all_copy)

    scale_col = jnp.broadcast_to(own_scale[0:1, :], (128, 128)).T
    for i in range(5):
        landed(2, i)
        landed(3, i)
    for i in range(5):
        landed(4, i)
        landed(5, i)

    def close(i, carry):
        lanes = tile(i)
        first = own[0, :, lanes] + rs_recv[4, :, lanes].astype(F32) + rs_recv[3, :, lanes].astype(F32)
        second = own[1, :, lanes] + rs_recv[2, :, lanes].astype(F32) + rs_recv[5, :, lanes].astype(F32)
        mixed_here[:, lanes] = (scale_col * first).astype(BF16)
        mixed_here[:, pl.ds(pl.multiple_of(HALF + i * 128, 128), 128)] = (scale_col * second).astype(BF16)
        return carry

    lax.fori_loop(0, 10, close, 0)
    copy_here("mixed", mixed_here, mixed)

    settle(all_copy)
    for i in range(10):
        a_here[:, i * 128 : i * 128 + 128] = v_all[i // 2, i % 2].astype(F32)
    for i in range(20):
        b_here[:, i * 128 : i * 128 + 128] = v_all[5 + i // 2, i % 2].astype(F32)
    copy_here("grad_a", a_here, grad_a)
    copy_here("grad_b", b_here, grad_b)

    for make, how_many in (
        (decay_copy, 16), (state_copy, 8), (back_copy, 8), (v_copy, 16), (all_copy, 16)
    ):
        settle(make, how_many, received=False)
    for copy in started:
        copy.wait_send()

    @pl.when(gives_rim)
    def _():
        for copy in rim_copies():
            copy.wait_send()

    for name in ("mixed", "grad_a", "grad_b"):
        local[name].wait()


def shards(
    input_raw, state_proj_raw, gate_branch, step_raw, convolution_taps, convolution_bias, step_bias,
    decay_log_rate, skip_weight, gated_norm_gain, output_weight, adapter_down, adapter_up, cotangent,
):
    hbm = pl.BlockSpec(memory_space=pl.ANY)
    dma = pltpu.SemaphoreType.DMA
    mixed, grad_a, grad_b = pl.pallas_call(
        kernel,
        out_shape=(
            jax.ShapeDtypeStruct((ROWS, OUT), BF16),
            jax.ShapeDtypeStruct((RANK, WIDTH), F32),
            jax.ShapeDtypeStruct((RANK, OUT), F32),
        ),
        in_specs=[hbm] * 14,
        out_specs=(hbm, hbm, hbm),
        scratch_shapes=[
            pltpu.VMEM((16 + 512, WIDTH), BF16),
            pltpu.VMEM((2, 64, WIDTH), BF16),
            pltpu.VMEM((4, ROWS, WIDTH), BF16),
            pltpu.VMEM((16 + 512, 256), BF16),
            pltpu.VMEM((4, ROWS, 256), BF16),
            pltpu.VMEM((4, 24, 128), BF16),
            pltpu.VMEM((4, ROWS, WIDTH), BF16),
            pltpu.VMEM((2, 64, WIDTH), BF16),
            pltpu.VMEM((WIDTH, OUT), BF16),
            pltpu.VMEM((ROWS, OUT), BF16),
            pltpu.VMEM((4, WIDTH), F32),
            pltpu.VMEM((4, 256), F32),
            pltpu.VMEM((42, 128), F32),
            pltpu.VMEM((3, 1, HEADS), F32),
            pltpu.VMEM((10, 128), F32),
            pltpu.VMEM((1, WIDTH), F32),
            pltpu.VMEM((RANK, WIDTH), BF16),
            pltpu.VMEM((RANK, OUT), BF16),
            pltpu.VMEM((8, WIDTH), F32),
            pltpu.VMEM((4, ROWS, WIDTH), F32),
            pltpu.VMEM((4, 8, WIDTH), F32),
            pltpu.VMEM((256, WIDTH), BF16),
            pltpu.VMEM((4, ROWS, 128), F32),
            pltpu.VMEM((4, ROWS, 128), F32),
            pltpu.VMEM((4, 8, 128), F32),
            pltpu.VMEM((4, 8, 128), F32),
            pltpu.VMEM((4, ROWS, WIDTH), F32),
            pltpu.VMEM((4, STATE, WIDTH), F32),
            pltpu.VMEM((4, 8, WIDTH), F32),
            pltpu.VMEM((STATE, WIDTH), F32),
            pltpu.VMEM((STATE, 640), F32),
            pltpu.VMEM((8, 16, 640), BF16),
            pltpu.VMEM((8, 16, 640), BF16),
            pltpu.VMEM((16, 8, 128), F32),
            pltpu.VMEM((128, WIDTH), F32),
            pltpu.VMEM((8, 16, 640), BF16),
            pltpu.VMEM((8, 16, 640), BF16),
            pltpu.VMEM((STATE, 640), BF16),
            pltpu.VMEM((STATE, 640), BF16),
            pltpu.VMEM((STATE, WIDTH), F32),
            pltpu.VMEM((4, ROWS, WIDTH), BF16),
            pltpu.VMEM((4, RANK, 128), F32),
            pltpu.VMEM((4, 8, 128), F32),
            pltpu.VMEM((4, RANK, 128), F32),
            pltpu.VMEM((4, RANK, 128), F32),
            pltpu.VMEM((6, ROWS, HALF), BF16),
            pltpu.VMEM((6, ROWS, HALF), BF16),
            pltpu.VMEM((2, ROWS, HALF), F32),
            pltpu.VMEM((16, 2, RANK, 128), BF16),
            pltpu.VMEM((16, 2, RANK, 128), BF16),
            pltpu.VMEM((4, 2, RANK, 128), F32),
            pltpu.VMEM((4, 2, RANK, 128), BF16),
            pltpu.VMEM((16, 2, RANK, 128), BF16),
            pltpu.VMEM((ROWS, OUT), BF16),
            pltpu.VMEM((RANK, WIDTH), F32),
            pltpu.VMEM((RANK, OUT), F32),
            dma((100,)), dma((100,)), dma((32,)),
            dma((8,)), dma((8,)), dma((16,)), dma((16,)), dma((8,)), dma((8,)),
            dma((16,)), dma((16,)), dma((16,)), dma((16,)),
        ],
        compiler_params=pltpu.CompilerParams(
            collective_id=0, has_side_effects=True, vmem_limit_bytes=64 * 1000 * 1000),
    )(
        input_raw[0], state_proj_raw[0], gate_branch[0], step_raw[0].T, output_weight, cotangent[0],
        convolution_taps, convolution_bias.reshape(42, 128), step_bias[None, :], decay_log_rate[None, :],
        skip_weight[None, :], gated_norm_gain.reshape(10, 128), adapter_down.T, adapter_up,
    )
    return (mixed[None], grad_a.T, grad_b)


def solution(mesh):
    torus = Mesh(
        mesh.devices.reshape(8, 2, mesh.shape["tensor"], mesh.shape["fsdp"]),
        ("context_0", "context_1", "tensor", "fsdp"),
    )
    tokens = P("fsdp", CONTEXT_TENSOR, None)
    return jax.shard_map(
        shards,
        mesh=torus,
        in_specs=(
            tokens, tokens, tokens, tokens, P(), P(), P("tensor"), P("tensor"), P("tensor"), P("tensor"),
            P("tensor", "fsdp"), P("tensor", None), P(), tokens,
        ),
        out_specs=(tokens, P("tensor", None), P()),
        check_vma=False,
    )
```

```python
import functools

import jax
import jax.numpy as jnp
from jax import lax
from jax.experimental import pallas as pl
from jax.experimental.pallas import tpu as pltpu
from jax.sharding import Mesh
from jax.sharding import PartitionSpec as P

MESH = pl.DeviceIdType.MESH
CONTEXT_TENSOR = ("context_0", "context_1", "tensor")
F32 = jnp.float32
BF16 = jnp.bfloat16

ROWS = 128
WIDTH = 1280
STATE = 128
OUT = 2560
HALF = 1280
RANK = 16
HEADS = 20
COLS = 640
TOKENS = 32768
EPS = 1e-05

NT = (((1,), (1,)), ((), ()))
TN = (((0,), (0,)), ((), ()))


def silu(v):
    half = 0.5 * v
    return half + half * jnp.tanh(half)


def dot(a, b, dims=(((1,), (0,)), ((), ())), precision=None):
    return lax.dot_general(a, b, dims, precision=precision, preferred_element_type=F32)


def kernel(
    x_in, bc_in, z_in, dt_in, w_in, cot_in, taps_in, bias_in, step_bias_in, rate_in, skip_in, gain_in, down_in, up_in,
    mixed, grad_a, grad_b,
    x_ext, xr, rim_x, rim_b, xc, bc_ext, bcc, dt_all, gate, zr, wt, cot,
    taps_x, taps_bc, bias, head_par, gain_rows, gain, down_t, up, skip, weights, tails,
    spread, step, cum, log_start, log_tail, y_in, blocks, kept, state, peer_state,
    st_send, st_recv, dec_all, dec_wide, back_send, back_recv, in_send, in_recv, s_in,
    gated, gt, sq, ap_send, ap_recv,
    rs_send, rs_recv, own,
    v_send, v_recv, y_recv, t_recv, v_all, mixed_here, a_here, b_here,
    sx, rx, sl, sc, rc_, sd, rd, sb, rb, sv, rv, sg, rg, sr, rr, rr_end,
):
    z, k = lax.axis_index("context_0"), lax.axis_index("context_1")
    t, s = lax.axis_index("tensor"), lax.axis_index("fsdp")
    c = 2 * z + k
    right, left, far = lax.rem(t + 1, 4), lax.rem(t + 3, 4), lax.rem(t + 2, 4)
    up_y, down_y, far_y = lax.rem(s + 1, 4), lax.rem(s + 3, 4), lax.rem(s + 2, 4)
    started = []
    slots = {}

    def slot(name):
        return slots.setdefault(name, len(slots))

    def remote(src, dst, name, where):
        return pltpu.make_async_remote_copy(
            src_ref=src, dst_ref=dst, send_sem=sx.at[slot(name)], recv_sem=rx.at[slot(name)],
            device_id=where, device_id_type=MESH,
        )

    def send(src, dst, name, where):
        copy = remote(src, dst, name, where)
        copy.start()
        started.append(copy)

    def arrived(dst, name):
        remote(dst, dst, name, {"tensor": right}).wait_recv()

    def chip_at(i):
        step_now = lax.div(i + 1, 2)
        return lax.rem(z + 4 + (1 - 2 * lax.rem(i, 2)) * step_now, 8)

    def core_at(j):
        return lax.rem(k + j, 2)

    def context_index(j):
        return 2 * chip_at(lax.div(j - 1, 2)) + core_at(j)

    def context_peer(j):
        return {"context_0": chip_at(lax.div(j - 1, 2)), "context_1": core_at(j)}

    def chip_peer(j):
        return {"context_0": chip_at(j - 1)}

    def exchange(make, how_many=16):
        def go(j, carry):
            make(j).start()
            return carry

        lax.fori_loop(1, how_many, go, 0)

    def settle(buffer, sem, how_many=15):
        several = buffer.at[pl.ds(0, how_many)]
        pltpu.make_async_copy(several, several, sem).wait()

    def tile(i):
        return pl.ds(pl.multiple_of(i * 128, 128), 128)

    barrier = pltpu.get_barrier_semaphore()

    def greet(j, carry):
        pl.semaphore_signal(barrier, inc=1, device_id=context_peer(j), device_id_type=MESH)
        return carry

    for j in range(1, 4):
        pl.semaphore_signal(barrier, inc=1, device_id={"tensor": lax.rem(t + j, 4)}, device_id_type=MESH)
        pl.semaphore_signal(barrier, inc=1, device_id={"fsdp": lax.rem(s + j, 4)}, device_id_type=MESH)
    lax.fori_loop(1, 16, greet, 0)
    before = lax.rem(c + 15, 16)
    after = lax.rem(c + 1, 16)

    @pl.when(c > 0)
    def _():
        pl.semaphore_signal(
            barrier, inc=1,
            device_id={"context_0": lax.div(before, 2), "context_1": lax.rem(before, 2), "tensor": 3},
            device_id_type=MESH,
        )

    def columns(p):
        return pl.ds(pl.multiple_of(p * WIDTH, WIDTH), WIDTH)

    def x_rows(p, first, count):
        return x_ext.at[pl.ds(pl.multiple_of(16 + p * ROWS + first, 16), count)]

    def z_rows(p, first, count):
        return gate.at[p, pl.ds(first, count)]

    def bc_rows(p, first, count):
        return bc_ext.at[pl.ds(pl.multiple_of(16 + p * ROWS + first, 16), count)]

    def w_part(rows_from, count, y):
        return wt.at[
            pl.ds(pl.multiple_of(rows_from, 64), count), pl.ds(pl.multiple_of(y * COLS, COLS), COLS)
        ]

    def dt_window(p):
        return dt_in.at[pl.ds(pl.multiple_of(8 * lax.div(5 * p, 2), 8), 24)]

    local = {}

    def copy_here(name, src, dst):
        local[name] = pltpu.make_async_copy(src, dst, sl.at[8 + len(local)])
        local[name].start()

    copy_here("cot", cot_in, cot)
    copy_here("up", up_in, up)
    copy_here("step_bias", step_bias_in, head_par.at[0])
    copy_here("rate", rate_in, head_par.at[1])
    copy_here("skip", skip_in, head_par.at[2])
    copy_here("bc", bc_in, bc_rows(t, 0, ROWS))
    copy_here("dt", dt_window(t), dt_all.at[t])
    copy_here("taps_x", taps_in.at[:, columns(t)], taps_x)
    copy_here("taps_bc", taps_in.at[:, pl.ds(4 * WIDTH, 256)], taps_bc)
    copy_here("bias", bias_in, bias)
    copy_here("x", x_in.at[:, columns(t)], x_rows(t, 0, ROWS))
    copy_here("gain", gain_in, gain_rows)
    copy_here("down", down_in, down_t)
    copy_here("gate", z_in.at[:, columns(t)], gate.at[t])
    copy_here("w", w_in, w_part(0, 1280, s))

    def head_mask(i, carry):
        head = lax.broadcasted_iota(jnp.int32, (256, 128), 0)
        head = jnp.where(head >= 128, head - 128, head)
        lane = lax.broadcasted_iota(jnp.int32, (256, 128), 1)
        own_head = 2 * i + jnp.where(lane >= 64, 1, 0)
        spread[:, tile(i)] = jnp.where(head == own_head, 1.0, 0.0).astype(BF16)
        return carry

    lax.fori_loop(0, 10, head_mask, 0)

    def widen(v):
        high = v.astype(BF16)
        low = (v - high.astype(F32)).astype(BF16)
        return dot(jnp.concatenate([high, low], axis=1), spread[...])

    scale = 2.0 / (TOKENS ** 0.5)

    local["cot"].wait()
    local["up"].wait()
    gt[t] = dot(up[...], cot[...], NT) * scale

    gives_rim = jnp.logical_and(t == 3, c < 15)

    @pl.when(gives_rim)
    def _():
        pl.semaphore_wait(barrier, 25)

    @pl.when(jnp.logical_not(gives_rim))
    def _():
        pl.semaphore_wait(barrier, 21)

    def far_start(src, relay, name):
        send(src.at[pl.ds(0, 64), columns(far)], relay.at[0], name + "0", {"tensor": right})
        send(src.at[pl.ds(64, 64), columns(far)], relay.at[1], name + "1", {"tensor": left})

    def near_start(src, rows, name):
        send(src.at[:, columns(right)], rows(t, 0, ROWS), name + "2", {"tensor": right})
        send(src.at[:, columns(left)], rows(t, 0, ROWS), name + "3", {"tensor": left})

    def far_forward(rows, relay, name):
        arrived(relay.at[0], name + "0")
        send(relay.at[0], rows(left, 0, 64), name + "4", {"tensor": right})
        arrived(relay.at[1], name + "1")
        send(relay.at[1], rows(right, 64, 64), name + "5", {"tensor": left})

    def near_wait(rows, name):
        arrived(rows(left, 0, ROWS), name + "2")
        arrived(rows(right, 0, ROWS), name + "3")

    def far_wait(rows, name):
        arrived(rows(far, 0, 64), name + "4")
        arrived(rows(far, 64, 64), name + "5")

    def rim_copies():
        copies = []
        for p in range(4):
            where = {"context_0": lax.div(after, 2), "context_1": lax.rem(after, 2), "tensor": p}
            copies.append(pltpu.make_async_remote_copy(
                src_ref=x_in.at[pl.ds(120, 8), pl.ds(p * WIDTH, WIDTH)], dst_ref=rim_x,
                send_sem=sl.at[p], recv_sem=rx.at[slot("rim_x")], device_id=where, device_id_type=MESH))
            copies.append(pltpu.make_async_remote_copy(
                src_ref=bc_in.at[pl.ds(120, 8)], dst_ref=rim_b,
                send_sem=sl.at[4 + p], recv_sem=rx.at[slot("rim_b")], device_id=where, device_id_type=MESH))
        return copies

    @pl.when(gives_rim)
    def _():
        for copy in rim_copies():
            copy.start()

    far_start(x_in, xr, "x")
    send(bc_in.at[pl.ds(0, 64)], bc_rows(t, 0, 64), "b0", {"tensor": right})
    send(bc_in.at[pl.ds(64, 64)], bc_rows(t, 64, 64), "b1", {"tensor": left})
    send(bc_in.at[pl.ds(64, 64)], bc_rows(t, 64, 64), "b2", {"tensor": right})
    send(bc_in.at[pl.ds(0, 64)], bc_rows(t, 0, 64), "b3", {"tensor": left})
    for j in (1, 3, 2):
        peer = lax.rem(t + j, 4)
        send(dt_window(peer), dt_all.at[t], "dt%d" % j, {"tensor": peer})
    near_start(x_in, x_rows, "x")

    @pl.when(c == 0)
    def _():
        x_ext[0:16, :] = jnp.zeros((16, WIDTH), BF16)
        bc_ext[0:16, :] = jnp.zeros((16, 256), BF16)

    mine, other = k * 640, (1 - k) * 640

    def w_src(first):
        return w_in.at[pl.ds(pl.multiple_of(mine + first, 64), 320)]

    send(w_src(0), w_part(mine, 320, s), "w0", {"fsdp": up_y})
    send(w_src(320), w_part(mine + 320, 320, s), "w1", {"fsdp": down_y})
    send(w_src(320), w_part(mine + 320, 320, s), "w2", {"fsdp": up_y})
    send(w_src(0), w_part(mine, 320, s), "w3", {"fsdp": down_y})

    for name in ("step_bias", "rate", "skip", "bc", "dt", "taps_x", "taps_bc", "bias", "x", "gain", "down"):
        local[name].wait()
    pick20 = jnp.where(
        lax.broadcasted_iota(jnp.int32, (HEADS, 128), 0) == lax.broadcasted_iota(jnp.int32, (HEADS, 128), 1), 1.0, 0.0)

    def head_row(i):
        return dot(jnp.broadcast_to(head_par[i], (8, HEADS)), pick20, precision=lax.Precision.HIGHEST)

    step_bias = head_row(0)[0:1, :]
    rate = jnp.exp(head_row(1))[0:1, :]
    skip[...] = widen(head_row(2))
    for i in range(10):
        gain[:, i * 128 : i * 128 + 128] = gain_rows[i : i + 1, :]

    for j in range(1, 4):
        arrived(dt_all.at[lax.rem(t + 4 - j, 4)], "dt%d" % j)

    row = lax.broadcasted_iota(jnp.int32, (128, 128), 0)
    col = lax.broadcasted_iota(jnp.int32, (128, 128), 1)
    causal = row >= col
    tri = jnp.where(causal, 1.0, 0.0)
    pick_row = lax.broadcasted_iota(jnp.int32, (24, 128), 0)
    pick_col = lax.broadcasted_iota(jnp.int32, (24, 128), 1)
    hit = jnp.logical_and(pick_row == pick_col + 4 * lax.rem(t, 2), pick_col < HEADS)
    pick = jnp.where(hit, 1.0, 0.0).astype(BF16)

    total = jnp.zeros((1, 128), F32)
    for p in range(4):
        raw = dot(dt_all[p], pick, TN) + step_bias
        step_now = jnp.maximum(raw, 0.0) + jnp.log1p(jnp.exp(-jnp.abs(raw)))
        cum_now = dot(tri, -step_now * rate, precision=lax.Precision.HIGHEST)
        step[p] = step_now
        cum[p] = cum_now
        log_start[p] = jnp.broadcast_to(total, (8, 128))
        total = total + cum_now[127:128, :]
    for p in range(4):
        log_tail[p] = total - log_start[p] - cum[p, 127:128, :]
        kept[p] = widen(jnp.broadcast_to(jnp.exp(cum[p, 127:128, :]), (8, 128)))
    dec_all[c] = jnp.broadcast_to(jnp.exp(total), (8, 128))

    arrived(bc_rows(left, 0, 64), "b0")
    send(bc_rows(left, 0, 64), bc_rows(left, 0, 64), "b4", {"tensor": right})
    arrived(bc_rows(right, 64, 64), "b1")
    send(bc_rows(right, 64, 64), bc_rows(right, 64, 64), "b5", {"tensor": left})
    def x_lanes(p, first, half):
        return x_ext.at[
            pl.ds(pl.multiple_of(16 + p * ROWS + first, 16), 64), pl.ds(half * 640, 640)]

    arrived(xr.at[0], "x0")
    arrived(xr.at[1], "x1")
    for half in range(2):
        lanes = pl.ds(half * 640, 640)
        send(xr.at[0, :, lanes], x_lanes(left, 0, half), "x4%d" % half, {"tensor": right})
        send(xr.at[1, :, lanes], x_lanes(right, 64, half), "x5%d" % half, {"tensor": left})
    far_start(z_in, zr, "z")
    near_start(z_in, z_rows, "z")

    def decay_copy(j):
        return pltpu.make_async_remote_copy(
            src_ref=dec_all.at[c], dst_ref=dec_all.at[c],
            send_sem=sd, recv_sem=rd, device_id=context_peer(j), device_id_type=MESH)

    exchange(decay_copy)
    for j in range(1, 4):
        send(gt.at[t], gt.at[t], "g%d" % j, {"tensor": lax.rem(t + j, 4)})

    def convolved(ext, p, lanes, taps, bias_row):
        v = ext[pl.ds(pl.multiple_of(p * ROWS, 16), ROWS + 16), lanes].astype(F32)
        acc = bias[pl.ds(bias_row, 1), :] + taps[0:1, lanes] * pltpu.roll(v, 3, 0)
        acc = acc + taps[1:2, lanes] * pltpu.roll(v, 2, 0)
        acc = acc + taps[2:3, lanes] * pltpu.roll(v, 1, 0)
        acc = acc + taps[3:4, lanes] * v
        return silu(acc[16:]).astype(BF16)

    @pl.when(c > 0)
    def _():
        arrived(rim_x, "rim_x")
        arrived(rim_b, "rim_b")
        x_ext[0:16, :] = jnp.concatenate([rim_x[...], rim_x[...]], axis=0)
        bc_ext[0:16, :] = jnp.concatenate([rim_b[...], rim_b[...]], axis=0)

    state[...] = jnp.zeros((STATE, WIDTH), F32)

    def shared(i, carry):
        p = lax.rem(t + i, 4)
        for half in range(2):
            bcc[p, :, pl.ds(half * 128, 128)] = convolved(bc_ext, p, pl.ds(half * 128, 128), taps_bc, 40 + half)
        return carry

    def block(first, count):
        def of(i, carry):
            p = lax.rem(t + i, 4)
            lanes = pl.ds(first * 128, count * 128)

            def lanes_of(j, inner):
                xc[p, :, tile(j)] = convolved(x_ext, p, tile(j), taps_x, 10 * t + j)
                return inner

            lax.fori_loop(first, first + count, lanes_of, 0)
            scaled = (xc[p, :, lanes].astype(F32) * weights[p, :, lanes]).astype(BF16)
            fresh = dot(bcc[p, :, 0:128], scaled, TN)
            blocks[p, :, lanes] = fresh
            state[:, lanes] = state[:, lanes] + tails[p, 0:1, lanes] * fresh
            return carry

        return of

    def weigh(p, carry):
        cum_now = cum[p]
        weights[p] = widen(step[p] * jnp.exp(cum_now[127:128, :] - cum_now))
        tails[p] = widen(jnp.exp(log_tail[p]))
        return carry

    lax.fori_loop(0, 4, weigh, 0)
    arrived(w_part(mine, 320, down_y), "w0")
    send(w_part(mine, 320, down_y), w_part(mine, 320, down_y), "w4", {"fsdp": up_y})
    arrived(w_part(mine + 320, 320, up_y), "w1")
    send(w_part(mine + 320, 320, up_y), w_part(mine + 320, 320, up_y), "w5", {"fsdp": down_y})
    arrived(bc_rows(left, 64, 64), "b2")
    arrived(bc_rows(right, 0, 64), "b3")
    lax.fori_loop(0, 2, shared, 0)
    near_wait(x_rows, "x")
    lax.fori_loop(0, 2, block(0, 10), 0)
    arrived(bc_rows(far, 0, 64), "b4")
    arrived(bc_rows(far, 64, 64), "b5")
    lax.fori_loop(2, 4, shared, 0)
    for half in range(2):
        arrived(x_lanes(far, 0, half), "x4%d" % half)
        arrived(x_lanes(far, 64, half), "x5%d" % half)
        lax.fori_loop(2, 4, block(5 * half, 5), 0)

    core = {"context_1": 1 - k}

    def half_lanes(i):
        return pl.ds(pl.multiple_of(i * 640, 640), 640)

    send(state.at[:, half_lanes(1 - k)], peer_state, "pair", core)
    settle(dec_all, rd)
    dec_wide[...] = widen(dec_all[...].reshape(128, 128))
    arrived(peer_state, "pair")

    def chip_decay(of):
        return dec_wide[pl.ds(pl.multiple_of(16 * of, 16), 8), half_lanes(k)] * dec_wide[
            pl.ds(pl.multiple_of(16 * of + 8, 8), 8), half_lanes(k)]

    decay_second = dec_wide[pl.ds(pl.multiple_of(16 * z + 8, 8), 8), half_lanes(k)][0:1, :]
    weight_mine = jnp.where(k == 0, decay_second, jnp.ones_like(decay_second))
    weight_peer = jnp.where(k == 0, jnp.ones_like(decay_second), decay_second)

    def pack_state(i, carry):
        rows = pl.ds(pl.multiple_of(i * 16, 16), 16)
        both = weight_mine * state[rows, half_lanes(k)] + weight_peer * peer_state[rows, :]
        st_send[i] = both.astype(BF16)
        return carry

    lax.fori_loop(0, 8, pack_state, 0)

    def state_copy(j):
        return pltpu.make_async_remote_copy(
            src_ref=st_send.at[chip_at(j - 1)], dst_ref=st_recv.at[z],
            send_sem=sc, recv_sem=rc_, device_id=chip_peer(j), device_id_type=MESH)

    exchange(state_copy, 8)
    st_recv[z] = st_send[z]

    arrived(w_part(mine + 320, 320, down_y), "w2")
    send(w_part(mine, 640, down_y), w_part(mine, 640, down_y), "w6", core)
    arrived(w_part(mine, 320, up_y), "w3")
    send(w_part(mine, 640, up_y), w_part(mine, 640, up_y), "w7", core)
    far_forward(z_rows, zr, "z")

    def inside(p, carry):
        b_now, c_now = bcc[p, :, 0:128], bcc[p, :, 128:256]
        gram = dot(c_now, b_now, NT)
        cum_now = cum[p]
        shifted = (cum_now - jnp.log(step[p])).T
        lane = lax.broadcasted_iota(jnp.int32, (1, 128), 1)
        low = jnp.where(lane < 64, 1.0, 0.0)
        for q in range(HEADS // 2):
            mats = []
            for h in (2 * q, 2 * q + 1):
                gap = cum_now[:, h : h + 1] - shifted[h : h + 1, :]
                mats.append(jnp.exp(jnp.where(causal, gap, -1e30)) * gram)
            both = jnp.concatenate(mats, axis=1).astype(BF16)
            x_pair = xc[p, :, pl.ds(q * 128, 128)].astype(F32)
            x_two = jnp.concatenate([x_pair * low, x_pair * (1.0 - low)], axis=0).astype(BF16)
            y_in[p, :, pl.ds(q * 128, 128)] = dot(both, x_two) + x_pair * skip[0:1, pl.ds(q * 128, 128)]
        return carry

    lax.fori_loop(0, 4, inside, 0)

    settle(st_recv, rc_, 7)

    def chain(i, held):
        back_send[i] = held.astype(BF16)
        return chip_decay(i)[0:1, :] * held + st_recv[i].astype(F32)

    lax.fori_loop(0, 8, chain, jnp.zeros((16, 640), F32))

    def back_copy(j):
        return pltpu.make_async_remote_copy(
            src_ref=back_send.at[chip_at(j - 1)], dst_ref=back_recv.at[z],
            send_sem=sb, recv_sem=rb, device_id=chip_peer(j), device_id_type=MESH)

    exchange(back_copy, 8)
    back_recv[z] = back_send[z]

    def starts(j, carry):
        held = jnp.zeros((STATE, 128), F32)
        for p in range(4):
            fresh = blocks[p, :, tile(j)]
            blocks[p, :, tile(j)] = held
            held = kept[p, 0:1, tile(j)] * held + fresh
        return carry

    lax.fori_loop(0, 10, starts, 0)

    arrived(w_part(mine, 320, far_y), "w4")
    arrived(w_part(mine + 320, 320, far_y), "w5")
    send(w_part(mine, 640, far_y), w_part(mine, 640, far_y), "w8", core)

    local["gate"].wait()
    near_wait(z_rows, "z")
    far_wait(z_rows, "z")
    settle(back_recv, rb, 7)

    decay_first = dec_wide[pl.ds(pl.multiple_of(16 * z, 8), 8), half_lanes(k)][0:1, :]

    def unpack_state(i, carry):
        rows = pl.ds(pl.multiple_of(i * 16, 16), 16)
        first = back_recv[i].astype(F32)
        span = jnp.where(k == 0, state[rows, half_lanes(k)], peer_state[rows, :])
        second = decay_first * first + span
        s_in[rows, half_lanes(k)] = jnp.where(k == 0, first, second)
        in_send[rows, :] = jnp.where(k == 0, second, first).astype(BF16)
        return carry

    lax.fori_loop(0, 8, unpack_state, 0)
    send(in_send, in_recv, "in", core)

    local["w"].wait()
    arrived(w_part(other, 640, down_y), "w6")
    arrived(w_part(other, 640, up_y), "w7")
    arrived(w_part(other, 640, far_y), "w8")
    arrived(in_recv, "in")
    s_in[:, half_lanes(1 - k)] = in_recv[...].astype(F32)

    def finish(i, carry):
        p = lax.rem(t + i, 4)
        start = blocks[p] + widen(jnp.exp(log_start[p]))[0:1, :] * s_in[...]
        reach = widen(jnp.exp(cum[p]))
        y_now = y_in[p] + reach * dot(bcc[p, :, 128:256], start.astype(BF16))
        now = y_now * silu(gate[p].astype(F32))
        squares = (now * now).astype(BF16)
        sq[t, pl.ds(p, 1), :] = dot(jnp.ones((8, WIDTH), BF16), squares, NT)[0:1, :]
        out = (now * gain[...]).astype(BF16)
        gated[p] = out
        ap_send[p] = dot(down_t[...], out, NT)
        return carry

    def project(p, half, store, first=0, count=5):
        def piece(i, carry):
            lanes = pl.ds(pl.multiple_of(i * 256, 256), 256)
            lanes_w = pl.ds(pl.multiple_of(half * HALF + i * 256, 256), 256)
            store(lanes, dot(gated[p], wt[:, lanes_w]))
            return carry

        lax.fori_loop(first, first + count, piece, 0)

    def to_slot(which, extra=None):
        def store(lanes, v):
            if extra is not None:
                v = v + rs_recv[extra, :, lanes].astype(F32)
            rs_send[which, :, lanes] = v.astype(BF16)

        return store

    def piece_at(ref, which, i):
        return ref.at[which, :, pl.ds(i * 256, 256)]

    def ship(which, where, i):
        pltpu.make_async_remote_copy(
            src_ref=piece_at(rs_send, which, i), dst_ref=piece_at(rs_recv, which, i),
            send_sem=sr, recv_sem=rr.at[5 * which + i] if which < 2 else rr_end.at[which - 2],
            device_id={"tensor": where}, device_id_type=MESH).start()

    def landed(which, i):
        piece = piece_at(rs_recv, which, i)
        pltpu.make_async_copy(piece, piece, rr.at[5 * which + i]).wait()

    lax.fori_loop(2, 3, finish, 0)
    for i in range(5):
        project(far, 0, to_slot(0), i, 1)
        project(far, 1, to_slot(1), i, 1)
        if i < 3:
            ship(0, right, i)
            ship(1, left, i)
    lax.fori_loop(3, 6, finish, 0)
    ap_recv[t] = ap_send[t]
    for j in (2, 1, 3):
        peer = lax.rem(t + j, 4)
        send(sq.at[t], sq.at[t], "q%d" % j, {"tensor": peer})
        send(ap_send.at[peer], ap_recv.at[t], "a%d" % j, {"tensor": peer})
    for i in range(3, 5):
        ship(0, right, i)
        ship(1, left, i)
    for i in range(5):
        project(right, 1, to_slot(2), i, 1)
        ship(2, right, i)
        project(left, 0, to_slot(3), i, 1)
        ship(3, left, i)

    for j in range(1, 4):
        source = lax.rem(t + 4 - j, 4)
        arrived(gt.at[source], "g%d" % j)
        arrived(sq.at[source], "q%d" % j)
        arrived(ap_recv.at[source], "a%d" % j)

    def row_scale(p):
        rows = pl.ds(p, 1)
        squares = (sq[0, rows, :] + sq[1, rows, :]) + (sq[2, rows, :] + sq[3, rows, :])
        return lax.rsqrt(squares * (1.0 / 5120.0) + EPS)

    adapter = ((ap_recv[0] + ap_recv[1]) + (ap_recv[2] + ap_recv[3])).astype(BF16)
    own_scale = row_scale(t)
    weighted = (scale * own_scale[0:1, :] * adapter.astype(F32)).astype(BF16)
    grad_a_now = jnp.zeros((RANK, WIDTH), F32)
    for p in range(4):
        rows_grad = (row_scale(p)[0:1, :] * gt[p]).astype(BF16)
        grad_a_now = grad_a_now + dot(rows_grad, gated[p])
    grad_b_now = dot(weighted, cot[...])
    for i in range(30):
        v_send[i // 2, i % 2] = (
            grad_a_now[:, i * 128 : i * 128 + 128] if i < 10
            else grad_b_now[:, (i - 10) * 128 : (i - 10) * 128 + 128]).astype(BF16)
    v_send[15] = jnp.zeros((2, RANK, 128), BF16)
    v_recv[c] = v_send[c]

    def v_copy(j):
        return pltpu.make_async_remote_copy(
            src_ref=v_send.at[context_index(j)], dst_ref=v_recv.at[c],
            send_sem=sv, recv_sem=rv, device_id=context_peer(j), device_id_type=MESH)

    exchange(v_copy)

    for i in range(1):
        landed(0, i)
        project(right, 0, to_slot(4, 0), i, 1)
        ship(4, right, i)
        landed(1, i)
        project(left, 1, to_slot(5, 1), i, 1)
        ship(5, left, i)

    settle(v_recv, rv)

    def add_v(i, held):
        return held + v_recv[i].astype(F32)

    y_recv[s] = lax.fori_loop(0, 16, add_v, jnp.zeros((2, RANK, 128), F32))
    for j in range(1, 4):
        send(y_recv.at[s], y_recv.at[s], "y%d" % j, {"fsdp": lax.rem(s + j, 4)})
    for i in range(1, 5):
        landed(0, i)
        project(right, 0, to_slot(4, 0), i, 1)
        landed(1, i)
        project(left, 1, to_slot(5, 1), i, 1)
    for j in range(1, 4):
        arrived(y_recv.at[lax.rem(s + 4 - j, 4)], "y%d" % j)
    t_recv[t] = ((y_recv[0] + y_recv[1]) + (y_recv[2] + y_recv[3])).astype(BF16)
    for j in range(1, 4):
        send(t_recv.at[t], t_recv.at[t], "t%d" % j, {"tensor": lax.rem(t + j, 4)})
    for i in range(1, 5):
        ship(4, right, i)
        ship(5, left, i)

    def own_part(half):
        def store(lanes, v):
            lanes_up = pl.ds(pl.multiple_of(half * HALF + lanes.start, 256), 256)
            own[half, :, lanes] = v + 2.0 * dot(adapter, up[:, lanes_up], TN)

        return store

    project(t, 0, own_part(0))
    project(t, 1, own_part(1))

    for j in range(1, 4):
        arrived(t_recv.at[lax.rem(t + 4 - j, 4)], "t%d" % j)

    def add_t(i, held):
        keep = jnp.where(jnp.logical_or(c >= 5, i == t), 1.0, 0.0)
        return held + keep * t_recv[i].astype(F32)

    v_all[c] = lax.fori_loop(0, 4, add_t, jnp.zeros((2, RANK, 128), F32)).astype(BF16)

    def all_copy(j):
        return pltpu.make_async_remote_copy(
            src_ref=v_all.at[c], dst_ref=v_all.at[c],
            send_sem=sg, recv_sem=rg, device_id=context_peer(j), device_id_type=MESH)

    exchange(all_copy)

    scale_col = jnp.broadcast_to(own_scale[0:1, :], (128, 128)).T
    for which in range(2, 6):
        pltpu.make_async_copy(rs_recv.at[which], rs_recv.at[which], rr_end.at[which - 2]).wait()

    def close(i, carry):
        lanes = tile(i)
        first = own[0, :, lanes] + rs_recv[4, :, lanes].astype(F32) + rs_recv[3, :, lanes].astype(F32)
        second = own[1, :, lanes] + rs_recv[2, :, lanes].astype(F32) + rs_recv[5, :, lanes].astype(F32)
        mixed_here[:, lanes] = (scale_col * first).astype(BF16)
        mixed_here[:, pl.ds(pl.multiple_of(HALF + i * 128, 128), 128)] = (scale_col * second).astype(BF16)
        return carry

    lax.fori_loop(0, 10, close, 0)
    copy_here("mixed", mixed_here, mixed)

    settle(v_all, rg)
    for i in range(10):
        a_here[:, i * 128 : i * 128 + 128] = v_all[i // 2, i % 2].astype(F32)
    for i in range(20):
        b_here[:, i * 128 : i * 128 + 128] = v_all[5 + i // 2, i % 2].astype(F32)
    copy_here("grad_a", a_here, grad_a)
    copy_here("grad_b", b_here, grad_b)

    settle(dec_all, sd)
    settle(st_send, sc, 7)
    settle(back_send, sb, 7)
    settle(v_send, sv)
    settle(v_all, sg)
    pltpu.make_async_copy(rs_send, rs_send, sr).wait()
    for copy in started:
        copy.wait_send()

    @pl.when(gives_rim)
    def _():
        for copy in rim_copies():
            copy.wait_send()

    for name in ("mixed", "grad_a", "grad_b"):
        local[name].wait()


def shards(
    input_raw, state_proj_raw, gate_branch, step_raw, convolution_taps, convolution_bias, step_bias,
    decay_log_rate, skip_weight, gated_norm_gain, output_weight, adapter_down, adapter_up, cotangent,
):
    hbm = pl.BlockSpec(memory_space=pl.ANY)
    dma = pltpu.SemaphoreType.DMA
    mixed, grad_a, grad_b = pl.pallas_call(
        kernel,
        out_shape=(
            jax.ShapeDtypeStruct((ROWS, OUT), BF16),
            jax.ShapeDtypeStruct((RANK, WIDTH), F32),
            jax.ShapeDtypeStruct((RANK, OUT), F32),
        ),
        in_specs=[hbm] * 14,
        out_specs=(hbm, hbm, hbm),
        scratch_shapes=[
            pltpu.VMEM((16 + 512, WIDTH), BF16),
            pltpu.VMEM((2, 64, WIDTH), BF16),
            pltpu.VMEM((8, WIDTH), BF16),
            pltpu.VMEM((8, 256), BF16),
            pltpu.VMEM((4, ROWS, WIDTH), BF16),
            pltpu.VMEM((16 + 512, 256), BF16),
            pltpu.VMEM((4, ROWS, 256), BF16),
            pltpu.VMEM((4, 24, 128), BF16),
            pltpu.VMEM((4, ROWS, WIDTH), BF16),
            pltpu.VMEM((2, 64, WIDTH), BF16),
            pltpu.VMEM((WIDTH, OUT), BF16),
            pltpu.VMEM((ROWS, OUT), BF16),
            pltpu.VMEM((4, WIDTH), F32),
            pltpu.VMEM((4, 256), F32),
            pltpu.VMEM((42, 128), F32),
            pltpu.VMEM((3, 1, HEADS), F32),
            pltpu.VMEM((10, 128), F32),
            pltpu.VMEM((1, WIDTH), F32),
            pltpu.VMEM((RANK, WIDTH), BF16),
            pltpu.VMEM((RANK, OUT), BF16),
            pltpu.VMEM((8, WIDTH), F32),
            pltpu.VMEM((4, ROWS, WIDTH), F32),
            pltpu.VMEM((4, 8, WIDTH), F32),
            pltpu.VMEM((256, WIDTH), BF16),
            pltpu.VMEM((4, ROWS, 128), F32),
            pltpu.VMEM((4, ROWS, 128), F32),
            pltpu.VMEM((4, 8, 128), F32),
            pltpu.VMEM((4, 8, 128), F32),
            pltpu.VMEM((4, ROWS, WIDTH), F32),
            pltpu.VMEM((4, STATE, WIDTH), F32),
            pltpu.VMEM((4, 8, WIDTH), F32),
            pltpu.VMEM((STATE, WIDTH), F32),
            pltpu.VMEM((STATE, 640), F32),
            pltpu.VMEM((8, 16, 640), BF16),
            pltpu.VMEM((8, 16, 640), BF16),
            pltpu.VMEM((16, 8, 128), F32),
            pltpu.VMEM((128, WIDTH), F32),
            pltpu.VMEM((8, 16, 640), BF16),
            pltpu.VMEM((8, 16, 640), BF16),
            pltpu.VMEM((STATE, 640), BF16),
            pltpu.VMEM((STATE, 640), BF16),
            pltpu.VMEM((STATE, WIDTH), F32),
            pltpu.VMEM((4, ROWS, WIDTH), BF16),
            pltpu.VMEM((4, RANK, 128), F32),
            pltpu.VMEM((4, 8, 128), F32),
            pltpu.VMEM((4, RANK, 128), F32),
            pltpu.VMEM((4, RANK, 128), F32),
            pltpu.VMEM((6, ROWS, HALF), BF16),
            pltpu.VMEM((6, ROWS, HALF), BF16),
            pltpu.VMEM((2, ROWS, HALF), F32),
            pltpu.VMEM((16, 2, RANK, 128), BF16),
            pltpu.VMEM((16, 2, RANK, 128), BF16),
            pltpu.VMEM((4, 2, RANK, 128), F32),
            pltpu.VMEM((4, 2, RANK, 128), BF16),
            pltpu.VMEM((16, 2, RANK, 128), BF16),
            pltpu.VMEM((ROWS, OUT), BF16),
            pltpu.VMEM((RANK, WIDTH), F32),
            pltpu.VMEM((RANK, OUT), F32),
            dma((60,)), dma((60,)), dma((26,)),
            dma, dma, dma, dma, dma, dma, dma, dma, dma, dma, dma, dma((10,)), dma((4,)),
        ],
        compiler_params=pltpu.CompilerParams(
            collective_id=0, has_side_effects=True, vmem_limit_bytes=64 * 1000 * 1000),
    )(
        input_raw[0], state_proj_raw[0], gate_branch[0], step_raw[0].T, output_weight, cotangent[0],
        convolution_taps, convolution_bias.reshape(42, 128), step_bias[None, :], decay_log_rate[None, :],
        skip_weight[None, :], gated_norm_gain.reshape(10, 128), adapter_down.T, adapter_up,
    )
    return (mixed[None], grad_a.T, grad_b)


def solution(mesh):
    torus = Mesh(
        mesh.devices.reshape(8, 2, mesh.shape["tensor"], mesh.shape["fsdp"]),
        ("context_0", "context_1", "tensor", "fsdp"),
    )
    tokens = P("fsdp", CONTEXT_TENSOR, None)
    return jax.shard_map(
        shards,
        mesh=torus,
        in_specs=(
            tokens, tokens, tokens, tokens, P(), P(), P("tensor"), P("tensor"), P("tensor"), P("tensor"),
            P("tensor", "fsdp"), P("tensor", None), P(), tokens,
        ),
        out_specs=(tokens, P("tensor", None), P()),
        check_vma=False,
    )
```

```python
import functools

import jax
import jax.numpy as jnp
from jax import lax
from jax.experimental import pallas as pl
from jax.experimental.pallas import tpu as pltpu
from jax.sharding import Mesh
from jax.sharding import PartitionSpec as P

MESH = pl.DeviceIdType.MESH
CONTEXT_TENSOR = ("context_0", "context_1", "tensor")
F32 = jnp.float32
BF16 = jnp.bfloat16

ROWS = 128
WIDTH = 1280
STATE = 128
OUT = 2560
HALF = 1280
RANK = 16
HEADS = 20
COLS = 640
TOKENS = 32768
EPS = 1e-05

NT = (((1,), (1,)), ((), ()))
TN = (((0,), (0,)), ((), ()))


def silu(v):
    half = 0.5 * v
    return half + half * jnp.tanh(half)


def dot(a, b, dims=(((1,), (0,)), ((), ())), precision=None):
    return lax.dot_general(a, b, dims, precision=precision, preferred_element_type=F32)


def kernel(
    x_in, bc_in, z_in, dt_in, w_in, cot_in, taps_in, bias_in, step_bias_in, rate_in, skip_in, gain_in, down_in, up_in,
    mixed, grad_a, grad_b,
    x_ext, xr, rim_x, rim_b, xc, bc_ext, bcc, dt_all, gate, zr, wt, cot,
    taps_x, taps_bc, bias, head_par, gain_rows, gain, down_t, up, skip, weights, tails,
    spread, step, cum, log_start, log_tail, y_in, blocks, kept, state, peer_state,
    st_send, st_recv, dec_all, dec_wide, back_send, back_recv, in_send, s_in,
    gated, gt, sq, ap_send, ap_recv,
    rs_send, rs_recv, own,
    v_send, v_recv, y_recv, t_recv, v_all, mixed_here, a_here, b_here,
    sx, rx, sl, sc, rc_, sd, rd, sb, rb, sv, rv, sg, rg, sr, rr, rr_end, sgroup, s3, r3, s_head,
):
    z, k = lax.axis_index("context_0"), lax.axis_index("context_1")
    t, s = lax.axis_index("tensor"), lax.axis_index("fsdp")
    c = 2 * z + k
    right, left, far = lax.rem(t + 1, 4), lax.rem(t + 3, 4), lax.rem(t + 2, 4)
    up_y, down_y, far_y = lax.rem(s + 1, 4), lax.rem(s + 3, 4), lax.rem(s + 2, 4)
    started = []
    slots, send_slots = {}, {}

    def slot(name):
        return slots.setdefault(name, len(slots))

    def send_slot(name):
        return send_slots.setdefault(name, len(send_slots))

    groups = {"x": 0, "z": 1, "w": 2}

    def send(src, dst, name, where):
        grouped = groups.get(name[0])
        copy = pltpu.make_async_remote_copy(
            src_ref=src, dst_ref=dst,
            send_sem=sx.at[send_slot(name)] if grouped is None else sgroup.at[grouped],
            recv_sem=rx.at[slot(name)], device_id=where, device_id_type=MESH,
        )
        copy.start()
        if groups.get(name[0]) is None:
            started.append(copy)

    def send_triple(make, which):
        for j in (2, 1, 3):
            src, dst, where = make(j)
            pltpu.make_async_remote_copy(
                src_ref=src, dst_ref=dst, send_sem=s3.at[which], recv_sem=r3.at[which],
                device_id=where, device_id_type=MESH).start()

    def tensor_peer(j):
        return lax.rem(t + j, 4)

    def arrived(dst, name):
        pltpu.make_async_copy(dst, dst, rx.at[slot(name)]).wait()

    def chip_at(i):
        step_now = lax.div(i + 1, 2)
        return lax.rem(z + 4 + (1 - 2 * lax.rem(i, 2)) * step_now, 8)

    def core_at(j):
        return lax.rem(k + j, 2)

    def context_index(j):
        return 2 * chip_at(lax.div(j - 1, 2)) + core_at(j)

    def context_peer(j):
        return {"context_0": chip_at(lax.div(j - 1, 2)), "context_1": core_at(j)}

    def chip_peer(j):
        return {"context_0": chip_at(j - 1)}

    def exchange(make, how_many=16):
        def go(j, carry):
            make(j).start()
            return carry

        lax.fori_loop(1, how_many, go, 0)

    def settle(several, sem):
        pltpu.make_async_copy(several, several, sem).wait()

    def tile(i):
        return pl.ds(pl.multiple_of(i * 128, 128), 128)

    barrier = pltpu.get_barrier_semaphore()

    def greet(j, carry):
        pl.semaphore_signal(barrier, inc=1, device_id=context_peer(j), device_id_type=MESH)
        return carry

    for j in range(1, 4):
        pl.semaphore_signal(barrier, inc=1, device_id={"tensor": lax.rem(t + j, 4)}, device_id_type=MESH)
        pl.semaphore_signal(barrier, inc=1, device_id={"fsdp": lax.rem(s + j, 4)}, device_id_type=MESH)
    lax.fori_loop(1, 16, greet, 0)
    before = lax.rem(c + 15, 16)
    after = lax.rem(c + 1, 16)

    @pl.when(c > 0)
    def _():
        pl.semaphore_signal(
            barrier, inc=1,
            device_id={"context_0": lax.div(before, 2), "context_1": lax.rem(before, 2), "tensor": 3},
            device_id_type=MESH,
        )

    def columns(p):
        return pl.ds(pl.multiple_of(p * WIDTH, WIDTH), WIDTH)

    def x_rows(p, first, count):
        return x_ext.at[pl.ds(pl.multiple_of(16 + p * ROWS + first, 16), count)]

    def z_rows(p, first, count):
        return gate.at[p, pl.ds(first, count)]

    def bc_rows(p, first, count):
        return bc_ext.at[pl.ds(pl.multiple_of(16 + p * ROWS + first, 16), count)]

    def b_lanes(p, first):
        return bc_ext.at[pl.ds(pl.multiple_of(16 + p * ROWS + first, 16), 64), pl.ds(0, 128)]

    def c_lanes(p, first):
        return bc_ext.at[pl.ds(pl.multiple_of(16 + p * ROWS + first, 16), 64), pl.ds(128, 128)]

    def w_part(rows_from, count, y):
        return wt.at[
            pl.ds(pl.multiple_of(rows_from, 64), count), pl.ds(pl.multiple_of(y * COLS, COLS), COLS)
        ]

    def dt_window(p):
        return dt_in.at[pl.ds(pl.multiple_of(8 * lax.div(5 * p, 2), 8), 24)]

    local = {}

    def copy_here(name, src, dst):
        local[name] = pltpu.make_async_copy(src, dst, sl.at[8 + len(local)])
        local[name].start()

    copy_here("cot", cot_in, cot)
    copy_here("up", up_in, up)
    for i, source in enumerate((step_bias_in, rate_in, skip_in)):
        pltpu.make_async_copy(source, head_par.at[i], s_head).start()
    copy_here("bc", bc_in, bc_rows(t, 0, ROWS))
    copy_here("dt", dt_window(t), dt_all.at[t])
    copy_here("taps_x", taps_in.at[:, columns(t)], taps_x)
    copy_here("taps_bc", taps_in.at[:, pl.ds(4 * WIDTH, 256)], taps_bc)
    copy_here("bias", bias_in, bias)
    copy_here("x", x_in.at[:, columns(t)], x_rows(t, 0, ROWS))
    copy_here("gain", gain_in, gain_rows)
    copy_here("down", down_in, down_t)
    copy_here("gate", z_in.at[:, columns(t)], gate.at[t])
    copy_here("w", w_in, w_part(0, 1280, s))

    def head_mask(i, carry):
        head = lax.broadcasted_iota(jnp.int32, (256, 128), 0)
        head = jnp.where(head >= 128, head - 128, head)
        lane = lax.broadcasted_iota(jnp.int32, (256, 128), 1)
        own_head = 2 * i + jnp.where(lane >= 64, 1, 0)
        spread[:, tile(i)] = jnp.where(head == own_head, 1.0, 0.0).astype(BF16)
        return carry

    lax.fori_loop(0, 10, head_mask, 0)

    def widen(v):
        high = v.astype(BF16)
        low = (v - high.astype(F32)).astype(BF16)
        return dot(jnp.concatenate([high, low], axis=1), spread[...])

    scale = 2.0 / (TOKENS ** 0.5)

    local["cot"].wait()
    local["up"].wait()
    gt[t] = dot(up[...], cot[...], NT) * scale

    gives_rim = jnp.logical_and(t == 3, c < 15)

    @pl.when(gives_rim)
    def _():
        pl.semaphore_wait(barrier, 25)

    @pl.when(jnp.logical_not(gives_rim))
    def _():
        pl.semaphore_wait(barrier, 21)

    def far_start(src, relay, name):
        send(src.at[pl.ds(0, 64), columns(far)], relay.at[0], name + "0", {"tensor": right})
        send(src.at[pl.ds(64, 64), columns(far)], relay.at[1], name + "1", {"tensor": left})

    def near_start(src, rows, name):
        send(src.at[:, columns(right)], rows(t, 0, ROWS), name + "2", {"tensor": right})
        send(src.at[:, columns(left)], rows(t, 0, ROWS), name + "3", {"tensor": left})

    def far_forward(rows, relay, name):
        arrived(relay.at[0], name + "0")
        send(relay.at[0], rows(left, 0, 64), name + "4", {"tensor": right})
        arrived(relay.at[1], name + "1")
        send(relay.at[1], rows(right, 64, 64), name + "5", {"tensor": left})

    def near_wait(rows, name):
        arrived(rows(left, 0, ROWS), name + "2")
        arrived(rows(right, 0, ROWS), name + "3")

    def far_wait(rows, name):
        arrived(rows(far, 0, 64), name + "4")
        arrived(rows(far, 64, 64), name + "5")

    def rim_copies():
        copies = []
        for p in range(4):
            where = {"context_0": lax.div(after, 2), "context_1": lax.rem(after, 2), "tensor": p}
            copies.append(pltpu.make_async_remote_copy(
                src_ref=x_in.at[pl.ds(120, 8), pl.ds(p * WIDTH, WIDTH)], dst_ref=rim_x,
                send_sem=sl.at[p], recv_sem=rx.at[slot("rim_x")], device_id=where, device_id_type=MESH))
            copies.append(pltpu.make_async_remote_copy(
                src_ref=bc_in.at[pl.ds(120, 8)], dst_ref=rim_b,
                send_sem=sl.at[4 + p], recv_sem=rx.at[slot("rim_b")], device_id=where, device_id_type=MESH))
        return copies

    @pl.when(gives_rim)
    def _():
        for copy in rim_copies():
            copy.start()

    far_start(x_in, xr, "x")
    send(bc_in.at[pl.ds(0, 64)], bc_rows(t, 0, 64), "b0", {"tensor": right})
    send(bc_in.at[pl.ds(64, 64)], bc_rows(t, 64, 64), "b1", {"tensor": left})
    send(bc_in.at[pl.ds(64, 64), pl.ds(0, 128)], b_lanes(t, 64), "b2", {"tensor": right})
    send(bc_in.at[pl.ds(0, 64), pl.ds(0, 128)], b_lanes(t, 0), "b3", {"tensor": left})
    send_triple(lambda j: (dt_window(tensor_peer(j)), dt_all.at[t], {"tensor": tensor_peer(j)}), 0)
    near_start(x_in, x_rows, "x")

    @pl.when(c == 0)
    def _():
        x_ext[0:16, :] = jnp.zeros((16, WIDTH), BF16)
        bc_ext[0:16, :] = jnp.zeros((16, 256), BF16)

    mine, other = k * 640, (1 - k) * 640

    def w_src(first):
        return w_in.at[pl.ds(pl.multiple_of(mine + first, 64), 320)]

    send(w_src(0), w_part(mine, 320, s), "w0", {"fsdp": up_y})
    send(w_src(320), w_part(mine + 320, 320, s), "w1", {"fsdp": down_y})
    send(w_src(320), w_part(mine + 320, 320, s), "w2", {"fsdp": up_y})
    send(w_src(0), w_part(mine, 320, s), "w3", {"fsdp": down_y})

    settle(head_par, s_head)
    for name in ("bc", "dt", "taps_x", "taps_bc", "bias", "x", "gain", "down"):
        local[name].wait()
    pick20 = jnp.where(
        lax.broadcasted_iota(jnp.int32, (HEADS, 128), 0) == lax.broadcasted_iota(jnp.int32, (HEADS, 128), 1), 1.0, 0.0)

    def head_row(i):
        return dot(jnp.broadcast_to(head_par[i], (8, HEADS)), pick20, precision=lax.Precision.HIGHEST)

    step_bias = head_row(0)[0:1, :]
    rate = jnp.exp(head_row(1))[0:1, :]
    skip[...] = widen(head_row(2))
    for i in range(10):
        gain[:, i * 128 : i * 128 + 128] = gain_rows[i : i + 1, :]

    settle(dt_all.at[pl.ds(0, 3)], r3.at[0])

    row = lax.broadcasted_iota(jnp.int32, (128, 128), 0)
    col = lax.broadcasted_iota(jnp.int32, (128, 128), 1)
    causal = row >= col
    tri = jnp.where(causal, 1.0, 0.0)
    pick_row = lax.broadcasted_iota(jnp.int32, (24, 128), 0)
    pick_col = lax.broadcasted_iota(jnp.int32, (24, 128), 1)
    hit = jnp.logical_and(pick_row == pick_col + 4 * lax.rem(t, 2), pick_col < HEADS)
    pick = jnp.where(hit, 1.0, 0.0).astype(BF16)

    total = jnp.zeros((1, 128), F32)
    for p in range(4):
        raw = dot(dt_all[p], pick, TN) + step_bias
        step_now = jnp.maximum(raw, 0.0) + jnp.log1p(jnp.exp(-jnp.abs(raw)))
        cum_now = dot(tri, -step_now * rate, precision=lax.Precision.HIGHEST)
        step[p] = step_now
        cum[p] = cum_now
        log_start[p] = jnp.broadcast_to(total, (8, 128))
        total = total + cum_now[127:128, :]
    for p in range(4):
        log_tail[p] = total - log_start[p] - cum[p, 127:128, :]
        kept[p] = widen(jnp.broadcast_to(jnp.exp(cum[p, 127:128, :]), (8, 128)))
    dec_all[c] = jnp.broadcast_to(jnp.exp(total), (8, 128))

    arrived(bc_rows(left, 0, 64), "b0")
    send(b_lanes(left, 0), b_lanes(left, 0), "b4", {"tensor": right})
    arrived(bc_rows(right, 64, 64), "b1")
    send(b_lanes(right, 64), b_lanes(right, 64), "b5", {"tensor": left})
    pieces = ((0, 5), (5, 3), (8, 2))

    def x_lanes(p, first, piece):
        return x_ext.at[
            pl.ds(pl.multiple_of(16 + p * ROWS + first, 16), 64), pl.ds(piece[0] * 128, piece[1] * 128)]

    arrived(xr.at[0], "x0")
    arrived(xr.at[1], "x1")
    for piece in pieces:
        lanes = pl.ds(piece[0] * 128, piece[1] * 128)
        send(xr.at[0, :, lanes], x_lanes(left, 0, piece), "x4%d" % piece[0], {"tensor": right})
        send(xr.at[1, :, lanes], x_lanes(right, 64, piece), "x5%d" % piece[0], {"tensor": left})
    send(bc_in.at[pl.ds(64, 64), pl.ds(128, 128)], c_lanes(t, 64), "c2", {"tensor": right})
    send(bc_in.at[pl.ds(0, 64), pl.ds(128, 128)], c_lanes(t, 0), "c3", {"tensor": left})
    send(c_lanes(left, 0), c_lanes(left, 0), "c4", {"tensor": right})
    send(c_lanes(right, 64), c_lanes(right, 64), "c5", {"tensor": left})
    far_start(z_in, zr, "z")

    def gate_near(first):
        rows = pl.ds(first, 64)
        send(z_in.at[rows, columns(right)], z_rows(t, first, 64), "z2%d" % first, {"tensor": right})
        send(z_in.at[rows, columns(left)], z_rows(t, first, 64), "z3%d" % first, {"tensor": left})

    gate_near(0)

    def decay_copy(j):
        return pltpu.make_async_remote_copy(
            src_ref=dec_all.at[c], dst_ref=dec_all.at[c],
            send_sem=sd, recv_sem=rd, device_id=context_peer(j), device_id_type=MESH)

    exchange(decay_copy)
    send_triple(lambda j: (gt.at[t], gt.at[t], {"tensor": tensor_peer(j)}), 1)

    def convolved(ext, p, lanes, taps, bias_row):
        v = ext[pl.ds(pl.multiple_of(p * ROWS, 16), ROWS + 16), lanes].astype(F32)
        acc = bias[pl.ds(bias_row, 1), :] + taps[0:1, lanes] * pltpu.roll(v, 3, 0)
        acc = acc + taps[1:2, lanes] * pltpu.roll(v, 2, 0)
        acc = acc + taps[2:3, lanes] * pltpu.roll(v, 1, 0)
        acc = acc + taps[3:4, lanes] * v
        return silu(acc[16:]).astype(BF16)

    @pl.when(c > 0)
    def _():
        arrived(rim_x, "rim_x")
        arrived(rim_b, "rim_b")
        x_ext[0:16, :] = jnp.concatenate([rim_x[...], rim_x[...]], axis=0)
        bc_ext[0:16, :] = jnp.concatenate([rim_b[...], rim_b[...]], axis=0)

    state[...] = jnp.zeros((STATE, WIDTH), F32)

    def shared(half):
        def of(i, carry):
            p = lax.rem(t + i, 4)
            bcc[p, :, pl.ds(half * 128, 128)] = convolved(bc_ext, p, pl.ds(half * 128, 128), taps_bc, 40 + half)
            return carry

        return of

    def block(first, count):
        def of(i, carry):
            p = lax.rem(t + i, 4)
            lanes = pl.ds(first * 128, count * 128)

            def lanes_of(j, inner):
                xc[p, :, tile(j)] = convolved(x_ext, p, tile(j), taps_x, 10 * t + j)
                return inner

            lax.fori_loop(first, first + count, lanes_of, 0)
            scaled = (xc[p, :, lanes].astype(F32) * weights[p, :, lanes]).astype(BF16)
            fresh = dot(bcc[p, :, 0:128], scaled, TN)
            blocks[p, :, lanes] = fresh
            state[:, lanes] = state[:, lanes] + tails[p, 0:1, lanes] * fresh
            return carry

        return of

    def weigh(p, carry):
        cum_now = cum[p]
        weights[p] = widen(step[p] * jnp.exp(cum_now[127:128, :] - cum_now))
        tails[p] = widen(jnp.exp(log_tail[p]))
        return carry

    lax.fori_loop(0, 4, weigh, 0)
    arrived(w_part(mine, 320, down_y), "w0")
    send(w_part(mine, 320, down_y), w_part(mine, 320, down_y), "w4", {"fsdp": up_y})
    arrived(w_part(mine + 320, 320, up_y), "w1")
    send(w_part(mine + 320, 320, up_y), w_part(mine + 320, 320, up_y), "w5", {"fsdp": down_y})
    settle(dec_all.at[pl.ds(0, 15)], rd)
    dec_wide[...] = widen(dec_all[...].reshape(128, 128))
    arrived(b_lanes(left, 64), "b2")
    arrived(b_lanes(right, 0), "b3")
    lax.fori_loop(0, 2, shared(0), 0)
    near_wait(x_rows, "x")
    lax.fori_loop(0, 2, block(0, 10), 0)
    core = {"context_1": 1 - k}

    def half_lanes(h):
        return pl.ds(h * 640, 640)

    rows_mine = pl.ds(pl.multiple_of(64 * k, 64), 64)
    rows_other = pl.ds(pl.multiple_of(64 * (1 - k), 64), 64)

    def pair(h):
        send(state.at[rows_other, half_lanes(h)], peer_state.at[:, half_lanes(h)], "pair%d" % h, core)

    arrived(b_lanes(far, 0), "b4")
    arrived(b_lanes(far, 64), "b5")
    lax.fori_loop(2, 4, shared(0), 0)
    for piece in pieces:
        arrived(x_lanes(far, 0, piece), "x4%d" % piece[0])
        arrived(x_lanes(far, 64, piece), "x5%d" % piece[0])
        lax.fori_loop(2, 4, block(*piece), 0)
        if piece[0] == 0:
            pair(0)
    pair(1)

    decay_second = dec_wide[pl.ds(pl.multiple_of(16 * z + 8, 8), 8), :]
    weight_mine = jnp.where(k == 0, decay_second, jnp.ones_like(decay_second))
    weight_peer = jnp.where(k == 0, jnp.ones_like(decay_second), decay_second)

    def state_copy(h):
        def of(j):
            return pltpu.make_async_remote_copy(
                src_ref=st_send.at[h, chip_at(j - 1)], dst_ref=st_recv.at[h, z],
                send_sem=sc.at[h], recv_sem=rc_.at[h], device_id=chip_peer(j), device_id_type=MESH)

        return of

    for h in range(2):
        arrived(peer_state.at[:, half_lanes(h)], "pair%d" % h)
        first_lane, last_lane = h * 640, h * 640 + 640

        def pack_state(i, carry):
            rows = pl.ds(pl.multiple_of(64 * k + i * 8, 8), 8)
            rows_peer = pl.ds(pl.multiple_of(i * 8, 8), 8)
            both = (weight_mine[:, first_lane:last_lane] * state[rows, half_lanes(h)]
                    + weight_peer[:, first_lane:last_lane] * peer_state[rows_peer, half_lanes(h)])
            st_send[h, i] = both.astype(BF16)
            return carry

        lax.fori_loop(0, 8, pack_state, 0)
        exchange(state_copy(h), 8)
        st_recv[h, z] = st_send[h, z]

    arrived(w_part(mine + 320, 320, down_y), "w2")
    send(w_part(mine, 640, down_y), w_part(mine, 640, down_y), "w6", core)
    arrived(w_part(mine, 320, up_y), "w3")
    send(w_part(mine, 640, up_y), w_part(mine, 640, up_y), "w7", core)
    far_forward(z_rows, zr, "z")
    gate_near(64)

    arrived(c_lanes(left, 64), "c2")
    arrived(c_lanes(right, 0), "c3")
    arrived(c_lanes(far, 0), "c4")
    arrived(c_lanes(far, 64), "c5")
    lax.fori_loop(0, 4, shared(1), 0)

    def inside(p, carry):
        b_now, c_now = bcc[p, :, 0:128], bcc[p, :, 128:256]
        gram = dot(c_now, b_now, NT)
        cum_now = cum[p]
        shifted = (cum_now - jnp.log(step[p])).T
        lane = lax.broadcasted_iota(jnp.int32, (1, 128), 1)
        low = jnp.where(lane < 64, 1.0, 0.0)
        for q in range(HEADS // 2):
            mats = []
            for h in (2 * q, 2 * q + 1):
                gap = cum_now[:, h : h + 1] - shifted[h : h + 1, :]
                mats.append(jnp.exp(jnp.where(causal, gap, -1e30)) * gram)
            both = jnp.concatenate(mats, axis=1).astype(BF16)
            x_pair = xc[p, :, pl.ds(q * 128, 128)].astype(F32)
            x_two = jnp.concatenate([x_pair * low, x_pair * (1.0 - low)], axis=0).astype(BF16)
            y_in[p, :, pl.ds(q * 128, 128)] = dot(both, x_two) + x_pair * skip[0:1, pl.ds(q * 128, 128)]
        return carry

    def back_copy(h):
        def of(j):
            return pltpu.make_async_remote_copy(
                src_ref=back_send.at[h, chip_at(j - 1)], dst_ref=back_recv.at[h, z],
                send_sem=sb.at[h], recv_sem=rb.at[h], device_id=chip_peer(j), device_id_type=MESH)

        return of

    for h in range(2):
        lax.fori_loop(2 * h, 2 * h + 2, inside, 0)
        settle(st_recv.at[h, pl.ds(0, 7)], rc_.at[h])

        def chain(i, held):
            back_send[h, i] = held.astype(BF16)
            decay = dec_wide[pl.ds(pl.multiple_of(16 * i, 8), 8), half_lanes(h)] * dec_wide[
                pl.ds(pl.multiple_of(16 * i + 8, 8), 8), half_lanes(h)]
            return decay * held + st_recv[h, i].astype(F32)

        lax.fori_loop(0, 8, chain, jnp.zeros((8, 640), F32))
        exchange(back_copy(h), 8)
        back_recv[h, z] = back_send[h, z]

    def starts(j, carry):
        held = jnp.zeros((STATE, 128), F32)
        for p in range(4):
            fresh = blocks[p, :, tile(j)]
            blocks[p, :, tile(j)] = held
            held = kept[p, 0:1, tile(j)] * held + fresh
        return carry

    lax.fori_loop(0, 10, starts, 0)

    arrived(w_part(mine, 320, far_y), "w4")
    arrived(w_part(mine + 320, 320, far_y), "w5")
    send(w_part(mine, 640, far_y), w_part(mine, 640, far_y), "w8", core)

    for h in range(2):
        settle(back_recv.at[h, pl.ds(0, 7)], rb.at[h])
        decay_first = dec_wide[pl.ds(pl.multiple_of(16 * z, 8), 8), half_lanes(h)]

        def unpack_state(i, carry):
            rows = pl.ds(pl.multiple_of(64 * k + i * 8, 8), 8)
            rows_peer = pl.ds(pl.multiple_of(i * 8, 8), 8)
            first = back_recv[h, i].astype(F32)
            span = jnp.where(k == 0, state[rows, half_lanes(h)], peer_state[rows_peer, half_lanes(h)])
            second = decay_first * first + span
            s_in[rows, half_lanes(h)] = jnp.where(k == 0, first, second)
            in_send[rows_peer, half_lanes(h)] = jnp.where(k == 0, second, first)
            return carry

        lax.fori_loop(0, 8, unpack_state, 0)
        send(in_send.at[:, half_lanes(h)], s_in.at[rows_mine, half_lanes(h)], "in%d" % h, core)

    local["w"].wait()
    arrived(w_part(other, 640, down_y), "w6")
    arrived(w_part(other, 640, up_y), "w7")
    arrived(w_part(other, 640, far_y), "w8")
    for h in range(2):
        arrived(s_in.at[rows_other, half_lanes(h)], "in%d" % h)

    def finish(i, carry):
        p = lax.rem(t + i, 4)
        start = blocks[p] + widen(jnp.exp(log_start[p]))[0:1, :] * s_in[...]
        reach = widen(jnp.exp(cum[p]))
        y_now = y_in[p] + reach * dot(bcc[p, :, 128:256], start.astype(BF16))
        now = y_now * silu(gate[p].astype(F32))
        squares = (now * now).astype(BF16)
        sq[t, pl.ds(p, 1), :] = dot(jnp.ones((8, WIDTH), BF16), squares, NT)[0:1, :]
        out = (now * gain[...]).astype(BF16)
        gated[p] = out
        ap_send[p] = dot(down_t[...], out, NT)
        return carry

    def project(p, half, store, first=0, count=5):
        def piece(i, carry):
            lanes = pl.ds(pl.multiple_of(i * 256, 256), 256)
            lanes_w = pl.ds(pl.multiple_of(half * HALF + i * 256, 256), 256)
            store(lanes, dot(gated[p], wt[:, lanes_w]))
            return carry

        lax.fori_loop(first, first + count, piece, 0)

    def to_slot(which, extra=None):
        def store(lanes, v):
            if extra is not None:
                v = v + rs_recv[extra, :, lanes].astype(F32)
            rs_send[which, :, lanes] = v.astype(BF16)

        return store

    def piece_at(ref, which, i):
        return ref.at[which, :, pl.ds(i * 256, 256)]

    def ship(which, where, i):
        pltpu.make_async_remote_copy(
            src_ref=piece_at(rs_send, which, i), dst_ref=piece_at(rs_recv, which, i),
            send_sem=sr, recv_sem=rr.at[5 * which + i] if which < 2 else rr_end.at[which - 2],
            device_id={"tensor": where}, device_id_type=MESH).start()

    def landed(which, i):
        piece = piece_at(rs_recv, which, i)
        pltpu.make_async_copy(piece, piece, rr.at[5 * which + i]).wait()

    far_wait(z_rows, "z")
    lax.fori_loop(2, 3, finish, 0)
    for i in range(5):
        project(far, 0, to_slot(0), i, 1)
        project(far, 1, to_slot(1), i, 1)
        if i < 3:
            ship(0, right, i)
            ship(1, left, i)
    local["gate"].wait()
    for first in (0, 64):
        arrived(z_rows(left, first, 64), "z2%d" % first)
        arrived(z_rows(right, first, 64), "z3%d" % first)
    lax.fori_loop(3, 6, finish, 0)
    ap_recv[t] = ap_send[t]
    send_triple(lambda j: (sq.at[t], sq.at[t], {"tensor": tensor_peer(j)}), 2)
    send_triple(lambda j: (ap_send.at[tensor_peer(j)], ap_recv.at[t], {"tensor": tensor_peer(j)}), 3)
    for i in range(3, 5):
        ship(0, right, i)
        ship(1, left, i)
    for i in range(5):
        project(right, 1, to_slot(2), i, 1)
        ship(2, right, i)
        project(left, 0, to_slot(3), i, 1)
        ship(3, left, i)

    settle(gt.at[pl.ds(0, 3)], r3.at[1])
    settle(sq.at[pl.ds(0, 3)], r3.at[2])
    settle(ap_recv.at[pl.ds(0, 3)], r3.at[3])

    def row_scale(p):
        rows = pl.ds(p, 1)
        squares = (sq[0, rows, :] + sq[1, rows, :]) + (sq[2, rows, :] + sq[3, rows, :])
        return lax.rsqrt(squares * (1.0 / 5120.0) + EPS)

    adapter = ((ap_recv[0] + ap_recv[1]) + (ap_recv[2] + ap_recv[3])).astype(BF16)
    own_scale = row_scale(t)
    weighted = (scale * own_scale[0:1, :] * adapter.astype(F32)).astype(BF16)
    grad_a_now = jnp.zeros((RANK, WIDTH), F32)
    for p in range(4):
        rows_grad = (row_scale(p)[0:1, :] * gt[p]).astype(BF16)
        grad_a_now = grad_a_now + dot(rows_grad, gated[p])
    grad_b_now = dot(weighted, cot[...])
    for i in range(30):
        v_send[i // 2, i % 2] = (
            grad_a_now[:, i * 128 : i * 128 + 128] if i < 10
            else grad_b_now[:, (i - 10) * 128 : (i - 10) * 128 + 128]).astype(BF16)
    v_send[15] = jnp.zeros((2, RANK, 128), BF16)
    v_recv[c] = v_send[c]

    def v_copy(j):
        return pltpu.make_async_remote_copy(
            src_ref=v_send.at[context_index(j)], dst_ref=v_recv.at[c],
            send_sem=sv, recv_sem=rv, device_id=context_peer(j), device_id_type=MESH)

    exchange(v_copy)

    for i in range(1):
        landed(0, i)
        project(right, 0, to_slot(4, 0), i, 1)
        ship(4, right, i)
        landed(1, i)
        project(left, 1, to_slot(5, 1), i, 1)
        ship(5, left, i)

    settle(v_recv.at[pl.ds(0, 15)], rv)

    def add_v(i, held):
        return held + v_recv[i].astype(F32)

    y_recv[s] = lax.fori_loop(0, 16, add_v, jnp.zeros((2, RANK, 128), F32))
    send_triple(lambda j: (y_recv.at[s], y_recv.at[s], {"fsdp": lax.rem(s + j, 4)}), 4)
    for i in range(1, 5):
        landed(0, i)
        project(right, 0, to_slot(4, 0), i, 1)
        landed(1, i)
        project(left, 1, to_slot(5, 1), i, 1)
    settle(y_recv.at[pl.ds(0, 3)], r3.at[4])
    t_recv[t] = ((y_recv[0] + y_recv[1]) + (y_recv[2] + y_recv[3])).astype(BF16)
    send_triple(lambda j: (t_recv.at[t], t_recv.at[t], {"tensor": tensor_peer(j)}), 5)
    for i in range(1, 5):
        ship(4, right, i)
        ship(5, left, i)

    def own_part(half):
        def store(lanes, v):
            lanes_up = pl.ds(pl.multiple_of(half * HALF + lanes.start, 256), 256)
            own[half, :, lanes] = v + 2.0 * dot(adapter, up[:, lanes_up], TN)

        return store

    project(t, 0, own_part(0))
    project(t, 1, own_part(1))

    settle(t_recv.at[pl.ds(0, 3)], r3.at[5])

    def add_t(i, held):
        keep = jnp.where(jnp.logical_or(c >= 5, i == t), 1.0, 0.0)
        return held + keep * t_recv[i].astype(F32)

    v_all[c] = lax.fori_loop(0, 4, add_t, jnp.zeros((2, RANK, 128), F32)).astype(BF16)

    def all_copy(j):
        return pltpu.make_async_remote_copy(
            src_ref=v_all.at[c], dst_ref=v_all.at[c],
            send_sem=sg, recv_sem=rg, device_id=context_peer(j), device_id_type=MESH)

    exchange(all_copy)

    scale_col = jnp.broadcast_to(own_scale[0:1, :], (128, 128)).T
    for which in range(2, 6):
        pltpu.make_async_copy(rs_recv.at[which], rs_recv.at[which], rr_end.at[which - 2]).wait()

    def close(i, carry):
        lanes = tile(i)
        first = own[0, :, lanes] + rs_recv[4, :, lanes].astype(F32) + rs_recv[3, :, lanes].astype(F32)
        second = own[1, :, lanes] + rs_recv[2, :, lanes].astype(F32) + rs_recv[5, :, lanes].astype(F32)
        mixed_here[:, lanes] = (scale_col * first).astype(BF16)
        mixed_here[:, pl.ds(pl.multiple_of(HALF + i * 128, 128), 128)] = (scale_col * second).astype(BF16)
        return carry

    lax.fori_loop(0, 10, close, 0)
    copy_here("mixed", mixed_here, mixed)

    settle(v_all.at[pl.ds(0, 15)], rg)
    for i in range(10):
        a_here[:, i * 128 : i * 128 + 128] = v_all[i // 2, i % 2].astype(F32)
    for i in range(20):
        b_here[:, i * 128 : i * 128 + 128] = v_all[5 + i // 2, i % 2].astype(F32)
    copy_here("grad_a", a_here, grad_a)
    copy_here("grad_b", b_here, grad_b)

    for which, buffer in enumerate((dt_all, gt, sq, ap_send, y_recv, t_recv)):
        settle(buffer.at[pl.ds(0, 3)], s3.at[which])
    settle(dec_all.at[pl.ds(0, 15)], sd)
    for h in range(2):
        settle(st_send.at[h, pl.ds(0, 7)], sc.at[h])
        settle(back_send.at[h, pl.ds(0, 7)], sb.at[h])
    settle(v_send.at[pl.ds(0, 15)], sv)
    settle(v_all.at[pl.ds(0, 15)], sg)
    pltpu.make_async_copy(rs_send, rs_send, sr).wait()
    pltpu.make_async_copy(x_ext.at[pl.ds(16, 512)], x_ext.at[pl.ds(16, 512)], sgroup.at[0]).wait()
    pltpu.make_async_copy(gate, gate, sgroup.at[1]).wait()
    pltpu.make_async_copy(wt.at[:, pl.ds(0, 1920)], wt.at[:, pl.ds(0, 1920)], sgroup.at[2]).wait()
    for copy in started:
        copy.wait_send()
    assert len(slots) <= 43 and len(send_slots) <= 14 and len(local) <= 15

    @pl.when(gives_rim)
    def _():
        for copy in rim_copies():
            copy.wait_send()

    for name in ("mixed", "grad_a", "grad_b"):
        local[name].wait()


def shards(
    input_raw, state_proj_raw, gate_branch, step_raw, convolution_taps, convolution_bias, step_bias,
    decay_log_rate, skip_weight, gated_norm_gain, output_weight, adapter_down, adapter_up, cotangent,
):
    hbm = pl.BlockSpec(memory_space=pl.ANY)
    dma = pltpu.SemaphoreType.DMA
    mixed, grad_a, grad_b = pl.pallas_call(
        kernel,
        out_shape=(
            jax.ShapeDtypeStruct((ROWS, OUT), BF16),
            jax.ShapeDtypeStruct((RANK, WIDTH), F32),
            jax.ShapeDtypeStruct((RANK, OUT), F32),
        ),
        in_specs=[hbm] * 14,
        out_specs=(hbm, hbm, hbm),
        scratch_shapes=[
            pltpu.VMEM((16 + 512, WIDTH), BF16),
            pltpu.VMEM((2, 64, WIDTH), BF16),
            pltpu.VMEM((8, WIDTH), BF16),
            pltpu.VMEM((8, 256), BF16),
            pltpu.VMEM((4, ROWS, WIDTH), BF16),
            pltpu.VMEM((16 + 512, 256), BF16),
            pltpu.VMEM((4, ROWS, 256), BF16),
            pltpu.VMEM((4, 24, 128), BF16),
            pltpu.VMEM((4, ROWS, WIDTH), BF16),
            pltpu.VMEM((2, 64, WIDTH), BF16),
            pltpu.VMEM((WIDTH, OUT), BF16),
            pltpu.VMEM((ROWS, OUT), BF16),
            pltpu.VMEM((4, WIDTH), F32),
            pltpu.VMEM((4, 256), F32),
            pltpu.VMEM((42, 128), F32),
            pltpu.VMEM((3, 1, HEADS), F32),
            pltpu.VMEM((10, 128), F32),
            pltpu.VMEM((1, WIDTH), F32),
            pltpu.VMEM((RANK, WIDTH), BF16),
            pltpu.VMEM((RANK, OUT), BF16),
            pltpu.VMEM((8, WIDTH), F32),
            pltpu.VMEM((4, ROWS, WIDTH), F32),
            pltpu.VMEM((4, 8, WIDTH), F32),
            pltpu.VMEM((256, WIDTH), BF16),
            pltpu.VMEM((4, ROWS, 128), F32),
            pltpu.VMEM((4, ROWS, 128), F32),
            pltpu.VMEM((4, 8, 128), F32),
            pltpu.VMEM((4, 8, 128), F32),
            pltpu.VMEM((4, ROWS, WIDTH), F32),
            pltpu.VMEM((4, STATE, WIDTH), F32),
            pltpu.VMEM((4, 8, WIDTH), F32),
            pltpu.VMEM((STATE, WIDTH), F32),
            pltpu.VMEM((64, WIDTH), F32),
            pltpu.VMEM((2, 8, 8, 640), BF16),
            pltpu.VMEM((2, 8, 8, 640), BF16),
            pltpu.VMEM((16, 8, 128), F32),
            pltpu.VMEM((128, WIDTH), F32),
            pltpu.VMEM((2, 8, 8, 640), BF16),
            pltpu.VMEM((2, 8, 8, 640), BF16),
            pltpu.VMEM((64, WIDTH), F32),
            pltpu.VMEM((STATE, WIDTH), F32),
            pltpu.VMEM((4, ROWS, WIDTH), BF16),
            pltpu.VMEM((4, RANK, 128), F32),
            pltpu.VMEM((4, 8, 128), F32),
            pltpu.VMEM((4, RANK, 128), F32),
            pltpu.VMEM((4, RANK, 128), F32),
            pltpu.VMEM((6, ROWS, HALF), BF16),
            pltpu.VMEM((6, ROWS, HALF), BF16),
            pltpu.VMEM((2, ROWS, HALF), F32),
            pltpu.VMEM((16, 2, RANK, 128), BF16),
            pltpu.VMEM((16, 2, RANK, 128), BF16),
            pltpu.VMEM((4, 2, RANK, 128), F32),
            pltpu.VMEM((4, 2, RANK, 128), BF16),
            pltpu.VMEM((16, 2, RANK, 128), BF16),
            pltpu.VMEM((ROWS, OUT), BF16),
            pltpu.VMEM((RANK, WIDTH), F32),
            pltpu.VMEM((RANK, OUT), F32),
            dma((14,)), dma((43,)), dma((23,)),
            dma((2,)), dma((2,)), dma, dma, dma((2,)), dma((2,)), dma, dma, dma, dma, dma, dma((10,)), dma((4,)), dma((3,)), dma((6,)), dma((6,)), dma,
        ],
        compiler_params=pltpu.CompilerParams(
            collective_id=0, has_side_effects=True, vmem_limit_bytes=64 * 1000 * 1000),
    )(
        input_raw[0], state_proj_raw[0], gate_branch[0], step_raw[0].T, output_weight, cotangent[0],
        convolution_taps, convolution_bias.reshape(42, 128), step_bias[None, :], decay_log_rate[None, :],
        skip_weight[None, :], gated_norm_gain.reshape(10, 128), adapter_down.T, adapter_up,
    )
    return (mixed[None], grad_a.T, grad_b)


def solution(mesh):
    torus = Mesh(
        mesh.devices.reshape(8, 2, mesh.shape["tensor"], mesh.shape["fsdp"]),
        ("context_0", "context_1", "tensor", "fsdp"),
    )
    tokens = P("fsdp", CONTEXT_TENSOR, None)
    return jax.shard_map(
        shards,
        mesh=torus,
        in_specs=(
            tokens, tokens, tokens, tokens, P(), P(), P("tensor"), P("tensor"), P("tensor"), P("tensor"),
            P("tensor", "fsdp"), P("tensor", None), P(), tokens,
        ),
        out_specs=(tokens, P("tensor", None), P()),
        check_vma=False,
    )
```

```python
import functools

import jax
import jax.numpy as jnp
from jax import lax
from jax.experimental import pallas as pl
from jax.experimental.pallas import tpu as pltpu
from jax.sharding import Mesh
from jax.sharding import PartitionSpec as P

MESH = pl.DeviceIdType.MESH
CONTEXT_TENSOR = ("context_0", "context_1", "tensor")
F32 = jnp.float32
BF16 = jnp.bfloat16

ROWS = 128
WIDTH = 1280
STATE = 128
OUT = 2560
HALF = 1280
RANK = 16
HEADS = 20
COLS = 640
TOKENS = 32768
EPS = 1e-05

NT = (((1,), (1,)), ((), ()))
TN = (((0,), (0,)), ((), ()))


def silu(v):
    half = 0.5 * v
    return half + half * jnp.tanh(half)


def dot(a, b, dims=(((1,), (0,)), ((), ())), precision=None):
    return lax.dot_general(a, b, dims, precision=precision, preferred_element_type=F32)


def kernel(
    x_in, bc_in, z_in, dt_in, w_in, cot_in, taps_in, bias_in, step_bias_in, rate_in, skip_in, gain_in, down_in, up_in,
    mixed, grad_a, grad_b,
    x_ext, xr, rim_x, rim_b, xc, bc_ext, bcc, dt_all, gate, zr, wt, cot,
    taps_x, taps_bc, bias, head_par, gain_rows, gain, down_t, up, skip, weights, tails,
    spread, step, cum, log_start, log_tail, y_in, blocks, kept, state, peer_state,
    st_send, st_recv, dec_all, dec_wide, back_send, back_recv, in_send, s_in,
    gated, gt, sq, ap_send, ap_recv,
    rs_send, rs_recv, own,
    v_send, v_recv, y_recv, t_recv, v_all,
    sx, rx, sl, sc, rc_, sd, rd, sb, rb, sv, rv, sg, rg, sr, rr, rr_end, sgroup, s3, r3, s_head,
):
    z, k = lax.axis_index("context_0"), lax.axis_index("context_1")
    t, s = lax.axis_index("tensor"), lax.axis_index("fsdp")
    c = 2 * z + k
    right, left, far = lax.rem(t + 1, 4), lax.rem(t + 3, 4), lax.rem(t + 2, 4)
    up_y, down_y, far_y = lax.rem(s + 1, 4), lax.rem(s + 3, 4), lax.rem(s + 2, 4)
    started = []
    slots, send_slots = {}, {}

    together = {"c3": "c2", "c4": "c2", "c5": "c2", "z30": "z20", "z264": "z20", "z364": "z20",
                "b5": "b4", "x3": "x2", "w7": "w6", "w8": "w6"}

    def slot(name):
        return slots.setdefault(together.get(name, name), len(slots))

    def send_slot(name):
        return send_slots.setdefault(name, len(send_slots))

    groups = {"x": 0, "z": 1, "w": 2, "c": 3, "p": 4, "i": 5}

    def send(src, dst, name, where):
        grouped = groups.get(name[0])
        copy = pltpu.make_async_remote_copy(
            src_ref=src, dst_ref=dst,
            send_sem=sx.at[send_slot(name)] if grouped is None else sgroup.at[grouped],
            recv_sem=rx.at[slot(name)], device_id=where, device_id_type=MESH,
        )
        copy.start()
        if groups.get(name[0]) is None:
            started.append(copy)

    def send_triple(make, which):
        for j in (2, 1, 3):
            src, dst, where = make(j)
            pltpu.make_async_remote_copy(
                src_ref=src, dst_ref=dst, send_sem=s3.at[which], recv_sem=r3.at[which],
                device_id=where, device_id_type=MESH).start()

    def tensor_peer(j):
        return lax.rem(t + j, 4)

    def arrived(dst, name):
        pltpu.make_async_copy(dst, dst, rx.at[slot(name)]).wait()

    def chip_at(i):
        step_now = lax.div(i + 1, 2)
        return lax.rem(z + 4 + (1 - 2 * lax.rem(i, 2)) * step_now, 8)

    def core_at(j):
        return lax.rem(k + j, 2)

    def context_index(j):
        return 2 * chip_at(lax.div(j - 1, 2)) + core_at(j)

    def context_peer(j):
        return {"context_0": chip_at(lax.div(j - 1, 2)), "context_1": core_at(j)}

    def chip_peer(j):
        return {"context_0": chip_at(j - 1)}

    def exchange(make, how_many=16):
        def go(j, carry):
            make(j).start()
            return carry

        lax.fori_loop(1, how_many, go, 0)

    def settle(several, sem):
        pltpu.make_async_copy(several, several, sem).wait()

    def tile(i):
        return pl.ds(pl.multiple_of(i * 128, 128), 128)

    barrier = pltpu.get_barrier_semaphore()

    def greet(j, carry):
        pl.semaphore_signal(barrier, inc=1, device_id=context_peer(j), device_id_type=MESH)
        return carry

    for j in range(1, 4):
        pl.semaphore_signal(barrier, inc=1, device_id={"tensor": lax.rem(t + j, 4)}, device_id_type=MESH)
        pl.semaphore_signal(barrier, inc=1, device_id={"fsdp": lax.rem(s + j, 4)}, device_id_type=MESH)
    lax.fori_loop(1, 16, greet, 0)
    before = lax.rem(c + 15, 16)
    after = lax.rem(c + 1, 16)

    @pl.when(c > 0)
    def _():
        pl.semaphore_signal(
            barrier, inc=1,
            device_id={"context_0": lax.div(before, 2), "context_1": lax.rem(before, 2), "tensor": 3},
            device_id_type=MESH,
        )

    def columns(p):
        return pl.ds(pl.multiple_of(p * WIDTH, WIDTH), WIDTH)

    def x_rows(p, first, count):
        return x_ext.at[pl.ds(pl.multiple_of(16 + p * ROWS + first, 16), count)]

    def z_rows(p, first, count):
        return gate.at[p, pl.ds(first, count)]

    def bc_rows(p, first, count):
        return bc_ext.at[pl.ds(pl.multiple_of(16 + p * ROWS + first, 16), count)]

    def b_lanes(p, first):
        return bc_ext.at[pl.ds(pl.multiple_of(16 + p * ROWS + first, 16), 64), pl.ds(0, 128)]

    def c_lanes(p, first):
        return bc_ext.at[pl.ds(pl.multiple_of(16 + p * ROWS + first, 16), 64), pl.ds(128, 128)]

    def w_part(rows_from, count, y):
        return wt.at[
            pl.ds(pl.multiple_of(rows_from, 64), count), pl.ds(pl.multiple_of(y * COLS, COLS), COLS)
        ]

    def dt_window(p):
        return dt_in.at[pl.ds(pl.multiple_of(8 * lax.div(5 * p, 2), 8), 24)]

    local = {}

    def copy_here(name, src, dst):
        local[name] = pltpu.make_async_copy(src, dst, sl.at[2 + len(local)])
        local[name].start()

    copy_here("cot", cot_in, cot)
    copy_here("up", up_in, up)
    for i, source in enumerate((step_bias_in, rate_in, skip_in)):
        pltpu.make_async_copy(source, head_par.at[i], s_head).start()
    copy_here("bc", bc_in, bc_rows(t, 0, ROWS))
    copy_here("dt", dt_window(t), dt_all.at[t])
    copy_here("taps_x", taps_in.at[:, columns(t)], taps_x)
    copy_here("taps_bc", taps_in.at[:, pl.ds(4 * WIDTH, 256)], taps_bc)
    copy_here("bias", bias_in, bias)
    copy_here("x", x_in.at[:, columns(t)], x_rows(t, 0, ROWS))
    copy_here("gain", gain_in, gain_rows)
    copy_here("down", down_in, down_t)
    copy_here("gate", z_in.at[:, columns(t)], gate.at[t])
    copy_here("w", w_in, w_part(0, 1280, s))

    def head_mask(i, carry):
        head = lax.broadcasted_iota(jnp.int32, (256, 128), 0)
        head = jnp.where(head >= 128, head - 128, head)
        lane = lax.broadcasted_iota(jnp.int32, (256, 128), 1)
        own_head = 2 * i + jnp.where(lane >= 64, 1, 0)
        spread[:, tile(i)] = jnp.where(head == own_head, 1.0, 0.0).astype(BF16)
        return carry

    lax.fori_loop(0, 10, head_mask, 0)

    def widen(v):
        high = v.astype(BF16)
        low = (v - high.astype(F32)).astype(BF16)
        return dot(jnp.concatenate([high, low], axis=1), spread[...])

    scale = 2.0 / (TOKENS ** 0.5)

    local["cot"].wait()
    local["up"].wait()
    gt[t] = dot(up[...], cot[...], NT) * scale

    gives_rim = jnp.logical_and(t == 3, c < 15)

    @pl.when(gives_rim)
    def _():
        pl.semaphore_wait(barrier, 25)

    @pl.when(jnp.logical_not(gives_rim))
    def _():
        pl.semaphore_wait(barrier, 21)

    def far_start(src, relay, name):
        send(src.at[pl.ds(0, 64), columns(far)], relay.at[0], name + "0", {"tensor": right})
        send(src.at[pl.ds(64, 64), columns(far)], relay.at[1], name + "1", {"tensor": left})

    def near_start(src, rows, name):
        send(src.at[:, columns(right)], rows(t, 0, ROWS), name + "2", {"tensor": right})
        send(src.at[:, columns(left)], rows(t, 0, ROWS), name + "3", {"tensor": left})

    def far_forward(rows, relay, name):
        arrived(relay.at[0], name + "0")
        send(relay.at[0], rows(left, 0, 64), name + "4", {"tensor": right})
        arrived(relay.at[1], name + "1")
        send(relay.at[1], rows(right, 64, 64), name + "5", {"tensor": left})

    def far_wait(rows, name):
        arrived(rows(far, 0, 64), name + "4")
        arrived(rows(far, 64, 64), name + "5")

    def rim_copies():
        copies = []
        for p in range(4):
            where = {"context_0": lax.div(after, 2), "context_1": lax.rem(after, 2), "tensor": p}
            copies.append(pltpu.make_async_remote_copy(
                src_ref=x_in.at[pl.ds(120, 8), pl.ds(p * WIDTH, WIDTH)], dst_ref=rim_x,
                send_sem=sl.at[0], recv_sem=rx.at[slot("rim_x")], device_id=where, device_id_type=MESH))
            copies.append(pltpu.make_async_remote_copy(
                src_ref=bc_in.at[pl.ds(120, 8)], dst_ref=rim_b,
                send_sem=sl.at[1], recv_sem=rx.at[slot("rim_b")], device_id=where, device_id_type=MESH))
        return copies

    @pl.when(gives_rim)
    def _():
        for copy in rim_copies():
            copy.start()

    far_start(x_in, xr, "x")
    send(bc_in.at[pl.ds(0, 64)], bc_rows(t, 0, 64), "b0", {"tensor": right})
    send(bc_in.at[pl.ds(64, 64)], bc_rows(t, 64, 64), "b1", {"tensor": left})
    send(bc_in.at[pl.ds(64, 64), pl.ds(0, 128)], b_lanes(t, 64), "b2", {"tensor": right})
    send(bc_in.at[pl.ds(0, 64), pl.ds(0, 128)], b_lanes(t, 0), "b3", {"tensor": left})
    send_triple(lambda j: (dt_window(tensor_peer(j)), dt_all.at[t], {"tensor": tensor_peer(j)}), 0)
    near_start(x_in, x_rows, "x")

    @pl.when(c == 0)
    def _():
        x_ext[0:16, :] = jnp.zeros((16, WIDTH), BF16)
        bc_ext[0:16, :] = jnp.zeros((16, 256), BF16)

    mine, other = k * 640, (1 - k) * 640

    def w_src(first):
        return w_in.at[pl.ds(pl.multiple_of(mine + first, 64), 320)]

    send(w_src(0), w_part(mine, 320, s), "w0", {"fsdp": up_y})
    send(w_src(320), w_part(mine + 320, 320, s), "w1", {"fsdp": down_y})
    send(w_src(320), w_part(mine + 320, 320, s), "w2", {"fsdp": up_y})
    send(w_src(0), w_part(mine, 320, s), "w3", {"fsdp": down_y})

    settle(head_par, s_head)
    for name in ("bc", "dt", "taps_x", "taps_bc", "bias", "x", "gain", "down"):
        local[name].wait()
    pick20 = jnp.where(
        lax.broadcasted_iota(jnp.int32, (HEADS, 128), 0) == lax.broadcasted_iota(jnp.int32, (HEADS, 128), 1), 1.0, 0.0)

    def head_row(i):
        return dot(jnp.broadcast_to(head_par[i], (8, HEADS)), pick20, precision=lax.Precision.HIGHEST)

    step_bias = head_row(0)[0:1, :]
    rate = jnp.exp(head_row(1))[0:1, :]
    skip[...] = widen(head_row(2))
    for i in range(10):
        gain[:, i * 128 : i * 128 + 128] = gain_rows[i : i + 1, :]

    settle(dt_all.at[pl.ds(0, 3)], r3.at[0])

    row = lax.broadcasted_iota(jnp.int32, (128, 128), 0)
    col = lax.broadcasted_iota(jnp.int32, (128, 128), 1)
    causal = row >= col
    tri = jnp.where(causal, 1.0, 0.0)
    pick_row = lax.broadcasted_iota(jnp.int32, (24, 128), 0)
    pick_col = lax.broadcasted_iota(jnp.int32, (24, 128), 1)
    hit = jnp.logical_and(pick_row == pick_col + 4 * lax.rem(t, 2), pick_col < HEADS)
    pick = jnp.where(hit, 1.0, 0.0).astype(BF16)

    total = jnp.zeros((1, 128), F32)
    for p in range(4):
        raw = dot(dt_all[p], pick, TN) + step_bias
        step_now = jnp.maximum(raw, 0.0) + jnp.log1p(jnp.exp(-jnp.abs(raw)))
        cum_now = dot(tri, -step_now * rate, precision=lax.Precision.HIGHEST)
        step[p] = step_now
        cum[p] = cum_now
        log_start[p] = jnp.broadcast_to(total, (8, 128))
        total = total + cum_now[127:128, :]
    for p in range(4):
        log_tail[p] = total - log_start[p] - cum[p, 127:128, :]
        kept[p] = widen(jnp.broadcast_to(jnp.exp(cum[p, 127:128, :]), (8, 128)))
    dec_all[c] = jnp.broadcast_to(jnp.exp(total), (8, 128))

    arrived(bc_rows(left, 0, 64), "b0")
    send(b_lanes(left, 0), b_lanes(left, 0), "b4", {"tensor": right})
    arrived(bc_rows(right, 64, 64), "b1")
    send(b_lanes(right, 64), b_lanes(right, 64), "b5", {"tensor": left})
    pieces = ((0, 5), (5, 3), (8, 2))

    def x_lanes(p, first, piece):
        return x_ext.at[
            pl.ds(pl.multiple_of(16 + p * ROWS + first, 16), 64), pl.ds(piece[0] * 128, piece[1] * 128)]

    arrived(xr.at[0], "x0")
    arrived(xr.at[1], "x1")
    for piece in pieces:
        lanes = pl.ds(piece[0] * 128, piece[1] * 128)
        send(xr.at[0, :, lanes], x_lanes(left, 0, piece), "x4%d" % piece[0], {"tensor": right})
        send(xr.at[1, :, lanes], x_lanes(right, 64, piece), "x5%d" % piece[0], {"tensor": left})
    send(bc_in.at[pl.ds(64, 64), pl.ds(128, 128)], c_lanes(t, 64), "c2", {"tensor": right})
    send(bc_in.at[pl.ds(0, 64), pl.ds(128, 128)], c_lanes(t, 0), "c3", {"tensor": left})
    send(c_lanes(left, 0), c_lanes(left, 0), "c4", {"tensor": right})
    send(c_lanes(right, 64), c_lanes(right, 64), "c5", {"tensor": left})
    far_start(z_in, zr, "z")

    def gate_near(first):
        rows = pl.ds(first, 64)
        send(z_in.at[rows, columns(right)], z_rows(t, first, 64), "z2%d" % first, {"tensor": right})
        send(z_in.at[rows, columns(left)], z_rows(t, first, 64), "z3%d" % first, {"tensor": left})

    gate_near(0)

    def decay_copy(j):
        return pltpu.make_async_remote_copy(
            src_ref=dec_all.at[c], dst_ref=dec_all.at[c],
            send_sem=sd, recv_sem=rd, device_id=context_peer(j), device_id_type=MESH)

    exchange(decay_copy)
    send_triple(lambda j: (gt.at[t], gt.at[t], {"tensor": tensor_peer(j)}), 1)

    def convolved(ext, p, lanes, taps, bias_row):
        v = ext[pl.ds(pl.multiple_of(p * ROWS, 16), ROWS + 16), lanes].astype(F32)
        acc = bias[pl.ds(bias_row, 1), :] + taps[0:1, lanes] * pltpu.roll(v, 3, 0)
        acc = acc + taps[1:2, lanes] * pltpu.roll(v, 2, 0)
        acc = acc + taps[2:3, lanes] * pltpu.roll(v, 1, 0)
        acc = acc + taps[3:4, lanes] * v
        return silu(acc[16:]).astype(BF16)

    @pl.when(c > 0)
    def _():
        arrived(rim_x, "rim_x")
        arrived(rim_b, "rim_b")
        x_ext[0:16, :] = jnp.concatenate([rim_x[...], rim_x[...]], axis=0)
        bc_ext[0:16, :] = jnp.concatenate([rim_b[...], rim_b[...]], axis=0)

    state[...] = jnp.zeros((STATE, WIDTH), F32)

    def shared(half):
        def of(i, carry):
            p = lax.rem(t + i, 4)
            bcc[p, :, pl.ds(half * 128, 128)] = convolved(bc_ext, p, pl.ds(half * 128, 128), taps_bc, 40 + half)
            return carry

        return of

    def block(first, count):
        def of(i, carry):
            p = lax.rem(t + i, 4)
            lanes = pl.ds(first * 128, count * 128)

            def lanes_of(j, inner):
                xc[p, :, tile(j)] = convolved(x_ext, p, tile(j), taps_x, 10 * t + j)
                return inner

            lax.fori_loop(first, first + count, lanes_of, 0)
            scaled = (xc[p, :, lanes].astype(F32) * weights[p, :, lanes]).astype(BF16)
            fresh = dot(bcc[p, :, 0:128], scaled, TN)
            blocks[p, :, lanes] = fresh
            state[:, lanes] = state[:, lanes] + tails[p, 0:1, lanes] * fresh
            return carry

        return of

    def weigh(p, carry):
        cum_now = cum[p]
        weights[p] = widen(step[p] * jnp.exp(cum_now[127:128, :] - cum_now))
        tails[p] = widen(jnp.exp(log_tail[p]))
        return carry

    lax.fori_loop(0, 4, weigh, 0)
    arrived(w_part(mine, 320, down_y), "w0")
    send(w_part(mine, 320, down_y), w_part(mine, 320, down_y), "w4", {"fsdp": up_y})
    arrived(w_part(mine + 320, 320, up_y), "w1")
    send(w_part(mine + 320, 320, up_y), w_part(mine + 320, 320, up_y), "w5", {"fsdp": down_y})
    settle(dec_all.at[pl.ds(0, 15)], rd)
    dec_wide[...] = widen(dec_all[...].reshape(128, 128))
    arrived(b_lanes(left, 64), "b2")
    arrived(b_lanes(right, 0), "b3")
    lax.fori_loop(0, 2, shared(0), 0)
    arrived(x_ext.at[pl.ds(16, 256)], "x2")
    lax.fori_loop(0, 2, block(0, 10), 0)
    core = {"context_1": 1 - k}

    def half_lanes(h):
        return pl.ds(h * 640, 640)

    rows_mine = pl.ds(pl.multiple_of(64 * k, 64), 64)
    rows_other = pl.ds(pl.multiple_of(64 * (1 - k), 64), 64)

    def pair(h):
        send(state.at[rows_other, half_lanes(h)], peer_state.at[:, half_lanes(h)], "pair%d" % h, core)

    arrived(bc_ext.at[pl.ds(16, 128), pl.ds(0, 128)], "b4")
    lax.fori_loop(2, 4, shared(0), 0)
    for piece in pieces:
        arrived(x_lanes(far, 0, piece), "x4%d" % piece[0])
        arrived(x_lanes(far, 64, piece), "x5%d" % piece[0])
        lax.fori_loop(2, 4, block(*piece), 0)
        if piece[0] == 0:
            pair(0)
    pair(1)

    decay_second = dec_wide[pl.ds(pl.multiple_of(16 * z + 8, 8), 8), :]
    weight_mine = jnp.where(k == 0, decay_second, jnp.ones_like(decay_second))
    weight_peer = jnp.where(k == 0, jnp.ones_like(decay_second), decay_second)

    def state_copy(h):
        def of(j):
            return pltpu.make_async_remote_copy(
                src_ref=st_send.at[h, chip_at(j - 1)], dst_ref=st_recv.at[h, z],
                send_sem=sc.at[h], recv_sem=rc_.at[h], device_id=chip_peer(j), device_id_type=MESH)

        return of

    for h in range(2):
        arrived(peer_state.at[:, half_lanes(h)], "pair%d" % h)
        first_lane, last_lane = h * 640, h * 640 + 640

        def pack_state(i, carry):
            rows = pl.ds(pl.multiple_of(64 * k + i * 8, 8), 8)
            rows_peer = pl.ds(pl.multiple_of(i * 8, 8), 8)
            both = (weight_mine[:, first_lane:last_lane] * state[rows, half_lanes(h)]
                    + weight_peer[:, first_lane:last_lane] * peer_state[rows_peer, half_lanes(h)])
            st_send[h, i] = both.astype(BF16)
            return carry

        lax.fori_loop(0, 8, pack_state, 0)
        exchange(state_copy(h), 8)
        st_recv[h, z] = st_send[h, z]

    arrived(bc_ext.at[pl.ds(16, 256), pl.ds(0, 128)], "c2")
    lax.fori_loop(0, 4, shared(1), 0)

    def inside(p, carry):
        b_now, c_now = bcc[p, :, 0:128], bcc[p, :, 128:256]
        gram = dot(c_now, b_now, NT)
        cum_now = cum[p]
        shifted = (cum_now - jnp.log(step[p])).T
        lane = lax.broadcasted_iota(jnp.int32, (1, 128), 1)
        low = jnp.where(lane < 64, 1.0, 0.0)
        for q in range(HEADS // 2):
            mats = []
            for h in (2 * q, 2 * q + 1):
                gap = cum_now[:, h : h + 1] - shifted[h : h + 1, :]
                mats.append(jnp.exp(jnp.where(causal, gap, -1e30)) * gram)
            both = jnp.concatenate(mats, axis=1).astype(BF16)
            x_pair = xc[p, :, pl.ds(q * 128, 128)].astype(F32)
            x_two = jnp.concatenate([x_pair * low, x_pair * (1.0 - low)], axis=0).astype(BF16)
            y_in[p, :, pl.ds(q * 128, 128)] = dot(both, x_two) + x_pair * skip[0:1, pl.ds(q * 128, 128)]
        return carry

    def back_copy(h):
        def of(j):
            return pltpu.make_async_remote_copy(
                src_ref=back_send.at[h, chip_at(j - 1)], dst_ref=back_recv.at[h, z],
                send_sem=sb.at[h], recv_sem=rb.at[h], device_id=chip_peer(j), device_id_type=MESH)

        return of

    for h in range(2):
        lax.fori_loop(2 * h, 2 * h + 2, inside, 0)
        if h == 0:
            far_forward(z_rows, zr, "z")
            gate_near(64)
        settle(st_recv.at[h, pl.ds(0, 7)], rc_.at[h])

        def chain(i, held):
            back_send[h, i] = held.astype(BF16)
            decay = dec_wide[pl.ds(pl.multiple_of(16 * i, 8), 8), half_lanes(h)] * dec_wide[
                pl.ds(pl.multiple_of(16 * i + 8, 8), 8), half_lanes(h)]
            return decay * held + st_recv[h, i].astype(F32)

        lax.fori_loop(0, 8, chain, jnp.zeros((8, 640), F32))
        exchange(back_copy(h), 8)
        back_recv[h, z] = back_send[h, z]

    def starts(j, carry):
        held = jnp.zeros((STATE, 128), F32)
        for p in range(4):
            fresh = blocks[p, :, tile(j)]
            blocks[p, :, tile(j)] = held
            held = kept[p, 0:1, tile(j)] * held + fresh
        return carry

    lax.fori_loop(0, 10, starts, 0)

    arrived(w_part(mine + 320, 320, down_y), "w2")
    send(w_part(mine, 640, down_y), w_part(mine, 640, down_y), "w6", core)
    arrived(w_part(mine, 320, up_y), "w3")
    send(w_part(mine, 640, up_y), w_part(mine, 640, up_y), "w7", core)
    arrived(w_part(mine, 320, far_y), "w4")
    arrived(w_part(mine + 320, 320, far_y), "w5")
    send(w_part(mine, 640, far_y), w_part(mine, 640, far_y), "w8", core)

    def prepare():
        far_wait(z_rows, "z")
        factor = silu(gate[far].astype(F32))
        reach = widen(jnp.exp(cum[far]))
        y_in[far] = (y_in[far] + reach * dot(bcc[far, :, 128:256], blocks[far].astype(BF16))) * factor
        weights[far] = reach * factor
        tails[far] = widen(jnp.exp(log_start[far]))

    for h in range(2):
        if h == 1:
            prepare()
        settle(back_recv.at[h, pl.ds(0, 7)], rb.at[h])
        decay_first = dec_wide[pl.ds(pl.multiple_of(16 * z, 8), 8), half_lanes(h)]

        def unpack_state(i, carry):
            rows = pl.ds(pl.multiple_of(64 * k + i * 8, 8), 8)
            rows_peer = pl.ds(pl.multiple_of(i * 8, 8), 8)
            first = back_recv[h, i].astype(F32)
            span = jnp.where(k == 0, state[rows, half_lanes(h)], peer_state[rows_peer, half_lanes(h)])
            second = decay_first * first + span
            s_in[rows, half_lanes(h)] = jnp.where(k == 0, first, second)
            in_send[rows_peer, half_lanes(h)] = jnp.where(k == 0, second, first)
            return carry

        lax.fori_loop(0, 8, unpack_state, 0)
        send(in_send.at[:, half_lanes(h)], s_in.at[rows_mine, half_lanes(h)], "in%d" % h, core)

    local["w"].wait()
    arrived(wt.at[pl.ds(0, 640), pl.ds(0, 1920)], "w6")
    for h in range(2):
        arrived(s_in.at[rows_other, half_lanes(h)], "in%d" % h)

    def close_block(p, now):
        squares = (now * now).astype(BF16)
        sq[t, pl.ds(p, 1), :] = dot(jnp.ones((8, WIDTH), BF16), squares, NT)[0:1, :]
        out = (now * gain[...]).astype(BF16)
        gated[p] = out
        ap_send[p] = dot(down_t[...], out, NT).astype(BF16)

    def finish(i, carry):
        p = lax.rem(t + i, 4)
        start = blocks[p] + widen(jnp.exp(log_start[p]))[0:1, :] * s_in[...]
        reach = widen(jnp.exp(cum[p]))
        y_now = y_in[p] + reach * dot(bcc[p, :, 128:256], start.astype(BF16))
        close_block(p, y_now * silu(gate[p].astype(F32)))
        return carry

    def project(p, half, store, first=0, count=5):
        def piece(i, carry):
            lanes = pl.ds(pl.multiple_of(i * 256, 256), 256)
            lanes_w = pl.ds(pl.multiple_of(half * HALF + i * 256, 256), 256)
            store(lanes, dot(gated[p], wt[:, lanes_w]))
            return carry

        lax.fori_loop(first, first + count, piece, 0)

    def to_slot(which, extra=None):
        def store(lanes, v):
            if extra is not None:
                v = v + rs_recv[extra, :, lanes].astype(F32)
            rs_send[which, :, lanes] = v.astype(BF16)

        return store

    def piece_at(ref, which, i):
        return ref.at[which, :, pl.ds(i * 256, 256)]

    def ship(which, where, i):
        pltpu.make_async_remote_copy(
            src_ref=piece_at(rs_send, which, i), dst_ref=piece_at(rs_recv, which, i),
            send_sem=sr, recv_sem=rr.at[5 * which + i] if which < 2 else rr_end.at[which - 2],
            device_id={"tensor": where}, device_id_type=MESH).start()

    def landed(which, i):
        piece = piece_at(rs_recv, which, i)
        pltpu.make_async_copy(piece, piece, rr.at[5 * which + i]).wait()

    incoming = (tails[far, 0:1, :] * s_in[...]).astype(BF16)
    close_block(far, y_in[far] + weights[far] * dot(bcc[far, :, 128:256], incoming))
    for i in range(5):
        project(far, 0, to_slot(0), i, 1)
        project(far, 1, to_slot(1), i, 1)
        if i < 3:
            ship(0, right, i)
            ship(1, left, i)
    local["gate"].wait()
    arrived(gate.at[pl.ds(0, 2)], "z20")
    lax.fori_loop(3, 6, finish, 0)
    ap_recv[t] = ap_send[t]
    send_triple(lambda j: (sq.at[t], sq.at[t], {"tensor": tensor_peer(j)}), 2)
    send_triple(lambda j: (ap_send.at[tensor_peer(j)], ap_recv.at[t], {"tensor": tensor_peer(j)}), 3)
    for i in range(3, 5):
        ship(0, right, i)
        ship(1, left, i)
    for i in range(5):
        project(right, 1, to_slot(2), i, 1)
        ship(2, right, i)
        project(left, 0, to_slot(3), i, 1)
        ship(3, left, i)

    settle(gt.at[pl.ds(0, 3)], r3.at[1])
    settle(sq.at[pl.ds(0, 3)], r3.at[2])
    settle(ap_recv.at[pl.ds(0, 3)], r3.at[3])

    def row_scale(p):
        rows = pl.ds(p, 1)
        squares = (sq[0, rows, :] + sq[1, rows, :]) + (sq[2, rows, :] + sq[3, rows, :])
        return lax.rsqrt(squares * (1.0 / 5120.0) + EPS)

    part = [ap_recv[i].astype(F32) for i in range(4)]
    adapter = ((part[0] + part[1]) + (part[2] + part[3])).astype(BF16)
    own_scale = row_scale(t)
    weighted = (scale * own_scale[0:1, :] * adapter.astype(F32)).astype(BF16)
    grad_a_now = jnp.zeros((RANK, WIDTH), F32)
    for p in range(4):
        rows_grad = (row_scale(p)[0:1, :] * gt[p]).astype(BF16)
        grad_a_now = grad_a_now + dot(rows_grad, gated[p])
    grad_b_now = dot(weighted, cot[...])
    for i in range(30):
        v_send[i // 2, i % 2] = (
            grad_a_now[:, i * 128 : i * 128 + 128] if i < 10
            else grad_b_now[:, (i - 10) * 128 : (i - 10) * 128 + 128]).astype(BF16)
    v_send[15] = jnp.zeros((2, RANK, 128), BF16)
    v_recv[c] = v_send[c]

    def v_copy(j):
        return pltpu.make_async_remote_copy(
            src_ref=v_send.at[context_index(j)], dst_ref=v_recv.at[c],
            send_sem=sv, recv_sem=rv, device_id=context_peer(j), device_id_type=MESH)

    exchange(v_copy)

    for i in range(1):
        landed(0, i)
        project(right, 0, to_slot(4, 0), i, 1)
        ship(4, right, i)
        landed(1, i)
        project(left, 1, to_slot(5, 1), i, 1)
        ship(5, left, i)

    settle(v_recv.at[pl.ds(0, 15)], rv)

    def add_v(i, held):
        return held + v_recv[i].astype(F32)

    y_recv[s] = lax.fori_loop(0, 16, add_v, jnp.zeros((2, RANK, 128), F32))
    send_triple(lambda j: (y_recv.at[s], y_recv.at[s], {"fsdp": lax.rem(s + j, 4)}), 4)
    for i in range(1, 5):
        landed(0, i)
        project(right, 0, to_slot(4, 0), i, 1)
        landed(1, i)
        project(left, 1, to_slot(5, 1), i, 1)
    settle(y_recv.at[pl.ds(0, 3)], r3.at[4])
    t_recv[t] = ((y_recv[0] + y_recv[1]) + (y_recv[2] + y_recv[3])).astype(BF16)
    send_triple(lambda j: (t_recv.at[t], t_recv.at[t], {"tensor": tensor_peer(j)}), 5)
    for i in range(1, 5):
        ship(4, right, i)
        ship(5, left, i)

    def own_part(half):
        def store(lanes, v):
            lanes_up = pl.ds(pl.multiple_of(half * HALF + lanes.start, 256), 256)
            own[half, :, lanes] = v + 2.0 * dot(adapter, up[:, lanes_up], TN)

        return store

    project(t, 0, own_part(0))
    project(t, 1, own_part(1))

    settle(t_recv.at[pl.ds(0, 3)], r3.at[5])

    def add_t(i, held):
        keep = jnp.where(jnp.logical_or(c >= 5, i == t), 1.0, 0.0)
        return held + keep * t_recv[i].astype(F32)

    v_all[c] = lax.fori_loop(0, 4, add_t, jnp.zeros((2, RANK, 128), F32)).astype(BF16)

    def all_copy(j):
        return pltpu.make_async_remote_copy(
            src_ref=v_all.at[c], dst_ref=v_all.at[c],
            send_sem=sg, recv_sem=rg, device_id=context_peer(j), device_id_type=MESH)

    exchange(all_copy)

    scale_col = jnp.broadcast_to(own_scale[0:1, :], (128, 128)).T
    for which in range(2, 6):
        pltpu.make_async_copy(rs_recv.at[which], rs_recv.at[which], rr_end.at[which - 2]).wait()

    def close(i, carry):
        lanes = tile(i)
        first = own[0, :, lanes] + rs_recv[4, :, lanes].astype(F32) + rs_recv[3, :, lanes].astype(F32)
        second = own[1, :, lanes] + rs_recv[2, :, lanes].astype(F32) + rs_recv[5, :, lanes].astype(F32)
        mixed[:, lanes] = (scale_col * first).astype(BF16)
        mixed[:, pl.ds(pl.multiple_of(HALF + i * 128, 128), 128)] = (scale_col * second).astype(BF16)
        return carry

    lax.fori_loop(0, 10, close, 0)

    settle(v_all.at[pl.ds(0, 15)], rg)
    for i in range(10):
        grad_a[:, i * 128 : i * 128 + 128] = v_all[i // 2, i % 2].astype(F32)
    for i in range(20):
        grad_b[:, i * 128 : i * 128 + 128] = v_all[5 + i // 2, i % 2].astype(F32)

    for which, buffer in enumerate((dt_all, gt, sq, ap_send, y_recv, t_recv)):
        settle(buffer.at[pl.ds(0, 3)], s3.at[which])
    settle(dec_all.at[pl.ds(0, 15)], sd)
    for h in range(2):
        settle(st_send.at[h, pl.ds(0, 7)], sc.at[h])
        settle(back_send.at[h, pl.ds(0, 7)], sb.at[h])
    settle(v_send.at[pl.ds(0, 15)], sv)
    settle(v_all.at[pl.ds(0, 15)], sg)
    pltpu.make_async_copy(rs_send, rs_send, sr).wait()
    pltpu.make_async_copy(x_ext.at[pl.ds(16, 512)], x_ext.at[pl.ds(16, 512)], sgroup.at[0]).wait()
    pltpu.make_async_copy(gate, gate, sgroup.at[1]).wait()
    settle(bc_ext.at[pl.ds(16, 256), pl.ds(0, 128)], sgroup.at[3])
    settle(peer_state, sgroup.at[4])
    settle(in_send, sgroup.at[5])
    pltpu.make_async_copy(wt.at[:, pl.ds(0, 1920)], wt.at[:, pl.ds(0, 1920)], sgroup.at[2]).wait()
    for copy in started:
        copy.wait_send()
    assert len(slots) <= 33 and len(send_slots) <= 6 and len(local) <= 12

    @pl.when(gives_rim)
    def _():
        settle(x_ext.at[pl.ds(16, 32)], sl.at[0])
        settle(bc_ext.at[pl.ds(16, 32)], sl.at[1])


def shards(
    input_raw, state_proj_raw, gate_branch, step_raw, convolution_taps, convolution_bias, step_bias,
    decay_log_rate, skip_weight, gated_norm_gain, output_weight, adapter_down, adapter_up, cotangent,
):
    hbm = pl.BlockSpec(memory_space=pltpu.HBM)
    vmem = pl.BlockSpec(memory_space=pltpu.VMEM)
    dma = pltpu.SemaphoreType.DMA
    mixed, grad_a, grad_b = pl.pallas_call(
        kernel,
        out_shape=(
            pltpu.VMEM((ROWS, OUT), BF16),
            pltpu.VMEM((RANK, WIDTH), F32),
            pltpu.VMEM((RANK, OUT), F32),
        ),
        in_specs=[hbm] * 14,
        out_specs=(vmem, vmem, vmem),
        scratch_shapes=[
            pltpu.VMEM((16 + 512, WIDTH), BF16),
            pltpu.VMEM((2, 64, WIDTH), BF16),
            pltpu.VMEM((8, WIDTH), BF16),
            pltpu.VMEM((8, 256), BF16),
            pltpu.VMEM((4, ROWS, WIDTH), BF16),
            pltpu.VMEM((16 + 512, 256), BF16),
            pltpu.VMEM((4, ROWS, 256), BF16),
            pltpu.VMEM((4, 24, 128), BF16),
            pltpu.VMEM((4, ROWS, WIDTH), BF16),
            pltpu.VMEM((2, 64, WIDTH), BF16),
            pltpu.VMEM((WIDTH, OUT), BF16),
            pltpu.VMEM((ROWS, OUT), BF16),
            pltpu.VMEM((4, WIDTH), F32),
            pltpu.VMEM((4, 256), F32),
            pltpu.VMEM((42, 128), F32),
            pltpu.VMEM((3, 1, HEADS), F32),
            pltpu.VMEM((10, 128), F32),
            pltpu.VMEM((1, WIDTH), F32),
            pltpu.VMEM((RANK, WIDTH), BF16),
            pltpu.VMEM((RANK, OUT), BF16),
            pltpu.VMEM((8, WIDTH), F32),
            pltpu.VMEM((4, ROWS, WIDTH), F32),
            pltpu.VMEM((4, 8, WIDTH), F32),
            pltpu.VMEM((256, WIDTH), BF16),
            pltpu.VMEM((4, ROWS, 128), F32),
            pltpu.VMEM((4, ROWS, 128), F32),
            pltpu.VMEM((4, 8, 128), F32),
            pltpu.VMEM((4, 8, 128), F32),
            pltpu.VMEM((4, ROWS, WIDTH), F32),
            pltpu.VMEM((4, STATE, WIDTH), F32),
            pltpu.VMEM((4, 8, WIDTH), F32),
            pltpu.VMEM((STATE, WIDTH), F32),
            pltpu.VMEM((64, WIDTH), F32),
            pltpu.VMEM((2, 8, 8, 640), BF16),
            pltpu.VMEM((2, 8, 8, 640), BF16),
            pltpu.VMEM((16, 8, 128), F32),
            pltpu.VMEM((128, WIDTH), F32),
            pltpu.VMEM((2, 8, 8, 640), BF16),
            pltpu.VMEM((2, 8, 8, 640), BF16),
            pltpu.VMEM((64, WIDTH), F32),
            pltpu.VMEM((STATE, WIDTH), F32),
            pltpu.VMEM((4, ROWS, WIDTH), BF16),
            pltpu.VMEM((4, RANK, 128), F32),
            pltpu.VMEM((4, 8, 128), F32),
            pltpu.VMEM((4, RANK, 128), BF16),
            pltpu.VMEM((4, RANK, 128), BF16),
            pltpu.VMEM((6, ROWS, HALF), BF16),
            pltpu.VMEM((6, ROWS, HALF), BF16),
            pltpu.VMEM((2, ROWS, HALF), F32),
            pltpu.VMEM((16, 2, RANK, 128), BF16),
            pltpu.VMEM((16, 2, RANK, 128), BF16),
            pltpu.VMEM((4, 2, RANK, 128), F32),
            pltpu.VMEM((4, 2, RANK, 128), BF16),
            pltpu.VMEM((16, 2, RANK, 128), BF16),
            dma((6,)), dma((33,)), dma((14,)),
            dma((2,)), dma((2,)), dma, dma, dma((2,)), dma((2,)), dma, dma, dma, dma, dma, dma((10,)), dma((4,)), dma((6,)), dma((6,)), dma((6,)), dma,
        ],
        compiler_params=pltpu.CompilerParams(
            collective_id=0, has_side_effects=True, vmem_limit_bytes=60 * 1000 * 1000),
    )(
        input_raw[0], state_proj_raw[0], gate_branch[0], step_raw[0].T, output_weight, cotangent[0],
        convolution_taps, convolution_bias.reshape(42, 128), step_bias[None, :], decay_log_rate[None, :],
        skip_weight[None, :], gated_norm_gain.reshape(10, 128), adapter_down.T, adapter_up,
    )
    return (mixed[None], grad_a.T, grad_b)


def solution(mesh):
    torus = Mesh(
        mesh.devices.reshape(8, 2, mesh.shape["tensor"], mesh.shape["fsdp"]),
        ("context_0", "context_1", "tensor", "fsdp"),
    )
    tokens = P("fsdp", CONTEXT_TENSOR, None)
    return jax.shard_map(
        shards,
        mesh=torus,
        in_specs=(
            tokens, tokens, tokens, tokens, P(), P(), P("tensor"), P("tensor"), P("tensor"), P("tensor"),
            P("tensor", "fsdp"), P("tensor", None), P(), tokens,
        ),
        out_specs=(tokens, P("tensor", None), P()),
        check_vma=False,
    )
```

```python
import functools

import jax
import jax.numpy as jnp
from jax import lax
from jax.experimental import pallas as pl
from jax.experimental.pallas import tpu as pltpu
from jax.sharding import Mesh
from jax.sharding import PartitionSpec as P

MESH = pl.DeviceIdType.MESH
CONTEXT_TENSOR = ("context_0", "context_1", "tensor")
F32 = jnp.float32
BF16 = jnp.bfloat16

ROWS = 128
WIDTH = 1280
STATE = 128
OUT = 2560
HALF = 1280
RANK = 16
HEADS = 20
COLS = 640
TOKENS = 32768
EPS = 1e-05

NT = (((1,), (1,)), ((), ()))
TN = (((0,), (0,)), ((), ()))


def silu(v):
    half = 0.5 * v
    return half + half * jnp.tanh(half)


def dot(a, b, dims=(((1,), (0,)), ((), ())), precision=None):
    return lax.dot_general(a, b, dims, precision=precision, preferred_element_type=F32)


def kernel(
    x_in, bc_in, z_in, dt_in, w_in, cot_in, taps_in, bias_in, step_bias_in, rate_in, skip_in, gain_in, down_in, up_in,
    mixed, grad_a, grad_b,
    x_here, x_ext, xr, rim_x, rim_b, xc, bc_ext, bcc, dt_all, gate, zr, wt, cot,
    taps_x, taps_bc, bias, head_par, gain_rows, gain, down_t, up, skip, weights, tails,
    spread, step, cum, log_start, log_tail, y_in, blocks, kept, state, peer_state,
    st_send, st_recv, dec_all, dec_wide, back_send, back_recv, in_send, s_in,
    gated, gt, sq, ap_send, ap_recv,
    rs_send, rs_recv, own,
    v_send, v_recv, y_recv, t_recv, v_all,
    sx, rx, sl, sc, rc_, sd, rd, sb, rb, sv, rv, sg, rg, sr, rr, rr_end, sgroup, s3, r3, s_head,
):
    z, k = lax.axis_index("context_0"), lax.axis_index("context_1")
    t, s = lax.axis_index("tensor"), lax.axis_index("fsdp")
    c = 2 * z + k
    right, left, far = lax.rem(t + 1, 4), lax.rem(t + 3, 4), lax.rem(t + 2, 4)
    up_y, down_y, far_y = lax.rem(s + 1, 4), lax.rem(s + 3, 4), lax.rem(s + 2, 4)
    started = []
    slots, send_slots = {}, {}

    together = {"c3": "c2", "c4": "c2", "c5": "c2", "z30": "z20", "z264": "z20", "z364": "z20",
                "b5": "b4", "x3": "x2", "w7": "w6", "w8": "w6"}

    def slot(name):
        return slots.setdefault(together.get(name, name), len(slots))

    def send_slot(name):
        return send_slots.setdefault(name, len(send_slots))

    groups = {"x": 0, "z": 1, "w": 2, "c": 3, "p": 4, "i": 5}

    def send(src, dst, name, where):
        grouped = groups.get(name[0])
        copy = pltpu.make_async_remote_copy(
            src_ref=src, dst_ref=dst,
            send_sem=sx.at[send_slot(name)] if grouped is None else sgroup.at[grouped],
            recv_sem=rx.at[slot(name)], device_id=where, device_id_type=MESH,
        )
        copy.start()
        if groups.get(name[0]) is None:
            started.append(copy)

    def send_triple(make, which):
        for j in (2, 1, 3):
            src, dst, where = make(j)
            pltpu.make_async_remote_copy(
                src_ref=src, dst_ref=dst, send_sem=s3.at[which], recv_sem=r3.at[which],
                device_id=where, device_id_type=MESH).start()

    def tensor_peer(j):
        return lax.rem(t + j, 4)

    def arrived(dst, name):
        pltpu.make_async_copy(dst, dst, rx.at[slot(name)]).wait()

    def chip_at(i):
        step_now = lax.div(i + 1, 2)
        return lax.rem(z + 4 + (1 - 2 * lax.rem(i, 2)) * step_now, 8)

    def core_at(j):
        return lax.rem(k + j, 2)

    def context_index(j):
        return 2 * chip_at(lax.div(j - 1, 2)) + core_at(j)

    def context_peer(j):
        return {"context_0": chip_at(lax.div(j - 1, 2)), "context_1": core_at(j)}

    def chip_peer(j):
        return {"context_0": chip_at(j - 1)}

    def exchange(make, how_many=16):
        def go(j, carry):
            make(j).start()
            return carry

        lax.fori_loop(1, how_many, go, 0)

    def settle(several, sem):
        pltpu.make_async_copy(several, several, sem).wait()

    def tile(i):
        return pl.ds(pl.multiple_of(i * 128, 128), 128)

    barrier = pltpu.get_barrier_semaphore()

    def greet(j, carry):
        pl.semaphore_signal(barrier, inc=1, device_id=context_peer(j), device_id_type=MESH)
        return carry

    lax.fori_loop(1, 16, greet, 0)
    for j in range(1, 4):
        pl.semaphore_signal(barrier, inc=1, device_id={"tensor": lax.rem(t + j, 4)}, device_id_type=MESH)
        pl.semaphore_signal(barrier, inc=1, device_id={"fsdp": lax.rem(s + j, 4)}, device_id_type=MESH)
    before = lax.rem(c + 15, 16)
    after = lax.rem(c + 1, 16)

    @pl.when(c > 0)
    def _():
        pl.semaphore_signal(
            barrier, inc=1,
            device_id={"context_0": lax.div(before, 2), "context_1": lax.rem(before, 2), "tensor": 3},
            device_id_type=MESH,
        )

    def columns(p):
        return pl.ds(pl.multiple_of(p * WIDTH, WIDTH), WIDTH)

    def x_rows(p, first, count):
        return x_ext.at[pl.ds(pl.multiple_of(16 + p * ROWS + first, 16), count)]

    def z_rows(p, first, count):
        return gate.at[p, pl.ds(first, count)]

    def bc_rows(p, first, count):
        return bc_ext.at[pl.ds(pl.multiple_of(16 + p * ROWS + first, 16), count)]

    def b_lanes(p, first):
        return bc_ext.at[pl.ds(pl.multiple_of(16 + p * ROWS + first, 16), 64), pl.ds(0, 128)]

    def c_lanes(p, first):
        return bc_ext.at[pl.ds(pl.multiple_of(16 + p * ROWS + first, 16), 64), pl.ds(128, 128)]

    def w_part(rows_from, count, y):
        return wt.at[
            pl.ds(pl.multiple_of(rows_from, 64), count), pl.ds(pl.multiple_of(y * COLS, COLS), COLS)
        ]

    def dt_window(p):
        return dt_in.at[pl.ds(pl.multiple_of(8 * lax.div(5 * p, 2), 8), 24)]

    local = {}

    def copy_here(name, src, dst):
        local[name] = pltpu.make_async_copy(src, dst, sl.at[2 + len(local)])
        local[name].start()

    copy_here("x_all", x_in, x_here)
    copy_here("cot", cot_in, cot)
    copy_here("up", up_in, up)
    for i, source in enumerate((step_bias_in, rate_in, skip_in)):
        pltpu.make_async_copy(source, head_par.at[i], s_head).start()
    copy_here("bc", bc_in, bc_rows(t, 0, ROWS))
    copy_here("dt", dt_window(t), dt_all.at[t])
    copy_here("taps_x", taps_in.at[:, columns(t)], taps_x)
    copy_here("taps_bc", taps_in.at[:, pl.ds(4 * WIDTH, 256)], taps_bc)
    copy_here("bias", bias_in, bias)
    copy_here("x", x_in.at[:, columns(t)], x_rows(t, 0, ROWS))
    copy_here("gain", gain_in, gain_rows)
    copy_here("down", down_in, down_t)
    copy_here("gate", z_in.at[:, columns(t)], gate.at[t])
    copy_here("w", w_in, w_part(0, 1280, s))

    local["x_all"].wait()

    gives_rim = jnp.logical_and(t == 3, c < 15)

    @pl.when(gives_rim)
    def _():
        pl.semaphore_wait(barrier, 25)

    @pl.when(jnp.logical_not(gives_rim))
    def _():
        pl.semaphore_wait(barrier, 21)

    def far_start(src, relay, name):
        send(src.at[pl.ds(0, 64), columns(far)], relay.at[0], name + "0", {"tensor": right})
        send(src.at[pl.ds(64, 64), columns(far)], relay.at[1], name + "1", {"tensor": left})

    def near_start(src, rows, name):
        send(src.at[:, columns(right)], rows(t, 0, ROWS), name + "2", {"tensor": right})
        send(src.at[:, columns(left)], rows(t, 0, ROWS), name + "3", {"tensor": left})

    def far_forward(rows, relay, name):
        arrived(relay.at[0], name + "0")
        send(relay.at[0], rows(left, 0, 64), name + "4", {"tensor": right})
        arrived(relay.at[1], name + "1")
        send(relay.at[1], rows(right, 64, 64), name + "5", {"tensor": left})

    def far_wait(rows, name):
        arrived(rows(far, 0, 64), name + "4")
        arrived(rows(far, 64, 64), name + "5")

    def rim_copies():
        copies = []
        for p in range(4):
            where = {"context_0": lax.div(after, 2), "context_1": lax.rem(after, 2), "tensor": p}
            copies.append(pltpu.make_async_remote_copy(
                src_ref=x_in.at[pl.ds(120, 8), pl.ds(p * WIDTH, WIDTH)], dst_ref=rim_x,
                send_sem=sl.at[0], recv_sem=rx.at[slot("rim_x")], device_id=where, device_id_type=MESH))
            copies.append(pltpu.make_async_remote_copy(
                src_ref=bc_in.at[pl.ds(120, 8)], dst_ref=rim_b,
                send_sem=sl.at[1], recv_sem=rx.at[slot("rim_b")], device_id=where, device_id_type=MESH))
        return copies

    @pl.when(gives_rim)
    def _():
        for copy in rim_copies():
            copy.start()

    far_start(x_here, xr, "x")
    send(bc_in.at[pl.ds(0, 64)], bc_rows(t, 0, 64), "b0", {"tensor": right})
    send(bc_in.at[pl.ds(64, 64)], bc_rows(t, 64, 64), "b1", {"tensor": left})
    send(bc_in.at[pl.ds(64, 64), pl.ds(0, 128)], b_lanes(t, 64), "b2", {"tensor": right})
    send(bc_in.at[pl.ds(0, 64), pl.ds(0, 128)], b_lanes(t, 0), "b3", {"tensor": left})
    send_triple(lambda j: (dt_window(tensor_peer(j)), dt_all.at[t], {"tensor": tensor_peer(j)}), 0)
    near_start(x_here, x_rows, "x")

    @pl.when(c == 0)
    def _():
        x_ext[0:16, :] = jnp.zeros((16, WIDTH), BF16)
        bc_ext[0:16, :] = jnp.zeros((16, 256), BF16)

    mine, other = k * 640, (1 - k) * 640

    def w_src(first):
        return w_in.at[pl.ds(pl.multiple_of(mine + first, 64), 320)]

    send(w_src(0), w_part(mine, 320, s), "w0", {"fsdp": up_y})
    send(w_src(320), w_part(mine + 320, 320, s), "w1", {"fsdp": down_y})
    send(w_src(320), w_part(mine + 320, 320, s), "w2", {"fsdp": up_y})
    send(w_src(0), w_part(mine, 320, s), "w3", {"fsdp": down_y})

    def head_mask(i, carry):
        head = lax.broadcasted_iota(jnp.int32, (256, 128), 0)
        head = jnp.where(head >= 128, head - 128, head)
        lane = lax.broadcasted_iota(jnp.int32, (256, 128), 1)
        own_head = 2 * i + jnp.where(lane >= 64, 1, 0)
        spread[:, tile(i)] = jnp.where(head == own_head, 1.0, 0.0).astype(BF16)
        return carry

    lax.fori_loop(0, 10, head_mask, 0)

    def widen(v):
        high = v.astype(BF16)
        low = (v - high.astype(F32)).astype(BF16)
        return dot(jnp.concatenate([high, low], axis=1), spread[...])

    scale = 2.0 / (TOKENS ** 0.5)

    local["cot"].wait()
    local["up"].wait()
    gt[t] = dot(up[...], cot[...], NT) * scale

    settle(head_par, s_head)
    for name in ("bc", "dt", "taps_x", "taps_bc", "bias", "x", "gain", "down"):
        local[name].wait()
    pick20 = jnp.where(
        lax.broadcasted_iota(jnp.int32, (HEADS, 128), 0) == lax.broadcasted_iota(jnp.int32, (HEADS, 128), 1), 1.0, 0.0)

    def head_row(i):
        return dot(jnp.broadcast_to(head_par[i], (8, HEADS)), pick20, precision=lax.Precision.HIGHEST)

    step_bias = head_row(0)[0:1, :]
    rate = jnp.exp(head_row(1))[0:1, :]
    skip[...] = widen(head_row(2))
    for i in range(10):
        gain[:, i * 128 : i * 128 + 128] = gain_rows[i : i + 1, :]

    settle(dt_all.at[pl.ds(0, 3)], r3.at[0])

    row = lax.broadcasted_iota(jnp.int32, (128, 128), 0)
    col = lax.broadcasted_iota(jnp.int32, (128, 128), 1)
    causal = row >= col
    tri = jnp.where(causal, 1.0, 0.0)
    pick_row = lax.broadcasted_iota(jnp.int32, (24, 128), 0)
    pick_col = lax.broadcasted_iota(jnp.int32, (24, 128), 1)
    hit = jnp.logical_and(pick_row == pick_col + 4 * lax.rem(t, 2), pick_col < HEADS)
    pick = jnp.where(hit, 1.0, 0.0).astype(BF16)

    total = jnp.zeros((1, 128), F32)
    for p in range(4):
        raw = dot(dt_all[p], pick, TN) + step_bias
        step_now = jnp.maximum(raw, 0.0) + jnp.log1p(jnp.exp(-jnp.abs(raw)))
        cum_now = dot(tri, -step_now * rate, precision=lax.Precision.HIGHEST)
        step[p] = step_now
        cum[p] = cum_now
        log_start[p] = jnp.broadcast_to(total, (8, 128))
        total = total + cum_now[127:128, :]
    for p in range(4):
        log_tail[p] = total - log_start[p] - cum[p, 127:128, :]
        kept[p] = widen(jnp.broadcast_to(jnp.exp(cum[p, 127:128, :]), (8, 128)))
    dec_all[c] = jnp.broadcast_to(jnp.exp(total), (8, 128))

    arrived(bc_rows(left, 0, 64), "b0")
    send(b_lanes(left, 0), b_lanes(left, 0), "b4", {"tensor": right})
    arrived(bc_rows(right, 64, 64), "b1")
    send(b_lanes(right, 64), b_lanes(right, 64), "b5", {"tensor": left})
    pieces = ((0, 5), (5, 3), (8, 2))

    def x_lanes(p, first, piece):
        return x_ext.at[
            pl.ds(pl.multiple_of(16 + p * ROWS + first, 16), 64), pl.ds(piece[0] * 128, piece[1] * 128)]

    arrived(xr.at[0], "x0")
    arrived(xr.at[1], "x1")
    for piece in pieces:
        lanes = pl.ds(piece[0] * 128, piece[1] * 128)
        send(xr.at[0, :, lanes], x_lanes(left, 0, piece), "x4%d" % piece[0], {"tensor": right})
        send(xr.at[1, :, lanes], x_lanes(right, 64, piece), "x5%d" % piece[0], {"tensor": left})
    send(bc_in.at[pl.ds(64, 64), pl.ds(128, 128)], c_lanes(t, 64), "c2", {"tensor": right})
    send(bc_in.at[pl.ds(0, 64), pl.ds(128, 128)], c_lanes(t, 0), "c3", {"tensor": left})
    send(c_lanes(left, 0), c_lanes(left, 0), "c4", {"tensor": right})
    send(c_lanes(right, 64), c_lanes(right, 64), "c5", {"tensor": left})
    far_start(z_in, zr, "z")

    def gate_near(first):
        rows = pl.ds(first, 64)
        send(z_in.at[rows, columns(right)], z_rows(t, first, 64), "z2%d" % first, {"tensor": right})
        send(z_in.at[rows, columns(left)], z_rows(t, first, 64), "z3%d" % first, {"tensor": left})

    gate_near(0)

    def decay_copy(j):
        return pltpu.make_async_remote_copy(
            src_ref=dec_all.at[c], dst_ref=dec_all.at[c],
            send_sem=sd, recv_sem=rd, device_id=context_peer(j), device_id_type=MESH)

    exchange(decay_copy)
    send_triple(lambda j: (gt.at[t], gt.at[t], {"tensor": tensor_peer(j)}), 1)

    def convolved(ext, p, lanes, taps, bias_row):
        v = ext[pl.ds(pl.multiple_of(p * ROWS, 16), ROWS + 16), lanes].astype(F32)
        acc = bias[pl.ds(bias_row, 1), :] + taps[0:1, lanes] * pltpu.roll(v, 3, 0)
        acc = acc + taps[1:2, lanes] * pltpu.roll(v, 2, 0)
        acc = acc + taps[2:3, lanes] * pltpu.roll(v, 1, 0)
        acc = acc + taps[3:4, lanes] * v
        return silu(acc[16:]).astype(BF16)

    @pl.when(c > 0)
    def _():
        arrived(rim_x, "rim_x")
        arrived(rim_b, "rim_b")
        x_ext[0:16, :] = jnp.concatenate([rim_x[...], rim_x[...]], axis=0)
        bc_ext[0:16, :] = jnp.concatenate([rim_b[...], rim_b[...]], axis=0)

    state[...] = jnp.zeros((STATE, WIDTH), F32)

    def shared(half):
        def of(i, carry):
            p = lax.rem(t + i, 4)
            bcc[p, :, pl.ds(half * 128, 128)] = convolved(bc_ext, p, pl.ds(half * 128, 128), taps_bc, 40 + half)
            return carry

        return of

    def block(first, count):
        def of(i, carry):
            p = lax.rem(t + i, 4)
            lanes = pl.ds(first * 128, count * 128)

            def lanes_of(j, inner):
                xc[p, :, tile(j)] = convolved(x_ext, p, tile(j), taps_x, 10 * t + j)
                return inner

            lax.fori_loop(first, first + count, lanes_of, 0)
            scaled = (xc[p, :, lanes].astype(F32) * weights[p, :, lanes]).astype(BF16)
            fresh = dot(bcc[p, :, 0:128], scaled, TN)
            blocks[p, :, lanes] = fresh
            state[:, lanes] = state[:, lanes] + tails[p, 0:1, lanes] * fresh
            return carry

        return of

    def weigh(p, carry):
        cum_now = cum[p]
        weights[p] = widen(step[p] * jnp.exp(cum_now[127:128, :] - cum_now))
        tails[p] = widen(jnp.exp(log_tail[p]))
        return carry

    lax.fori_loop(0, 4, weigh, 0)
    arrived(w_part(mine, 320, down_y), "w0")
    send(w_part(mine, 320, down_y), w_part(mine, 320, down_y), "w4", {"fsdp": up_y})
    arrived(w_part(mine + 320, 320, up_y), "w1")
    send(w_part(mine + 320, 320, up_y), w_part(mine + 320, 320, up_y), "w5", {"fsdp": down_y})
    settle(dec_all.at[pl.ds(0, 15)], rd)
    dec_wide[...] = widen(dec_all[...].reshape(128, 128))
    arrived(b_lanes(left, 64), "b2")
    arrived(b_lanes(right, 0), "b3")
    lax.fori_loop(0, 2, shared(0), 0)
    arrived(x_ext.at[pl.ds(16, 256)], "x2")
    lax.fori_loop(0, 2, block(0, 10), 0)
    core = {"context_1": 1 - k}

    def half_lanes(h):
        return pl.ds(h * 640, 640)

    rows_mine = pl.ds(pl.multiple_of(64 * k, 64), 64)
    rows_other = pl.ds(pl.multiple_of(64 * (1 - k), 64), 64)

    def pair(h):
        send(state.at[rows_other, half_lanes(h)], peer_state.at[:, half_lanes(h)], "pair%d" % h, core)

    arrived(bc_ext.at[pl.ds(16, 128), pl.ds(0, 128)], "b4")
    lax.fori_loop(2, 4, shared(0), 0)
    for piece in pieces:
        arrived(x_lanes(far, 0, piece), "x4%d" % piece[0])
        arrived(x_lanes(far, 64, piece), "x5%d" % piece[0])
        lax.fori_loop(2, 4, block(*piece), 0)
        if piece[0] == 0:
            pair(0)
    pair(1)

    decay_second = dec_wide[pl.ds(pl.multiple_of(16 * z + 8, 8), 8), :]
    weight_mine = jnp.where(k == 0, decay_second, jnp.ones_like(decay_second))
    weight_peer = jnp.where(k == 0, jnp.ones_like(decay_second), decay_second)

    def state_copy(h):
        def of(j):
            return pltpu.make_async_remote_copy(
                src_ref=st_send.at[h, chip_at(j - 1)], dst_ref=st_recv.at[h, z],
                send_sem=sc.at[h], recv_sem=rc_.at[h], device_id=chip_peer(j), device_id_type=MESH)

        return of

    for h in range(2):
        arrived(peer_state.at[:, half_lanes(h)], "pair%d" % h)
        first_lane, last_lane = h * 640, h * 640 + 640

        def pack_state(i, carry):
            rows = pl.ds(pl.multiple_of(64 * k + i * 8, 8), 8)
            rows_peer = pl.ds(pl.multiple_of(i * 8, 8), 8)
            both = (weight_mine[:, first_lane:last_lane] * state[rows, half_lanes(h)]
                    + weight_peer[:, first_lane:last_lane] * peer_state[rows_peer, half_lanes(h)])
            st_send[h, i] = both.astype(BF16)
            return carry

        lax.fori_loop(0, 8, pack_state, 0)
        exchange(state_copy(h), 8)
        st_recv[h, z] = st_send[h, z]

    arrived(bc_ext.at[pl.ds(16, 256), pl.ds(0, 128)], "c2")
    lax.fori_loop(0, 4, shared(1), 0)

    def inside(p, carry):
        b_now, c_now = bcc[p, :, 0:128], bcc[p, :, 128:256]
        gram = dot(c_now, b_now, NT)
        cum_now = cum[p]
        shifted = (cum_now - jnp.log(step[p])).T
        lane = lax.broadcasted_iota(jnp.int32, (1, 128), 1)
        low = jnp.where(lane < 64, 1.0, 0.0)
        for q in range(HEADS // 2):
            mats = []
            for h in (2 * q, 2 * q + 1):
                gap = cum_now[:, h : h + 1] - shifted[h : h + 1, :]
                mats.append(jnp.exp(jnp.where(causal, gap, -1e30)) * gram)
            both = jnp.concatenate(mats, axis=1).astype(BF16)
            x_pair = xc[p, :, pl.ds(q * 128, 128)].astype(F32)
            x_two = jnp.concatenate([x_pair * low, x_pair * (1.0 - low)], axis=0).astype(BF16)
            y_in[p, :, pl.ds(q * 128, 128)] = dot(both, x_two) + x_pair * skip[0:1, pl.ds(q * 128, 128)]
        return carry

    def back_copy(h):
        def of(j):
            return pltpu.make_async_remote_copy(
                src_ref=back_send.at[h, chip_at(j - 1)], dst_ref=back_recv.at[h, z],
                send_sem=sb.at[h], recv_sem=rb.at[h], device_id=chip_peer(j), device_id_type=MESH)

        return of

    for h in range(2):
        lax.fori_loop(2 * h, 2 * h + 2, inside, 0)
        if h == 0:
            far_forward(z_rows, zr, "z")
            gate_near(64)
        settle(st_recv.at[h, pl.ds(0, 7)], rc_.at[h])

        def chain(i, held):
            back_send[h, i] = held.astype(BF16)
            decay = dec_wide[pl.ds(pl.multiple_of(16 * i, 8), 8), half_lanes(h)] * dec_wide[
                pl.ds(pl.multiple_of(16 * i + 8, 8), 8), half_lanes(h)]
            return decay * held + st_recv[h, i].astype(F32)

        lax.fori_loop(0, 8, chain, jnp.zeros((8, 640), F32))
        exchange(back_copy(h), 8)
        back_recv[h, z] = back_send[h, z]

    def starts(j, carry):
        held = jnp.zeros((STATE, 128), F32)
        for p in range(4):
            fresh = blocks[p, :, tile(j)]
            blocks[p, :, tile(j)] = held
            held = kept[p, 0:1, tile(j)] * held + fresh
        return carry

    lax.fori_loop(0, 10, starts, 0)

    arrived(w_part(mine + 320, 320, down_y), "w2")
    send(w_part(mine, 640, down_y), w_part(mine, 640, down_y), "w6", core)
    arrived(w_part(mine, 320, up_y), "w3")
    send(w_part(mine, 640, up_y), w_part(mine, 640, up_y), "w7", core)
    arrived(w_part(mine, 320, far_y), "w4")
    arrived(w_part(mine + 320, 320, far_y), "w5")
    send(w_part(mine, 640, far_y), w_part(mine, 640, far_y), "w8", core)

    def prepare():
        far_wait(z_rows, "z")
        factor = silu(gate[far].astype(F32))
        reach = widen(jnp.exp(cum[far]))
        y_in[far] = (y_in[far] + reach * dot(bcc[far, :, 128:256], blocks[far].astype(BF16))) * factor
        weights[far] = reach * factor
        tails[far] = widen(jnp.exp(log_start[far]))

    for h in range(2):
        if h == 1:
            prepare()
        settle(back_recv.at[h, pl.ds(0, 7)], rb.at[h])
        decay_first = dec_wide[pl.ds(pl.multiple_of(16 * z, 8), 8), half_lanes(h)]

        def unpack_state(i, carry):
            rows = pl.ds(pl.multiple_of(64 * k + i * 8, 8), 8)
            rows_peer = pl.ds(pl.multiple_of(i * 8, 8), 8)
            first = back_recv[h, i].astype(F32)
            span = jnp.where(k == 0, state[rows, half_lanes(h)], peer_state[rows_peer, half_lanes(h)])
            second = decay_first * first + span
            s_in[rows, half_lanes(h)] = jnp.where(k == 0, first, second)
            in_send[rows_peer, half_lanes(h)] = jnp.where(k == 0, second, first)
            return carry

        lax.fori_loop(0, 8, unpack_state, 0)
        send(in_send.at[:, half_lanes(h)], s_in.at[rows_mine, half_lanes(h)], "in%d" % h, core)

    local["w"].wait()
    arrived(wt.at[pl.ds(0, 640), pl.ds(0, 1920)], "w6")
    for h in range(2):
        arrived(s_in.at[rows_other, half_lanes(h)], "in%d" % h)

    def close_block(p, now):
        squares = (now * now).astype(BF16)
        sq[t, pl.ds(p, 1), :] = dot(jnp.ones((8, WIDTH), BF16), squares, NT)[0:1, :]
        out = (now * gain[...]).astype(BF16)
        gated[p] = out
        ap_send[p] = dot(down_t[...], out, NT).astype(BF16)

    def finish(i, carry):
        p = lax.rem(t + i, 4)
        start = blocks[p] + widen(jnp.exp(log_start[p]))[0:1, :] * s_in[...]
        reach = widen(jnp.exp(cum[p]))
        y_now = y_in[p] + reach * dot(bcc[p, :, 128:256], start.astype(BF16))
        close_block(p, y_now * silu(gate[p].astype(F32)))
        return carry

    def project(p, half, store, first=0, count=5):
        def piece(i, carry):
            lanes = pl.ds(pl.multiple_of(i * 256, 256), 256)
            lanes_w = pl.ds(pl.multiple_of(half * HALF + i * 256, 256), 256)
            store(lanes, dot(gated[p], wt[:, lanes_w]))
            return carry

        lax.fori_loop(first, first + count, piece, 0)

    def to_slot(which, extra=None):
        def store(lanes, v):
            if extra is not None:
                v = v + rs_recv[extra, :, lanes].astype(F32)
            rs_send[which, :, lanes] = v.astype(BF16)

        return store

    def piece_at(ref, which, i):
        return ref.at[which, :, pl.ds(i * 256, 256)]

    def ship(which, where, i):
        pltpu.make_async_remote_copy(
            src_ref=piece_at(rs_send, which, i), dst_ref=piece_at(rs_recv, which, i),
            send_sem=sr, recv_sem=rr.at[5 * which + i] if which < 2 else rr_end.at[which - 2],
            device_id={"tensor": where}, device_id_type=MESH).start()

    def landed(which, i):
        piece = piece_at(rs_recv, which, i)
        pltpu.make_async_copy(piece, piece, rr.at[5 * which + i]).wait()

    incoming = (tails[far, 0:1, :] * s_in[...]).astype(BF16)
    close_block(far, y_in[far] + weights[far] * dot(bcc[far, :, 128:256], incoming))
    for i in range(5):
        project(far, 0, to_slot(0), i, 1)
        project(far, 1, to_slot(1), i, 1)
        if i < 3:
            ship(0, right, i)
            ship(1, left, i)
    local["gate"].wait()
    arrived(gate.at[pl.ds(0, 2)], "z20")
    lax.fori_loop(3, 6, finish, 0)
    ap_recv[t] = ap_send[t]
    send_triple(lambda j: (sq.at[t], sq.at[t], {"tensor": tensor_peer(j)}), 2)
    send_triple(lambda j: (ap_send.at[tensor_peer(j)], ap_recv.at[t], {"tensor": tensor_peer(j)}), 3)
    for i in range(3, 5):
        ship(0, right, i)
        ship(1, left, i)
    for i in range(5):
        project(right, 1, to_slot(2), i, 1)
        ship(2, right, i)
        project(left, 0, to_slot(3), i, 1)
        ship(3, left, i)

    settle(gt.at[pl.ds(0, 3)], r3.at[1])
    settle(sq.at[pl.ds(0, 3)], r3.at[2])
    settle(ap_recv.at[pl.ds(0, 3)], r3.at[3])

    def row_scale(p):
        rows = pl.ds(p, 1)
        squares = (sq[0, rows, :] + sq[1, rows, :]) + (sq[2, rows, :] + sq[3, rows, :])
        return lax.rsqrt(squares * (1.0 / 5120.0) + EPS)

    part = [ap_recv[i].astype(F32) for i in range(4)]
    adapter = ((part[0] + part[1]) + (part[2] + part[3])).astype(BF16)
    own_scale = row_scale(t)
    weighted = (scale * own_scale[0:1, :] * adapter.astype(F32)).astype(BF16)
    grad_a_now = jnp.zeros((RANK, WIDTH), F32)
    for p in range(4):
        rows_grad = (row_scale(p)[0:1, :] * gt[p]).astype(BF16)
        grad_a_now = grad_a_now + dot(rows_grad, gated[p])
    grad_b_now = dot(weighted, cot[...])
    for i in range(30):
        v_send[i // 2, i % 2] = (
            grad_a_now[:, i * 128 : i * 128 + 128] if i < 10
            else grad_b_now[:, (i - 10) * 128 : (i - 10) * 128 + 128]).astype(BF16)
    v_send[15] = jnp.zeros((2, RANK, 128), BF16)
    v_recv[c] = v_send[c]

    def v_copy(j):
        return pltpu.make_async_remote_copy(
            src_ref=v_send.at[context_index(j)], dst_ref=v_recv.at[c],
            send_sem=sv, recv_sem=rv, device_id=context_peer(j), device_id_type=MESH)

    exchange(v_copy)

    for i in range(1):
        landed(0, i)
        project(right, 0, to_slot(4, 0), i, 1)
        ship(4, right, i)
        landed(1, i)
        project(left, 1, to_slot(5, 1), i, 1)
        ship(5, left, i)

    settle(v_recv.at[pl.ds(0, 15)], rv)

    def add_v(i, held):
        return held + v_recv[i].astype(F32)

    y_recv[s] = lax.fori_loop(0, 16, add_v, jnp.zeros((2, RANK, 128), F32))
    send_triple(lambda j: (y_recv.at[s], y_recv.at[s], {"fsdp": lax.rem(s + j, 4)}), 4)
    for i in range(1, 5):
        landed(0, i)
        project(right, 0, to_slot(4, 0), i, 1)
        landed(1, i)
        project(left, 1, to_slot(5, 1), i, 1)
    settle(y_recv.at[pl.ds(0, 3)], r3.at[4])
    t_recv[t] = ((y_recv[0] + y_recv[1]) + (y_recv[2] + y_recv[3])).astype(BF16)
    send_triple(lambda j: (t_recv.at[t], t_recv.at[t], {"tensor": tensor_peer(j)}), 5)
    for i in range(1, 5):
        ship(4, right, i)
        ship(5, left, i)

    def own_part(half):
        def store(lanes, v):
            lanes_up = pl.ds(pl.multiple_of(half * HALF + lanes.start, 256), 256)
            own[half, :, lanes] = v + 2.0 * dot(adapter, up[:, lanes_up], TN)

        return store

    project(t, 0, own_part(0))
    project(t, 1, own_part(1))

    settle(t_recv.at[pl.ds(0, 3)], r3.at[5])

    def add_t(i, held):
        keep = jnp.where(jnp.logical_or(c >= 5, i == t), 1.0, 0.0)
        return held + keep * t_recv[i].astype(F32)

    v_all[c] = lax.fori_loop(0, 4, add_t, jnp.zeros((2, RANK, 128), F32)).astype(BF16)

    def all_copy(j):
        return pltpu.make_async_remote_copy(
            src_ref=v_all.at[c], dst_ref=v_all.at[c],
            send_sem=sg, recv_sem=rg, device_id=context_peer(j), device_id_type=MESH)

    exchange(all_copy)

    scale_col = jnp.broadcast_to(own_scale[0:1, :], (128, 128)).T
    for which in range(2, 6):
        pltpu.make_async_copy(rs_recv.at[which], rs_recv.at[which], rr_end.at[which - 2]).wait()

    def close(i, carry):
        lanes = tile(i)
        first = own[0, :, lanes] + rs_recv[4, :, lanes].astype(F32) + rs_recv[3, :, lanes].astype(F32)
        second = own[1, :, lanes] + rs_recv[2, :, lanes].astype(F32) + rs_recv[5, :, lanes].astype(F32)
        mixed[:, lanes] = (scale_col * first).astype(BF16)
        mixed[:, pl.ds(pl.multiple_of(HALF + i * 128, 128), 128)] = (scale_col * second).astype(BF16)
        return carry

    lax.fori_loop(0, 10, close, 0)

    settle(v_all.at[pl.ds(0, 15)], rg)
    for i in range(10):
        grad_a[:, i * 128 : i * 128 + 128] = v_all[i // 2, i % 2].astype(F32)
    for i in range(20):
        grad_b[:, i * 128 : i * 128 + 128] = v_all[5 + i // 2, i % 2].astype(F32)

    for which, buffer in enumerate((dt_all, gt, sq, ap_send, y_recv, t_recv)):
        settle(buffer.at[pl.ds(0, 3)], s3.at[which])
    settle(dec_all.at[pl.ds(0, 15)], sd)
    for h in range(2):
        settle(st_send.at[h, pl.ds(0, 7)], sc.at[h])
        settle(back_send.at[h, pl.ds(0, 7)], sb.at[h])
    settle(v_send.at[pl.ds(0, 15)], sv)
    settle(v_all.at[pl.ds(0, 15)], sg)
    pltpu.make_async_copy(rs_send, rs_send, sr).wait()
    pltpu.make_async_copy(x_ext.at[pl.ds(16, 512)], x_ext.at[pl.ds(16, 512)], sgroup.at[0]).wait()
    pltpu.make_async_copy(gate, gate, sgroup.at[1]).wait()
    settle(bc_ext.at[pl.ds(16, 256), pl.ds(0, 128)], sgroup.at[3])
    settle(peer_state, sgroup.at[4])
    settle(in_send, sgroup.at[5])
    pltpu.make_async_copy(wt.at[:, pl.ds(0, 1920)], wt.at[:, pl.ds(0, 1920)], sgroup.at[2]).wait()
    for copy in started:
        copy.wait_send()
    assert len(slots) <= 33 and len(send_slots) <= 6 and len(local) <= 13

    @pl.when(gives_rim)
    def _():
        settle(x_ext.at[pl.ds(16, 32)], sl.at[0])
        settle(bc_ext.at[pl.ds(16, 32)], sl.at[1])


def shards(
    input_raw, state_proj_raw, gate_branch, step_raw, convolution_taps, convolution_bias, step_bias,
    decay_log_rate, skip_weight, gated_norm_gain, output_weight, adapter_down, adapter_up, cotangent,
):
    hbm = pl.BlockSpec(memory_space=pltpu.HBM)
    vmem = pl.BlockSpec(memory_space=pltpu.VMEM)
    dma = pltpu.SemaphoreType.DMA
    mixed, grad_a, grad_b = pl.pallas_call(
        kernel,
        out_shape=(
            pltpu.VMEM((ROWS, OUT), BF16),
            pltpu.VMEM((RANK, WIDTH), F32),
            pltpu.VMEM((RANK, OUT), F32),
        ),
        in_specs=[hbm] * 14,
        out_specs=(vmem, vmem, vmem),
        scratch_shapes=[
            pltpu.VMEM((ROWS, 4 * WIDTH), BF16),
            pltpu.VMEM((16 + 512, WIDTH), BF16),
            pltpu.VMEM((2, 64, WIDTH), BF16),
            pltpu.VMEM((8, WIDTH), BF16),
            pltpu.VMEM((8, 256), BF16),
            pltpu.VMEM((4, ROWS, WIDTH), BF16),
            pltpu.VMEM((16 + 512, 256), BF16),
            pltpu.VMEM((4, ROWS, 256), BF16),
            pltpu.VMEM((4, 24, 128), BF16),
            pltpu.VMEM((4, ROWS, WIDTH), BF16),
            pltpu.VMEM((2, 64, WIDTH), BF16),
            pltpu.VMEM((WIDTH, OUT), BF16),
            pltpu.VMEM((ROWS, OUT), BF16),
            pltpu.VMEM((4, WIDTH), F32),
            pltpu.VMEM((4, 256), F32),
            pltpu.VMEM((42, 128), F32),
            pltpu.VMEM((3, 1, HEADS), F32),
            pltpu.VMEM((10, 128), F32),
            pltpu.VMEM((1, WIDTH), F32),
            pltpu.VMEM((RANK, WIDTH), BF16),
            pltpu.VMEM((RANK, OUT), BF16),
            pltpu.VMEM((8, WIDTH), F32),
            pltpu.VMEM((4, ROWS, WIDTH), F32),
            pltpu.VMEM((4, 8, WIDTH), F32),
            pltpu.VMEM((256, WIDTH), BF16),
            pltpu.VMEM((4, ROWS, 128), F32),
            pltpu.VMEM((4, ROWS, 128), F32),
            pltpu.VMEM((4, 8, 128), F32),
            pltpu.VMEM((4, 8, 128), F32),
            pltpu.VMEM((4, ROWS, WIDTH), F32),
            pltpu.VMEM((4, STATE, WIDTH), F32),
            pltpu.VMEM((4, 8, WIDTH), F32),
            pltpu.VMEM((STATE, WIDTH), F32),
            pltpu.VMEM((64, WIDTH), F32),
            pltpu.VMEM((2, 8, 8, 640), BF16),
            pltpu.VMEM((2, 8, 8, 640), BF16),
            pltpu.VMEM((16, 8, 128), F32),
            pltpu.VMEM((128, WIDTH), F32),
            pltpu.VMEM((2, 8, 8, 640), BF16),
            pltpu.VMEM((2, 8, 8, 640), BF16),
            pltpu.VMEM((64, WIDTH), F32),
            pltpu.VMEM((STATE, WIDTH), F32),
            pltpu.VMEM((4, ROWS, WIDTH), BF16),
            pltpu.VMEM((4, RANK, 128), F32),
            pltpu.VMEM((4, 8, 128), F32),
            pltpu.VMEM((4, RANK, 128), BF16),
            pltpu.VMEM((4, RANK, 128), BF16),
            pltpu.VMEM((6, ROWS, HALF), BF16),
            pltpu.VMEM((6, ROWS, HALF), BF16),
            pltpu.VMEM((2, ROWS, HALF), F32),
            pltpu.VMEM((16, 2, RANK, 128), BF16),
            pltpu.VMEM((16, 2, RANK, 128), BF16),
            pltpu.VMEM((4, 2, RANK, 128), F32),
            pltpu.VMEM((4, 2, RANK, 128), BF16),
            pltpu.VMEM((16, 2, RANK, 128), BF16),
            dma((6,)), dma((33,)), dma((15,)),
            dma((2,)), dma((2,)), dma, dma, dma((2,)), dma((2,)), dma, dma, dma, dma, dma, dma((10,)), dma((4,)), dma((6,)), dma((6,)), dma((6,)), dma,
        ],
        compiler_params=pltpu.CompilerParams(
            collective_id=0, has_side_effects=True, vmem_limit_bytes=60 * 1000 * 1000),
    )(
        input_raw[0], state_proj_raw[0], gate_branch[0], step_raw[0].T, output_weight, cotangent[0],
        convolution_taps, convolution_bias.reshape(42, 128), step_bias[None, :], decay_log_rate[None, :],
        skip_weight[None, :], gated_norm_gain.reshape(10, 128), adapter_down.T, adapter_up,
    )
    return (mixed[None], grad_a.T, grad_b)


def solution(mesh):
    torus = Mesh(
        mesh.devices.reshape(8, 2, mesh.shape["tensor"], mesh.shape["fsdp"]),
        ("context_0", "context_1", "tensor", "fsdp"),
    )
    tokens = P("fsdp", CONTEXT_TENSOR, None)
    return jax.shard_map(
        shards,
        mesh=torus,
        in_specs=(
            tokens, tokens, tokens, tokens, P(), P(), P("tensor"), P("tensor"), P("tensor"), P("tensor"),
            P("tensor", "fsdp"), P("tensor", None), P(), tokens,
        ),
        out_specs=(tokens, P("tensor", None), P()),
        check_vma=False,
    )
```
